32 devices in a mesh: dp: 1 (over z), sp: 4 (over y), tp: 8 (over x, core).
Axes of the slice: x: 4, y: 4, z: 1, core: 2. Of those that a mesh axis runs over, the one named last changes fastest.
The devices are a block of a 4x4x8 slice.
Arguments:
- x_in: bfloat16 [8192, 8192], P(('dp', 'sp', 'tp'))
- seg_ids: int32 [8192], P(('dp', 'sp', 'tp'))
- w_zx: bfloat16 [8192, 2, 16384], P(None, None, 'tp')
- w_bc: bfloat16 [8192, 2, 1024], P(None, None, 'tp')
- w_dt: bfloat16 [8192, 256], P(None, 'tp')
- conv_x: bfloat16 [4, 16384], P(None, 'tp')
- conv_bc: bfloat16 [4, 2, 1024], P(None, None, 'tp')
- bias_x: bfloat16 [16384], P('tp')
- bias_bc: bfloat16 [2, 1024], P(None, 'tp')
- a_log: float32 [256], P('tp')
- dt_bias: float32 [256], P('tp')
- d_skip: float32 [256], P('tp')
- norm_w: bfloat16 [16384], P('tp')
- w_out: bfloat16 [16384, 8192], P('tp')
Outputs:
- output: bfloat16 [8192, 8192], P(('dp', 'sp', 'tp'))
All inputs are finite; a program needn't handle non-finite values.
Results may differ from the reference program's by a relative error of at most 0.00685.
Values are sent between devices in bfloat16 or wider.
A program may use at most 768 MiB of HBM per device.

```python
import math
import jax
import jax.numpy as jnp
from jax import lax

D_MODEL = 8192
NUM_HEADS = 256
NUM_GROUPS = 8
TOK_DEV = 256
SEQ_SHARDS = 4
HEAD_SHARDS = 8
HEAD_DIM = 64
STATE_DIM = 128
CONV_WIDTH = 4
SSD_TILE = 256
NORM_EPS = 1e-5
SEQ_LEN = TOK_DEV * SEQ_SHARDS * HEAD_SHARDS
BLOCK_LEN = TOK_DEV * HEAD_SHARDS
INNER_DIM = NUM_HEADS * HEAD_DIM
GROUP_WIDTH = NUM_GROUPS * STATE_DIM
PER_GROUP = NUM_HEADS // NUM_GROUPS


def setup_inputs(seed: int = 0, part: int = 0) -> dict:
    shared = jax.random.split(jax.random.key(seed), 12)
    part_key = jax.random.fold_in(jax.random.key(seed + 1), part)
    key_x, key_seg, key_pos = jax.random.split(part_key, 3)
    x_in = jax.random.normal(key_x, (SEQ_LEN, D_MODEL), jnp.float32)
    start_draw = jax.random.randint(key_seg, (SEQ_LEN,), 0, BLOCK_LEN)
    forced_pos = jax.random.randint(key_pos, (), 1, SEQ_LEN)
    is_start = (start_draw == 0) | (jnp.arange(SEQ_LEN) == forced_pos)
    seg_ids = jnp.cumsum(is_start.astype(jnp.int32)).astype(jnp.int32)
    in_scale = D_MODEL ** -0.5
    w_zx = jax.random.normal(shared[0], (D_MODEL, 2, INNER_DIM), jnp.float32) * in_scale
    w_bc = jax.random.normal(shared[1], (D_MODEL, 2, GROUP_WIDTH), jnp.float32) * in_scale
    w_dt = jax.random.normal(shared[2], (D_MODEL, NUM_HEADS), jnp.float32) * in_scale
    conv_x = jax.random.normal(shared[3], (CONV_WIDTH, INNER_DIM), jnp.float32) * 0.5
    conv_bc = jax.random.normal(shared[4], (CONV_WIDTH, 2, GROUP_WIDTH), jnp.float32) * 0.5
    bias_x = jax.random.normal(shared[5], (INNER_DIM,), jnp.float32) * 0.5
    bias_bc = jax.random.normal(shared[6], (2, GROUP_WIDTH), jnp.float32) * 0.5
    a_base = math.log(0.5 * math.sqrt(STATE_DIM / BLOCK_LEN))
    dt_base = math.log(1.0 / math.sqrt(BLOCK_LEN * STATE_DIM))
    a_log = a_base + jax.random.uniform(shared[7], (NUM_HEADS,), jnp.float32, -0.5, 0.5)
    dt_bias = dt_base + jax.random.uniform(shared[8], (NUM_HEADS,), jnp.float32, -0.5, 0.5)
    d_skip = jax.random.uniform(shared[9], (NUM_HEADS,), jnp.float32, 0.5, 1.5)
    norm_w = jax.random.uniform(shared[10], (INNER_DIM,), jnp.float32, 0.5, 1.5)
    w_out = jax.random.normal(shared[11], (INNER_DIM, D_MODEL), jnp.float32) * INNER_DIM ** -0.5
    return {'x_in': x_in.astype(jnp.bfloat16), 'seg_ids': seg_ids, 'w_zx': w_zx.astype(jnp.bfloat16), 'w_bc': w_bc.astype(jnp.bfloat16), 'w_dt': w_dt.astype(jnp.bfloat16), 'conv_x': conv_x.astype(jnp.bfloat16), 'conv_bc': conv_bc.astype(jnp.bfloat16), 'bias_x': bias_x.astype(jnp.bfloat16), 'bias_bc': bias_bc.astype(jnp.bfloat16), 'a_log': a_log, 'dt_bias': dt_bias, 'd_skip': d_skip, 'norm_w': norm_w.astype(jnp.bfloat16), 'w_out': w_out.astype(jnp.bfloat16)}


def reference(x_in, seg_ids, w_zx, w_bc, w_dt, conv_x, conv_bc, bias_x, bias_bc, a_log, dt_bias, d_skip, norm_w, w_out):
    halo_len = CONV_WIDTH - 1
    n_tiles = SEQ_LEN // SSD_TILE
    last_row = SSD_TILE - 1
    conv_w = jnp.concatenate([conv_x, conv_bc.reshape(CONV_WIDTH, 2 * GROUP_WIDTH)], axis=1).astype(jnp.float32)
    conv_b = jnp.concatenate([bias_x, bias_bc.reshape(2 * GROUP_WIDTH)]).astype(jnp.float32)
    decay_rate = jnp.exp(a_log).reshape(NUM_GROUPS, PER_GROUP)
    skip_gain = d_skip.reshape(NUM_GROUPS, PER_GROUP)
    w_zx_flat = w_zx.reshape(D_MODEL, 2 * INNER_DIM)
    w_bc_flat = w_bc.reshape(D_MODEL, 2 * GROUP_WIDTH)
    norm_gain = norm_w.astype(jnp.float32)
    causal = jnp.arange(SSD_TILE)[:, None] >= jnp.arange(SSD_TILE)[None, :]

    def step(carry, inputs):
        xbc_tail, seg_tail, state = carry
        x_tile, seg_tile = inputs
        zx_proj = jnp.dot(x_tile, w_zx_flat, preferred_element_type=jnp.float32).astype(jnp.bfloat16)
        bc_pre = jnp.dot(x_tile, w_bc_flat, preferred_element_type=jnp.float32).astype(jnp.bfloat16)
        dt_raw = jnp.dot(x_tile, w_dt, preferred_element_type=jnp.float32).astype(jnp.bfloat16)
        xbc = jnp.concatenate([zx_proj[:, INNER_DIM:], bc_pre], axis=1)
        padded = jnp.concatenate([xbc_tail, xbc], axis=0).astype(jnp.float32)
        seg_pad = jnp.concatenate([seg_tail, seg_tile])
        conv_acc = conv_b
        for tap_idx in range(CONV_WIDTH):
            keep_tap = (seg_pad[tap_idx:tap_idx + SSD_TILE] == seg_tile)[:, None]
            conv_acc = conv_acc + jnp.where(keep_tap, padded[tap_idx:tap_idx + SSD_TILE] * conv_w[tap_idx], 0.0)
        conv_act = jax.nn.silu(conv_acc).astype(jnp.bfloat16).astype(jnp.float32)
        x_ssm = conv_act[:, :INNER_DIM].reshape(SSD_TILE, NUM_GROUPS, PER_GROUP, HEAD_DIM)
        b_ssm = conv_act[:, INNER_DIM:INNER_DIM + GROUP_WIDTH].reshape(SSD_TILE, NUM_GROUPS, STATE_DIM)
        c_ssm = conv_act[:, INNER_DIM + GROUP_WIDTH:].reshape(SSD_TILE, NUM_GROUPS, STATE_DIM)
        dt_val = jax.nn.softplus(dt_raw.astype(jnp.float32) + dt_bias).reshape(SSD_TILE, NUM_GROUPS, PER_GROUP)
        log_a = -decay_rate * dt_val
        seg_prev = seg_tail[halo_len - 1]
        cum_log = jnp.cumsum(log_a, axis=0)
        same_doc = ((seg_tile[:, None] == seg_tile[None, :]) & causal)[:, :, None, None]
        decay = jnp.where(same_doc, jnp.exp(jnp.where(same_doc, cum_log[:, None] - cum_log[None, :], 0.0)), 0.0)
        scores = jnp.einsum('tgn,sgn->tsg', c_ssm, b_ssm)
        mix_mat = scores[..., None] * decay * dt_val[None]
        y_ssm = jnp.einsum('tsgr,sgrp->tgrp', mix_mat, x_ssm)
        keep_in = (seg_tile == seg_prev)[:, None, None]
        y_ssm = y_ssm + jnp.einsum('tgn,grpn->tgrp', c_ssm, state) * jnp.where(keep_in, jnp.exp(cum_log), 0.0)[..., None]
        y_ssm = y_ssm + skip_gain[None, :, :, None] * x_ssm
        keep_end = (seg_tile == seg_tile[last_row])[:, None, None]
        end_w = jnp.where(keep_end, jnp.exp(cum_log[last_row][None] - cum_log), 0.0) * dt_val
        carry_fac = jnp.where(seg_tile[last_row] == seg_prev, jnp.exp(cum_log[last_row]), 0.0)
        state = carry_fac[:, :, None, None] * state + jnp.einsum('sgrp,sgn->grpn', x_ssm * end_w[..., None], b_ssm)
        gate_val = jax.nn.silu(zx_proj[:, :INNER_DIM].astype(jnp.float32))
        gated = (y_ssm.reshape(SSD_TILE, INNER_DIM) * gate_val).reshape(SSD_TILE, NUM_GROUPS, INNER_DIM // NUM_GROUPS)
        normed = gated * lax.rsqrt(jnp.mean(gated * gated, axis=-1, keepdims=True) + NORM_EPS)
        y_norm = (normed.reshape(SSD_TILE, INNER_DIM) * norm_gain).astype(jnp.bfloat16)
        out_proj = jnp.dot(y_norm, w_out, preferred_element_type=jnp.float32)
        y_tile = (x_tile.astype(jnp.float32) + out_proj).astype(jnp.bfloat16)
        return (xbc[SSD_TILE - halo_len:], seg_tile[SSD_TILE - halo_len:], state), y_tile

    init_carry = (jnp.zeros((halo_len, INNER_DIM + 2 * GROUP_WIDTH), jnp.bfloat16), jnp.zeros((halo_len,), jnp.int32), jnp.zeros((NUM_GROUPS, PER_GROUP, HEAD_DIM, STATE_DIM), jnp.float32))
    tiles_in = (x_in.reshape(n_tiles, SSD_TILE, D_MODEL), seg_ids.reshape(n_tiles, SSD_TILE))
    scan_out = lax.scan(step, init_carry, tiles_in)
    return scan_out[1].reshape(SEQ_LEN, D_MODEL)
```

```python
import functools
import jax
import jax.numpy as jnp
from jax import lax
from jax.experimental import pallas as pl
from jax.experimental.pallas import tpu as pltpu
from jax.sharding import PartitionSpec as P

MESH = pl.DeviceIdType.MESH
NORM_EPS = 1e-5
LOG2E = 1.4426950408889634
F32 = jnp.float32
BF16 = jnp.bfloat16
HI = lax.Precision.HIGHEST
NEG = -1e30


def silu(v):
    return v * (1.0 / (1.0 + jnp.exp(-v)))


def head_lanes(cols, tile_idx, head_dim, rows):
    per = 128 // head_dim
    lane = lax.broadcasted_iota(jnp.int32, (rows, 128), 1)
    out = jnp.broadcast_to(cols[:, tile_idx * per:tile_idx * per + 1], (rows, 128))
    for j in range(1, per):
        nxt = jnp.broadcast_to(cols[:, tile_idx * per + j:tile_idx * per + j + 1], (rows, 128))
        out = jnp.where(lane >= j * head_dim, nxt, out)
    return out


def expand_heads(row, head_dim):
    heads = row.shape[1]
    width = heads * head_dim
    eye = (lax.broadcasted_iota(jnp.int32, (heads, width), 1) // head_dim == lax.broadcasted_iota(jnp.int32, (heads, width), 0)).astype(F32)
    return jnp.dot(row, eye, precision=HI, preferred_element_type=F32)


def phase_a_kernel(q, heads, inner, gw, x_ref, bc_ref, dt_ref, seg_ref, tailx_ref, tailbc_ref, tailseg_ref, cw_ref, cb_ref, alog_ref, dtb_ref,
                   xact_ref, bcact_ref, cum_ref, cl_ref, sloc_ref, send_ref, dec_ref, pad, xw, state, segtail):
    c = pl.program_id(0)
    head_dim = inner // heads
    width = inner + gw

    @pl.when(c == 0)
    def _():
        pad[0:8, 0:inner] = tailx_ref[...].astype(F32)
        pad[0:8, inner:inner + gw // 2] = tailbc_ref[0].astype(F32)
        pad[0:8, inner + gw // 2:width] = tailbc_ref[1].astype(F32)
        segtail[...] = tailseg_ref[...]
        state[...] = jnp.zeros_like(state)
        dec_ref[...] = jnp.ones_like(dec_ref)

    @pl.when(c > 0)
    def _():
        pad[0:8, :] = pad[q:q + 8, :]

    pad[8:q + 8, 0:inner] = x_ref[0].astype(F32)
    pad[8:q + 8, inner:inner + gw // 2] = bc_ref[0].astype(F32)
    pad[8:q + 8, inner + gw // 2:width] = bc_ref[1].astype(F32)
    seg_row = seg_ref[...]
    prev_row = segtail[...]
    ext = jnp.concatenate([prev_row, seg_row], axis=1)
    segtail[...] = seg_row[:, q - 128:]
    seg_last = seg_row[:, q - 1:q]
    seg_prev = prev_row[:, 127:128]
    keeps = []
    for j in range(1, 4):
        shifted = ext[:, 128 - j:128 - j + q]
        keep_row = jnp.where(shifted == seg_row, 1.0, 0.0)
        keeps.append(jnp.broadcast_to(keep_row, (128, q)).T)
    for i in range(width // 128):
        cols = slice(i * 128, (i + 1) * 128)
        acc = cb_ref[0:1, cols] + pad[8:q + 8, cols] * cw_ref[3:4, cols]
        for j in range(1, 4):
            tap = pad[8 - j:q + 8 - j, cols] * cw_ref[3 - j:4 - j, cols]
            acc = acc + tap * keeps[j - 1]
        act = silu(acc).astype(BF16)
        if i * 128 < inner:
            xact_ref[:, cols] = act
        else:
            bcact_ref[:, i * 128 - inner:(i + 1) * 128 - inner] = act
    raw = dt_ref[...].astype(F32) + dtb_ref[...]
    dt = jnp.maximum(raw, 0.0) + jnp.log1p(jnp.exp(-jnp.abs(raw)))
    log_a = dt * (alog_ref[...] * LOG2E)
    tri = (lax.broadcasted_iota(jnp.int32, (q, q), 0) <= lax.broadcasted_iota(jnp.int32, (q, q), 1)).astype(F32)
    cum = jnp.dot(log_a, tri, precision=HI, preferred_element_type=F32)
    cl = cum - jnp.log(dt) * LOG2E
    cum_ref[...] = cum
    cl_ref[...] = cl
    cum_last = cum[:, q - 1:q]
    end_w = jnp.where(seg_row == seg_last, jnp.exp2(cum_last - cum), 0.0) * dt
    carry = jnp.where(seg_last == seg_prev, jnp.exp2(cum_last), 0.0)
    end_cols = end_w.T
    carry_lane = expand_heads(jnp.broadcast_to(carry, (heads, 128)).T[0:8, :], head_dim)[0:1, :]
    for i in range(inner // 128):
        cols = slice(i * 128, (i + 1) * 128)
        xw[:, cols] = (xact_ref[:, cols].astype(F32) * head_lanes(end_cols, i, head_dim, q)).astype(BF16)
    sloc_ref[0] = state[...]
    b_t = bcact_ref[:, 0:gw // 2].T
    new_state = carry_lane * state[...] + jnp.dot(b_t, xw[...], preferred_element_type=F32)
    state[...] = new_state
    send_ref[...] = new_state
    dec_ref[...] = dec_ref[...] * carry_lane


def phase_a(zx, bc_pre, dt_t, seg_row, tail_x, tail_bc, tail_seg, conv_w, conv_b, neg_a, dt_bias, q=256):
    _, t, inner = zx.shape
    gw = 2 * bc_pre.shape[2]
    heads = dt_t.shape[0]
    n_state = gw // 2
    nt = t // q
    width = inner + gw
    full = lambda shape: pl.BlockSpec(shape, lambda c: (0,) * len(shape))
    return pl.pallas_call(
        functools.partial(phase_a_kernel, q, heads, inner, gw),
        grid=(nt,),
        in_specs=[pl.BlockSpec((1, q, inner), lambda c: (1, c, 0)), pl.BlockSpec((2, q, gw // 2), lambda c: (0, c, 0)),
                  pl.BlockSpec((heads, q), lambda c: (0, c)), pl.BlockSpec((1, q), lambda c: (0, c)),
                  full((8, inner)), full((2, 8, gw // 2)), full((1, 128)), full((4, width)), full((1, width)), full((heads, 1)), full((heads, 1))],
        out_specs=[pl.BlockSpec((q, inner), lambda c: (c, 0)), pl.BlockSpec((q, gw), lambda c: (c, 0)),
                   pl.BlockSpec((heads, q), lambda c: (0, c)), pl.BlockSpec((heads, q), lambda c: (0, c)),
                   pl.BlockSpec((1, n_state, inner), lambda c: (c, 0, 0)), full((n_state, inner)), full((1, inner))],
        out_shape=[jax.ShapeDtypeStruct((t, inner), BF16), jax.ShapeDtypeStruct((t, gw), BF16),
                   jax.ShapeDtypeStruct((heads, t), F32), jax.ShapeDtypeStruct((heads, t), F32),
                   jax.ShapeDtypeStruct((nt, n_state, inner), F32), jax.ShapeDtypeStruct((n_state, inner), F32),
                   jax.ShapeDtypeStruct((1, inner), F32)],
        scratch_shapes=[pltpu.VMEM((q + 8, width), F32), pltpu.VMEM((q, inner), BF16), pltpu.VMEM((n_state, inner), F32), pltpu.VMEM((1, 128), F32)],
        compiler_params=pltpu.CompilerParams(dimension_semantics=("arbitrary",), vmem_limit_bytes=48 * 2**20),
        cost_estimate=pl.CostEstimate(flops=20 * 10**9, bytes_accessed=40 * 2**20, transcendentals=0),
        name="phase_a",
    )(zx, bc_pre, dt_t, seg_row, tail_x, tail_bc, tail_seg, conv_w, conv_b, neg_a, dt_bias)


def phase_b_kernel(q, heads, inner, gw, xact_ref, bc_ref, cum_ref, cl_ref, seg_ref, sloc_ref, sin_ref, z_ref, dskip_ref, nw_ref,
                   out_ref, pd, sbf, yoff, gated, segprev):
    c = pl.program_id(0)
    head_dim = inner // heads
    n_state = gw // 2
    half = q // 2

    @pl.when(c == 0)
    def _():
        pd[...] = jnp.ones_like(pd)
        segprev[...] = jnp.zeros_like(segprev)

    seg_row = seg_ref[...]
    seg_prev = segprev[:, 127:128]
    segprev[...] = seg_row[:, q - 128:]
    seg_last = seg_row[:, q - 1:q]
    seg_rows = jnp.broadcast_to(seg_row, (q, q))
    seg_cols = seg_rows.T
    causal = lax.broadcasted_iota(jnp.int32, (q, q), 0) >= lax.broadcasted_iota(jnp.int32, (q, q), 1)
    bias = jnp.where(causal & (seg_rows == seg_cols), 0.0, NEG)
    cum = cum_ref[...]
    cl = cl_ref[...]
    cum_cols = cum.T
    keep_in = jnp.where(seg_row == seg_prev, jnp.exp2(cum), 0.0)
    in_cols = keep_in.T
    carry = jnp.where(seg_last == seg_prev, jnp.exp2(cum[:, q - 1:q]), 0.0)
    carry_lane = expand_heads(jnp.broadcast_to(carry, (heads, 128)).T[0:8, :], head_dim)[0:1, :]
    sbf[...] = (sloc_ref[0] + pd[...] * sin_ref[...]).astype(BF16)
    pd[...] = pd[...] * carry_lane
    b_act = bc_ref[:, 0:n_state]
    c_act = bc_ref[:, n_state:gw]
    scores = lax.dot_general(c_act, b_act, (((1,), (1,)), ((), ())), preferred_element_type=F32)
    yoff[...] = jnp.dot(c_act, sbf[...], preferred_element_type=F32)
    lane = lax.broadcasted_iota(jnp.int32, (q, 128), 1)
    per = 128 // head_dim
    sq = jnp.zeros((q, 128), F32)
    for i in range(inner // 128):
        cols = slice(i * 128, (i + 1) * 128)
        x_b = xact_ref[:, cols]
        x_f = x_b.astype(F32)
        y_top = jnp.zeros((half, 128), F32)
        y_bot = jnp.zeros((half, 128), F32)
        for j in range(per):
            h = i * per + j
            x_h = jnp.where((lane >= j * head_dim) & (lane < (j + 1) * head_dim), x_f, 0.0).astype(BF16)
            ccol = cum_cols[:, h:h + 1]
            crow = cl[h:h + 1, :]
            m_top = jnp.exp2(ccol[0:half] + bias[0:half, 0:half] - crow[:, 0:half]) * scores[0:half, 0:half]
            m_bot = jnp.exp2(ccol[half:q] + bias[half:q, :] - crow) * scores[half:q, :]
            y_top = y_top + jnp.dot(m_top.astype(BF16), x_h[0:half], preferred_element_type=F32)
            y_bot = y_bot + jnp.dot(m_bot.astype(BF16), x_h, preferred_element_type=F32)
        y = jnp.concatenate([y_top, y_bot], axis=0)
        y = y + yoff[:, cols] * head_lanes(in_cols, i, head_dim, q)
        y = y + dskip_ref[0:1, cols] * x_f
        v = y * silu(z_ref[0, :, cols].astype(F32))
        gated[:, cols] = v
        sq = sq + v * v
    inv = lax.rsqrt(jnp.sum(sq, axis=1, keepdims=True) * (1.0 / inner) + NORM_EPS)
    inv = jnp.broadcast_to(inv, (q, 128))
    for i in range(inner // 128):
        cols = slice(i * 128, (i + 1) * 128)
        out_ref[:, cols] = (gated[:, cols] * inv * nw_ref[0:1, cols]).astype(BF16)


def phase_b(x_act, bc_act, cum, cl, seg_row, sloc, s_in, z_arr, dskip_lane, norm_w, q=256):
    t, inner = x_act.shape
    gw = bc_act.shape[1]
    heads = cum.shape[0]
    n_state = gw // 2
    nt = t // q
    full = lambda shape: pl.BlockSpec(shape, lambda c: (0,) * len(shape))
    return pl.pallas_call(
        functools.partial(phase_b_kernel, q, heads, inner, gw),
        grid=(nt,),
        in_specs=[pl.BlockSpec((q, inner), lambda c: (c, 0)), pl.BlockSpec((q, gw), lambda c: (c, 0)),
                  pl.BlockSpec((heads, q), lambda c: (0, c)), pl.BlockSpec((heads, q), lambda c: (0, c)),
                  pl.BlockSpec((1, q), lambda c: (0, c)), pl.BlockSpec((1, n_state, inner), lambda c: (c, 0, 0)),
                  full((n_state, inner)), pl.BlockSpec((1, q, inner), lambda c: (0, c, 0)), full((1, inner)), full((1, inner))],
        out_specs=pl.BlockSpec((q, inner), lambda c: (c, 0)),
        out_shape=jax.ShapeDtypeStruct((t, inner), BF16),
        scratch_shapes=[pltpu.VMEM((1, inner), F32), pltpu.VMEM((n_state, inner), BF16), pltpu.VMEM((q, inner), F32), pltpu.VMEM((q, inner), F32), pltpu.VMEM((1, 128), F32)],
        compiler_params=pltpu.CompilerParams(dimension_semantics=("arbitrary",), vmem_limit_bytes=48 * 2**20),
        cost_estimate=pl.CostEstimate(flops=20 * 10**9, bytes_accessed=40 * 2**20, transcendentals=0),
        name="phase_b",
    )(x_act, bc_act, cum, cl, seg_row, sloc, s_in, z_arr, dskip_lane, norm_w)


def out_kernel(chips, nb, wc, slots, v_ref, wo_ref, wp_ref, x_ref, o_ref,
               va_own, va_par, wbuf, send, recv, xo,
               vo_sem, vs_sem, vr_sem, w_sem, s_sem, r_sem, x_sem, o_sem):
    me = lax.axis_index('tp')
    chip = me // 2
    core = lax.rem(me, 2)
    partner = 2 * chip + 1 - core
    right = 2 * lax.rem(chip + 1, chips) + core
    left = 2 * lax.rem(chip + chips - 1, chips) + core
    rows = va_own.shape[1]
    half = nb * wc
    steps = chips * nb * 2

    barrier = pltpu.get_barrier_semaphore()
    for peer in (partner, left, right):
        pl.semaphore_signal(barrier, inc=1, device_id={'tp': peer}, device_id_type=MESH)

    def cols_of(u):
        return pl.multiple_of(lax.rem(u, 2) * half + lax.rem(u // 2, nb) * wc, wc)

    def w_copies(u, slot):
        col = cols_of(u)
        return (pltpu.make_async_copy(wo_ref.at[:, pl.ds(col, wc)], wbuf.at[slot, 0], w_sem.at[slot, 0]),
                pltpu.make_async_copy(wp_ref.at[:, pl.ds(col, wc)], wbuf.at[slot, 1], w_sem.at[slot, 1]))

    for cp in w_copies(0, 0):
        cp.start()
    x_copy = pltpu.make_async_copy(x_ref, xo, x_sem)
    order = [lax.rem(chip + d, chips) for d in (chips - 1, 1, 2, 0)]

    def own_copy(j):
        return pltpu.make_async_copy(v_ref.at[pl.ds(pl.multiple_of((2 * j + core) * rows, rows), rows), :], va_own.at[j], vo_sem.at[j])

    def par_copy(j):
        return pltpu.make_async_remote_copy(
            src_ref=v_ref.at[pl.ds(pl.multiple_of((2 * j + 1 - core) * rows, rows), rows), :], dst_ref=va_par.at[j],
            send_sem=vs_sem.at[j], recv_sem=vr_sem.at[j], device_id={'tp': partner}, device_id_type=MESH)

    for j in order:
        own_copy(j).start()
    pl.semaphore_wait(barrier, 3)
    for j in order:
        par_copy(j).start()
    x_copy.start()
    for j in order:
        own_copy(j).wait()

    def ring_copy(d, unit):
        slot = lax.rem(unit, slots)
        return pltpu.make_async_remote_copy(
            src_ref=send.at[d, slot], dst_ref=recv.at[d, unit], send_sem=s_sem.at[d, slot], recv_sem=r_sem.at[d, unit],
            device_id={'tp': jnp.where(d == 0, right, left)}, device_id_type=MESH)

    def body(u, carry):
        d = lax.rem(u, 2)
        k = u // (2 * nb)
        b = lax.rem(u // 2, nb)
        slot = lax.rem(u, 2)
        unit = k * nb + b
        dest = lax.rem(jnp.where(d == 0, chip + 2 * chips - 1 - k, chip + 1 + k), chips)
        for cp in w_copies(u, slot):
            cp.wait()

        @pl.when(u + 1 < steps)
        def _():
            for cp in w_copies(u + 1, 1 - slot):
                cp.start()

        @pl.when((b == 0) & ((k == 0) | ((d == 0) & ((k == 1) | (k == 3)))))
        def _():
            par_copy(dest).wait_recv()

        part = jnp.dot(va_own[dest], wbuf[slot, 0], preferred_element_type=F32)
        part = part + jnp.dot(va_par[dest], wbuf[slot, 1], preferred_element_type=F32)

        @pl.when(k < chips - 1)
        def _():
            sslot = lax.rem(unit, slots)

            @pl.when(unit >= slots)
            def _():
                ring_copy(d, unit - slots).wait_send()

            @pl.when(k == 0)
            def _():
                send[d, sslot] = part

            @pl.when(k > 0)
            def _():
                ring_copy(d, unit - nb).wait_recv()
                send[d, sslot] = part + recv[d, unit - nb]
            ring_copy(d, unit).start()

        @pl.when(k == chips - 1)
        def _():
            @pl.when((b == 0) & (d == 0))
            def _():
                x_copy.wait()
            ring_copy(d, unit - nb).wait_recv()
            cols = pl.ds(cols_of(u), wc)
            xo[:, cols] = (xo[:, cols].astype(F32) + (part + recv[d, unit - nb])).astype(BF16)
            pltpu.make_async_copy(xo.at[:, cols], o_ref.at[:, cols], o_sem.at[d, b]).start()
        return carry

    lax.fori_loop(0, steps, body, 0)

    def drain_out(u, carry):
        d = lax.rem(u, 2)
        b = u // 2
        cols = pl.ds(pl.multiple_of(d * half + b * wc, wc), wc)
        pltpu.make_async_copy(xo.at[:, cols], o_ref.at[:, cols], o_sem.at[d, b]).wait()
        return carry

    def drain_send(u, carry):
        ring_copy(lax.rem(u, 2), (chips - 1) * nb - slots + u // 2).wait_send()
        return carry

    lax.fori_loop(0, 2 * slots, drain_send, 0)
    for j in order:
        par_copy(j).wait_send()
    lax.fori_loop(0, 2 * nb, drain_out, 0)


def out_proj_scatter(v, w_own, w_par, x_loc, chips, wc=512, slots=4):
    t, inner = v.shape
    rows, d_model = x_loc.shape
    nb = d_model // 2 // wc
    any_spec = pl.BlockSpec(memory_space=pl.ANY)
    dma = pltpu.SemaphoreType.DMA
    return pl.pallas_call(
        functools.partial(out_kernel, chips, nb, wc, slots),
        in_specs=[any_spec] * 4,
        out_specs=any_spec,
        out_shape=jax.ShapeDtypeStruct((rows, d_model), BF16),
        scratch_shapes=[pltpu.VMEM((chips, rows, inner), BF16), pltpu.VMEM((chips, rows, inner), BF16), pltpu.VMEM((2, 2, inner, wc), BF16),
                        pltpu.VMEM((2, slots, rows, wc), F32), pltpu.VMEM((2, (chips - 1) * nb, rows, wc), F32), pltpu.VMEM((rows, d_model), BF16),
                        dma((chips,)), dma((chips,)), dma((chips,)), dma((2, 2)), dma((2, slots)), dma((2, (chips - 1) * nb)), dma, dma((2, nb))],
        compiler_params=pltpu.CompilerParams(collective_id=1, has_side_effects=True, vmem_limit_bytes=60 * 2**20),
        cost_estimate=pl.CostEstimate(flops=2 * t * inner * d_model, bytes_accessed=300 * 2**20, transcendentals=0),
        name="out_proj_scatter",
    )(v, w_own, w_par, x_loc)


def chain_state(end_state, block_decay, seq_axis, n_blocks):
    dev_index = lax.axis_index(seq_axis)
    to_next = [(src_dev, src_dev + 1) for src_dev in range(n_blocks - 1)]
    state_in = lax.ppermute(end_state, seq_axis, to_next)
    decay_in = jnp.where(dev_index == 0, 1.0, lax.ppermute(block_decay, seq_axis, to_next))
    for step_idx in range((n_blocks - 1).bit_length()):
        hop_span = 2 ** step_idx
        hop_perm = [(src_dev, src_dev + hop_span) for src_dev in range(n_blocks - hop_span)]
        prev_state = lax.ppermute(state_in, seq_axis, hop_perm)
        prev_decay = lax.ppermute(decay_in, seq_axis, hop_perm)
        has_prev = dev_index >= hop_span
        state_in = jnp.where(has_prev, decay_in * prev_state + state_in, state_in)
        decay_in = jnp.where(has_prev, decay_in * prev_decay, decay_in)
    return state_in


def local_layer(x_loc, x_blk, seg_blk, w_out_par, weights, n_blocks, chips):
    w_zx, w_bc, w_dt, conv_x, conv_bc, bias_x, bias_bc, a_log, dt_bias, d_skip, norm_w, w_out = weights
    t = x_blk.shape[0]
    inner = w_zx.shape[2]
    n_state = w_bc.shape[2]
    heads = w_dt.shape[1]
    head_dim = inner // heads
    zx = jnp.einsum('ld,dkc->klc', x_blk, w_zx, preferred_element_type=F32).astype(BF16)
    bc_pre = jnp.einsum('ld,dkc->klc', x_blk, w_bc, preferred_element_type=F32).astype(BF16)
    dt_t = jnp.einsum('ld,dh->hl', x_blk, w_dt, preferred_element_type=F32).astype(BF16)
    to_next = [(src, src + 1) for src in range(n_blocks - 1)]
    tail_x = lax.ppermute(zx[1, t - 8:], 'sp', to_next)
    tail_bc = lax.ppermute(bc_pre[:, t - 8:], 'sp', to_next)
    tail_seg = lax.ppermute(seg_blk[t - 8:], 'sp', to_next)
    seg_prev = jnp.where(lax.axis_index('sp') == 0, seg_blk[0], tail_seg[7])
    seg_row = (seg_blk - seg_prev).astype(F32)[None]
    tail_row = jnp.pad((tail_seg - seg_prev).astype(F32), (120, 0), constant_values=-1e6)[None]
    conv_w = jnp.concatenate([conv_x, conv_bc.reshape(conv_bc.shape[0], 2 * n_state)], axis=1).astype(F32)
    conv_b = jnp.concatenate([bias_x, bias_bc.reshape(2 * n_state)]).astype(F32)[None]
    x_act, bc_act, cum, cl, sloc, s_end, dec = phase_a(zx, bc_pre, dt_t, seg_row, tail_x, tail_bc, tail_row, conv_w, conv_b, -jnp.exp(a_log)[:, None], dt_bias[:, None])
    s_in = chain_state(s_end, dec, 'sp', n_blocks)
    v = phase_b(x_act, bc_act, cum, cl, seg_row, sloc, s_in, zx, jnp.repeat(d_skip, head_dim)[None], norm_w.astype(F32)[None])
    return out_proj_scatter(v, w_out, w_out_par, x_loc, chips)


def solution(mesh):
    n_blocks = mesh.shape['sp']
    n_tp = mesh.shape['tp']
    token_spec = P(('dp', 'sp', 'tp'), None)
    seg_spec = P(('dp', 'sp', 'tp'))
    weight_specs = (P(None, None, 'tp'), P(None, None, 'tp'), P(None, 'tp'), P(None, 'tp'), P(None, None, 'tp'), P('tp'), P(None, 'tp'), P('tp'), P('tp'), P('tp'), P('tp'), P('tp', None))

    def body(x_loc, seg_loc, *weights):
        w_out_par = lax.ppermute(weights[-1], 'tp', [(i, i ^ 1) for i in range(n_tp)])
        x_blk = lax.all_gather(x_loc, 'tp', axis=0, tiled=True)
        seg_blk = lax.all_gather(seg_loc, 'tp', axis=0, tiled=True)
        return local_layer(x_loc, x_blk, seg_blk, w_out_par, weights, n_blocks, n_tp // 2)

    return jax.shard_map(body, mesh=mesh, in_specs=(token_spec, seg_spec) + weight_specs, out_specs=token_spec, check_vma=False)
```

```python
import functools
import jax
import jax.numpy as jnp
from jax import lax
from jax.experimental import pallas as pl
from jax.experimental.pallas import tpu as pltpu
from jax.sharding import PartitionSpec as P

MESH = pl.DeviceIdType.MESH
NORM_EPS = 1e-5
LOG2E = 1.4426950408889634
FAR = -1e6
NEG = -1e30
F32 = jnp.float32
BF16 = jnp.bfloat16
HI = lax.Precision.HIGHEST
MIB = 2 ** 20
LANES = 128
ROW8 = 8
CORES = 2
PAIR = range(2)
ANY = pl.BlockSpec(memory_space=pl.ANY)
VMEM = pl.BlockSpec(memory_space=pltpu.VMEM)
DMA = pltpu.SemaphoreType.DMA


def scratch(dtype, *shape):
    return pltpu.VMEM(shape, dtype)


def out_of(dtype, *shape):
    return jax.ShapeDtypeStruct(shape, dtype)


def sems(*shape):
    return DMA(shape)


def rows_at(start, size):
    return pl.ds(pl.multiple_of(start, size), size)


def odd(i):
    return lax.rem(i, 2)


def flip(i):
    return 1 - i


def dot32(a, b):
    return jnp.dot(a, b, preferred_element_type=F32)


def params(limit, name_id=None):
    if name_id is None:
        return pltpu.CompilerParams(dimension_semantics=('arbitrary',), vmem_limit_bytes=limit * MIB)
    return pltpu.CompilerParams(collective_id=name_id, has_side_effects=True, vmem_limit_bytes=limit * MIB)


def greet(peers):
    barrier = pltpu.get_barrier_semaphore()
    for axis, index in peers:
        pl.semaphore_signal(barrier, inc=1, device_id={axis: index}, device_id_type=MESH)
    return lambda: pl.semaphore_wait(barrier, len(peers))


def remote(src, dst, send, recv, axis, index):
    return pltpu.make_async_remote_copy(src_ref=src, dst_ref=dst, send_sem=send, recv_sem=recv, device_id={axis: index}, device_id_type=MESH)


def silu(v):
    return v * (1.0 / (1.0 + jnp.exp(-v)))


def head_lanes(cols, tile_idx, head_dim):
    rows = cols.shape[0]
    per = LANES // head_dim
    lane = lax.broadcasted_iota(jnp.int32, (rows, LANES), 1)
    out = None
    for j in range(per):
        h = tile_idx * per + j
        nxt = jnp.broadcast_to(cols[:, h:h + 1], (rows, LANES))
        out = nxt if out is None else jnp.where(lane >= j * head_dim, nxt, out)
    return out


def expand_heads(row, head_dim):
    heads = row.shape[1]
    shape = (heads, heads * head_dim)
    eye = (lax.broadcasted_iota(jnp.int32, shape, 1) // head_dim == lax.broadcasted_iota(jnp.int32, shape, 0)).astype(F32)
    return jnp.dot(jnp.broadcast_to(row, (ROW8, heads)), eye, precision=HI, preferred_element_type=F32)[0:1]


def column(row):
    return jnp.broadcast_to(row, (LANES, row.shape[1])).T[:, 0:1]


def gather_kernel(chips, blocks, kb, nb, sub, nt, pace, x_ref, wzx_ref, wbc_ref, wdt_ref, wo_ref, seg_ref,
                  xf_ref, xp_ref, bp_ref, wz_ref, wp_ref, segf_ref, segt_ref, tx_ref, tb_ref,
                  wx, wsm, xg, ost, bst, blk, bblk, zst, wdt,
                  ra_sem, rd_sem, so_sem, sf_sem, sd_sem, xl_sem, xs_sem, in_sem, zo_sem, bb_sem, dt_sem, oo_sem, bo_sem,
                  wp_sem, sg_sem, sr_sem, st_sem, hx_sem, hb_sem):
    me = lax.axis_index('tp')
    blk_id = lax.axis_index('sp')
    chip, core = me // CORES, odd(me)
    partner = CORES * chip + flip(core)
    near = [lax.rem(chip + chips - 1, chips), lax.rem(chip + 1, chips)]
    far = lax.rem(chip + chips // 2, chips)
    ring = [CORES * c + core for c in near]
    sp_next = lax.rem(blk_id + 1, blocks)
    n_tp = CORES * chips
    rows = x_ref.shape[0]
    quarters = xl_sem.shape[1]
    qr = rows // quarters
    d_model, inner = wx.shape
    heads = wdt.shape[0]
    n_state = bblk.shape[3]
    nk = d_model // kb
    nblk = nk * (inner // nb)
    opp = 2 + quarters
    last = opp + quarters // 2 - 1
    ready = greet([('tp', lax.rem(me + d, n_tp)) for d in range(1, n_tp)] + [('sp', sp_next), ('sp', lax.rem(blk_id + blocks - 1, blocks))])

    def row_of(lv, b):
        side = odd(b)
        other = jnp.where(lv < 2, lv, b // 2)
        cc = jnp.where(other == 1, flip(core), core)
        ch = jnp.where(lv < 2, chip, jnp.where(lv >= opp, far, jnp.where(side == 0, near[0], near[1])))
        q = jnp.where(lv < 2, b, jnp.where(lv >= opp, side * (quarters // 2) + lv - opp, lv - 2))
        return (CORES * ch + cc) * rows + q * qr

    def full_rows(lv, b, size=qr):
        return xf_ref.at[rows_at(row_of(lv, b), size), :]

    def w_tile(i):
        return rows_at(lax.rem(i, nk) * kb, kb), rows_at((i // nk) * nb, nb)

    def blk_copy(i):
        kk, nn = w_tile(i)
        slot = lax.rem(i, blk.shape[0])
        return pltpu.make_async_copy(wzx_ref.at[kk, :, nn], blk.at[slot], in_sem.at[slot])

    def z_copy(i):
        kk, nn = w_tile(i)
        return pltpu.make_async_copy(zst.at[odd(i)], wz_ref.at[kk, nn], zo_sem.at[odd(i)])

    def bc_copy(i):
        return pltpu.make_async_copy(wbc_ref.at[rows_at(i * kb, kb)], bblk.at[odd(i)], bb_sem.at[odd(i)])

    own_load = pltpu.make_async_copy(x_ref, xg.at[0], xs_sem.at[0])
    dt_load = pltpu.make_async_copy(wdt_ref, wdt, dt_sem)
    own_load.start()
    dt_load.start()
    bc_copy(0).start()
    for i in range(blk.shape[0]):
        blk_copy(i).start()
    ready()

    def own_send(q, to):
        return remote(x_ref.at[rows_at(q * qr, qr), :], full_rows(0, q), so_sem.at[to, q], ra_sem.at[2 + q, flip(to)], 'tp', ring[to])

    own_pair = remote(x_ref, full_rows(0, 0, rows), sd_sem.at[1, 0], rd_sem.at[1, 0], 'tp', partner)

    def pair_send(lv, side):
        return remote(full_rows(lv, side), full_rows(lv, side), sd_sem.at[lv, side], rd_sem.at[lv, side], 'tp', partner)

    def forward(lv, to):
        side = flip(to)
        h = lax.rem(lv - 2, quarters // 2)
        dst_sem = ra_sem.at[opp + h, side]
        return remote(full_rows(lv, side), full_rows(lv, side), sf_sem.at[to, h], dst_sem, 'tp', ring[to])

    def arrival(lv, side):
        return remote(full_rows(lv, side), full_rows(lv, side), so_sem.at[0, 0], ra_sem.at[lv, side], 'tp', ring[0])

    def pair_arrival(lv, side):
        ref = full_rows(lv, 2 + side)
        return remote(ref, ref, sd_sem.at[1, 0], rd_sem.at[lv, side], 'tp', partner)

    pair_own_arrival = remote(full_rows(1, 0, rows), full_rows(1, 0, rows), sd_sem.at[1, 0], rd_sem.at[1, 0], 'tp', partner)

    def send_quarter(q):
        for to in PAIR:
            own_send(q, flip(to)).start()
    send_quarter(0)
    own_pair.start()

    def seg_cols(index):
        return segf_ref.at[:, rows_at(index * rows, rows)]

    def seg_send(d):
        return remote(seg_ref, seg_cols(me), sg_sem.at[d], sr_sem.at[d], 'tp', lax.rem(me + d, n_tp))

    def seg_arrival(d):
        return remote(seg_ref, seg_cols(lax.rem(me + n_tp - d, n_tp)), sg_sem.at[d], sr_sem.at[d], 'tp', lax.rem(me + d, n_tp))

    seg_own = pltpu.make_async_copy(seg_ref, seg_cols(me), sg_sem.at[0])
    seg_own.start()
    for d in range(1, n_tp):
        seg_send(d).start()
    w_swap = remote(wo_ref, wp_ref, wp_sem.at[0], wp_sem.at[1], 'tp', partner)
    w_swap.start()
    seg_halo = remote(segf_ref.at[:, pl.ds(n_tp * rows - LANES, LANES)], segt_ref, st_sem.at[0], st_sem.at[1], 'sp', sp_next)

    end_chip = chips - 1
    hrows = tx_ref.shape[0]
    halo_lv = jnp.where(chip == end_chip, flip(core), jnp.where(far == end_chip, last, opp - 1))
    halo_b = jnp.where(chip == end_chip, quarters - 1, jnp.where((far != end_chip) & (near[0] == end_chip), 0, 1) + CORES * flip(core))

    def halo_copies(slot):
        src = rows_at(halo_b * qr + qr - hrows, hrows)
        return [remote(ost.at[slot, src, :], tx_ref, hx_sem.at[0], hx_sem.at[1], 'sp', sp_next),
                remote(bst.at[slot, src, :], tb_ref, hb_sem.at[0], hb_sem.at[1], 'sp', sp_next)]

    dt_load.wait()

    def small_body(i, carry):
        bc_copy(i).wait()

        @pl.when(i + 1 < nk)
        def _():
            bc_copy(i + 1).start()

        def inner_body(s, carry2):
            part = jnp.swapaxes(bblk[odd(i), rows_at(s * sub, sub)], 0, 1)
            at = rows_at(i * kb + s * sub, sub)
            for g in PAIR:
                wsm[at, g * n_state:(g + 1) * n_state] = part[g]
            wd = jnp.concatenate([wdt[:, at].astype(F32), jnp.zeros((LANES - heads, sub), F32)], axis=0)
            wsm[at, 2 * n_state:] = wd.T.astype(BF16)
            return carry2
        return lax.fori_loop(0, kb // sub, inner_body, carry)
    lax.fori_loop(0, nk, small_body, 0)

    def relay(i, carry):
        slot = lax.rem(i, blk.shape[0])
        blk_copy(i).wait()

        @pl.when(i >= 2)
        def _():
            z_copy(i - 2).wait()
        kk = lax.rem(i, nk) * kb

        def inner_body(s, carry2):
            at = rows_at(s * sub, sub)
            part = jnp.swapaxes(blk[slot, at].astype(F32), 0, 1)
            zst[odd(i), at, :] = part[0].astype(BF16)
            wx[rows_at(kk + s * sub, sub), w_tile(i)[1]] = part[1].astype(BF16)
            return carry2
        lax.fori_loop(0, kb // sub, inner_body, 0)
        z_copy(i).start()
        for q in range(1, quarters - 1):
            pl.when(i == q * pace - 1)(functools.partial(send_quarter, q))

        @pl.when(i + blk.shape[0] < nblk)
        def _():
            blk_copy(i + blk.shape[0]).start()
        return carry
    lax.fori_loop(0, nblk, relay, 0)

    seg_own.wait()
    for d in range(1, n_tp):
        seg_arrival(d).wait_recv()
    seg_halo.start()
    own_load.wait()
    own_store = pltpu.make_async_copy(xg.at[0], full_rows(0, 0, rows), xs_sem.at[1])
    own_store.start()

    def load(lv, b):
        return pltpu.make_async_copy(full_rows(lv, b), xg.at[odd(lv), rows_at(b * qr, qr), :], xl_sem.at[odd(lv), b])

    def take(lv):
        @pl.when(lv >= 2)
        def _():
            for side in PAIR:
                arrival(lv, side).wait_recv()
                pair_send(lv, side).start()

    def fetch(lv):
        @pl.when(lv == 1)
        def _():
            pair_own_arrival.wait_recv()

        @pl.when(lv >= 2)
        def _():
            for side in PAIR:
                pair_arrival(lv, side).wait_recv()
        for b in range(quarters):
            load(lv, b).start()

    def out_copies(lv):
        slot = odd(lv)
        res = []
        for b in range(quarters):
            src, dst = rows_at(b * qr, qr), rows_at(row_of(lv, b), qr)
            res.append(pltpu.make_async_copy(ost.at[slot, src, :], xp_ref.at[dst, :], oo_sem.at[slot, b]))
            res.append(pltpu.make_async_copy(bst.at[slot, src, :], bp_ref.at[dst, :], bo_sem.at[slot, b]))
        return res

    early = opp - 1
    cut = 2 + quarters // 2

    def feed(lv):
        @pl.when(lv == 1)
        def _():
            send_quarter(quarters - 1)
        for h in range(quarters // 2):
            @pl.when(lv == 3 + 2 * h)
            def _(h=h):
                forward(2 + h, 1).start()
                forward(cut + h, 0).start()

    def round_body(lv, carry):
        slot = odd(lv)

        @pl.when(lv > 0)
        def _():
            for b in range(quarters):
                load(lv, b).wait()

        @pl.when(lv == 1)
        def _():
            own_store.wait()

        @pl.when(lv < early)
        def _():
            take(lv + 1)

        @pl.when(lv >= 2)
        def _():
            for cp in out_copies(lv - 2):
                cp.wait()

        def dots(n, carry2):
            @pl.when(n == inner // nt // 2)
            def _():
                feed(lv)

                @pl.when(lv < early)
                def _():
                    fetch(lv + 1)
            cols = rows_at(n * nt, nt)
            ost[slot, :, cols] = dot32(xg[slot], wx[:, cols]).astype(BF16)
            return carry2
        lax.fori_loop(0, inner // nt, dots, 0)
        bst[slot] = dot32(xg[slot], wsm[...]).astype(BF16)
        for cp in out_copies(lv):
            cp.start()

        @pl.when(lv == halo_lv + 1)
        def _():
            for cp in halo_copies(flip(slot)):
                cp.wait_send()

        @pl.when(lv == halo_lv)
        def _():
            for cp in halo_copies(slot):
                cp.start()

        @pl.when((lv >= early) & (lv < last))
        def _():
            take(lv + 1)
            fetch(lv + 1)
        return carry
    lax.fori_loop(0, last + 1, round_body, 0)

    @pl.when(halo_lv == last)
    def _():
        for cp in halo_copies(last % 2):
            cp.wait_send()
    for cp in halo_copies(0):
        cp.wait_recv()
    seg_halo.wait()
    for d in range(1, n_tp):
        seg_send(d).wait_send()
    w_swap.wait()
    for i in PAIR:
        for cp in out_copies(last - i):
            cp.wait()
        z_copy(nblk - 1 - i).wait()
    own_pair.wait_send()
    for to in PAIR:
        for q in range(quarters):
            own_send(q, to).wait_send()
        for h in range(quarters // 2):
            forward(2 + h, to).wait_send()
    for lv in range(2, last + 1):
        for side in PAIR:
            pair_send(lv, side).wait_send()


def gather_proj(x_loc, w_zx, w_bc, w_dt_t, w_out, seg, chips, blocks, kb=2048, nb=256, sub=256, nt=512, quarters=4, pace=12):
    rows, d_model = x_loc.shape
    inner, n_state, heads = w_zx.shape[2], w_bc.shape[2], w_dt_t.shape[0]
    n_tp = CORES * chips
    t = rows * n_tp
    small = CORES * n_state + LANES
    lv = CORES + quarters + quarters // 2
    halo = 16
    two = sems(2)
    return pl.pallas_call(
        functools.partial(gather_kernel, chips, blocks, kb, nb, sub, nt, pace),
        in_specs=[ANY] * 6,
        out_specs=[ANY] * 9,
        out_shape=[out_of(BF16, t, d_model), out_of(BF16, t, inner), out_of(BF16, t, small), out_of(BF16, d_model, inner), out_of(BF16, *w_out.shape),
                   out_of(jnp.int32, 1, t), out_of(jnp.int32, 1, LANES), out_of(BF16, halo, inner), out_of(BF16, halo, small)],
        scratch_shapes=[scratch(BF16, d_model, inner), scratch(BF16, d_model, small), scratch(BF16, 2, rows, d_model),
                        scratch(BF16, 2, rows, inner), scratch(BF16, 2, rows, small), scratch(BF16, 3, kb, CORES, nb),
                        scratch(BF16, 2, kb, CORES, n_state), scratch(BF16, 2, kb, nb), scratch(BF16, heads, d_model),
                        sems(lv, 2), sems(lv, 2), sems(2, quarters), sems(2, quarters), sems(lv, 2), sems(2, quarters), two, sems(3), two, two, DMA,
                        sems(2, quarters), sems(2, quarters), two, sems(n_tp), sems(n_tp), two, two, two],
        compiler_params=params(63, 0),
        cost_estimate=pl.CostEstimate(flops=t * inner * d_model, bytes_accessed=t * inner, transcendentals=0),
        name='gather_proj',
    )(x_loc, w_zx, w_bc, w_dt_t, w_out, seg)


def phase_a_kernel(q, x_ref, small_ref, seg_ref, segt_ref, tailx_ref, tailb_ref, cx_ref, cbc_ref, bx_ref, bbc_ref, alog_ref, dtb_ref,
                   xact_ref, bcact_ref, cum_ref, cl_ref, segf_ref, segp_ref, sloc_ref, pd_ref, send_ref, dec_ref,
                   pad, xw, state, segtail, base, cw):
    inner = x_ref.shape[1]
    gw = bcact_ref.shape[1]
    n_state = gw // 2
    heads = alog_ref.shape[1]
    head_dim = inner // heads
    taps = cx_ref.shape[0]

    @pl.when(pl.program_id(0) == 0)
    def _():
        first = lax.axis_index('sp') == 0
        base[...] = jnp.broadcast_to(jnp.where(first, seg_ref[:, 0:1], segt_ref[:, LANES - 1:]), base.shape)
        segtail[...] = jnp.where(first, FAR, (segt_ref[...] - base[...]).astype(F32))
        pad[0:ROW8, 0:inner] = tailx_ref[...].astype(F32)[ROW8:]
        pad[0:ROW8, inner:] = tailb_ref[:, 0:gw].astype(F32)[ROW8:]
        cw[0:taps, 0:inner] = cx_ref[...].astype(F32)
        cw[taps:taps + 1, 0:inner] = bx_ref[...].astype(F32)
        for g in PAIR:
            cols = slice(inner + g * n_state, inner + (g + 1) * n_state)
            cw[0:taps, cols] = cbc_ref[:, g, :].astype(F32)
            cw[taps:taps + 1, cols] = bbc_ref[g:g + 1, :].astype(F32)
        state[...] = jnp.zeros_like(state)
        dec_ref[...] = jnp.ones_like(dec_ref)

    @pl.when(pl.program_id(0) > 0)
    def _():
        pad[0:ROW8, :] = pad[q:q + ROW8, :]

    pad[ROW8:, 0:inner] = x_ref[...].astype(F32)
    pad[ROW8:, inner:] = small_ref[:, 0:gw].astype(F32)
    seg_row = (seg_ref[...] - base[:, 0:1]).astype(F32)
    prev_row = segtail[...]
    segf_ref[...] = seg_row
    segp_ref[0] = prev_row
    segtail[...] = seg_row[:, q - LANES:]
    ext = jnp.concatenate([prev_row, seg_row], axis=1)
    seg_last, seg_prev = seg_row[:, q - 1:], prev_row[:, LANES - 1:]
    keeps = []
    for j in range(1, taps):
        keep_row = jnp.where(ext[:, LANES - j:LANES - j + q] == seg_row, 1.0, 0.0)
        keeps.append(jnp.broadcast_to(keep_row, (LANES, q)).T)
    for i in range((inner + gw) // LANES):
        cols = slice(i * LANES, (i + 1) * LANES)
        acc = cw[taps:taps + 1, cols] + pad[ROW8:, cols] * cw[taps - 1:taps, cols]
        for j in range(1, taps):
            at = taps - 1 - j
            acc = acc + pad[ROW8 - j:q + ROW8 - j, cols] * cw[at:at + 1, cols] * keeps[j - 1]
        act = silu(acc).astype(BF16)
        if i * LANES < inner:
            xact_ref[:, cols] = act
        else:
            bcact_ref[:, i * LANES - inner:(i + 1) * LANES - inner] = act
    raw = small_ref[:, gw:].astype(F32).T[0:heads] + column(dtb_ref[...])
    dt = jnp.maximum(raw, 0.0) + jnp.log1p(jnp.exp(-jnp.abs(raw)))
    log_a = dt * column(jnp.exp(alog_ref[...]) * -LOG2E)
    tri = (lax.broadcasted_iota(jnp.int32, (q, q), 0) <= lax.broadcasted_iota(jnp.int32, (q, q), 1)).astype(F32)
    cum = jnp.dot(log_a, tri, precision=HI, preferred_element_type=F32)
    cum_ref[...] = cum
    cl_ref[...] = cum - jnp.log(dt) * LOG2E
    cum_last = cum[:, q - 1:]
    end_cols = (jnp.where(seg_row == seg_last, jnp.exp2(cum_last - cum), 0.0) * dt).T
    carry = jnp.where(seg_last == seg_prev, jnp.exp2(cum_last), 0.0)
    carry_lane = expand_heads(jnp.broadcast_to(carry, (heads, LANES)).T[0:1], head_dim)
    for i in range(inner // LANES):
        cols = slice(i * LANES, (i + 1) * LANES)
        xw[:, cols] = (xact_ref[:, cols].astype(F32) * head_lanes(end_cols, i, head_dim)).astype(BF16)
    sloc_ref[0] = state[...]
    pd_ref[0] = dec_ref[...]
    new_state = carry_lane * state[...] + dot32(bcact_ref[:, 0:n_state].T, xw[...])
    state[...] = new_state
    send_ref[...] = new_state
    dec_ref[...] = dec_ref[...] * carry_lane


def phase_a(x_pre, small, seg, seg_tail, tail_x, tail_b, conv_x, conv_bc, bias_x, bias_bc, a_log, dt_bias, q):
    t, inner = x_pre.shape
    n_state = conv_bc.shape[2]
    gw = CORES * n_state
    heads = a_log.shape[1]
    nt = t // q

    def full(shape):
        return pl.BlockSpec(shape, lambda c: (0,) * len(shape))

    def by_row(width):
        return pl.BlockSpec((q, width), lambda c: (c, 0))

    def by_col(height):
        return pl.BlockSpec((height, q), lambda c: (0, c))

    def by_chunk(a, b):
        return pl.BlockSpec((1, a, b), lambda c: (c, 0, 0))

    rest = (seg_tail, tail_x, tail_b, conv_x, conv_bc, bias_x, bias_bc, a_log, dt_bias)
    return pl.pallas_call(
        functools.partial(phase_a_kernel, q),
        grid=(nt,),
        in_specs=[by_row(inner), by_row(small.shape[1]), by_col(1)] + [full(v.shape) for v in rest],
        out_specs=[by_row(inner), by_row(gw), by_col(heads), by_col(heads), by_col(1), by_chunk(1, LANES), by_chunk(n_state, inner), by_chunk(1, inner),
                   full((n_state, inner)), full((1, inner))],
        out_shape=[out_of(BF16, t, inner), out_of(BF16, t, gw), out_of(F32, heads, t), out_of(F32, heads, t), out_of(F32, 1, t), out_of(F32, nt, 1, LANES),
                   out_of(F32, nt, n_state, inner), out_of(F32, nt, 1, inner), out_of(F32, n_state, inner), out_of(F32, 1, inner)],
        scratch_shapes=[scratch(F32, q + ROW8, inner + gw), scratch(BF16, q, inner), scratch(F32, n_state, inner), scratch(F32, 1, LANES),
                        scratch(jnp.int32, 1, LANES), scratch(F32, ROW8, inner + gw)],
        compiler_params=params(56),
        cost_estimate=pl.CostEstimate(flops=t * inner * gw, bytes_accessed=t * inner, transcendentals=0),
        name='phase_a',
    )(x_pre, small, seg, *rest)


def chain_kernel(chips, blocks, pieces, hop, nt, xf_ref, wz_ref, send_ref, dec_ref, z_ref, sin_ref,
                 xg, wzb, zst, sbuf, rbuf, x_sem, w_sem, z_sem, s_sem, r_sem):
    chip = lax.axis_index('tp') // CORES
    blk_id = lax.axis_index('sp')
    sp_next = lax.rem(blk_id + 1, blocks)
    ready = greet([('sp', sp_next), ('sp', lax.rem(blk_id + blocks - 1, blocks))])
    n_state, inner = send_ref.shape
    tm = xg.shape[1]
    nn = inner // nt
    tiles = CORES * nn
    pw = inner // pieces

    def tok(g):
        return rows_at(lax.rem(chip + jnp.where(g == 0, chips - 1, 1), chips) * tm, tm)

    def col(i):
        return rows_at(lax.rem(i, nn) * nt, nt)

    def x_copy(g):
        return pltpu.make_async_copy(xf_ref.at[tok(g), :], xg.at[g], x_sem.at[g])

    def w_copy(i):
        return pltpu.make_async_copy(wz_ref.at[:, col(i)], wzb.at[odd(i)], w_sem.at[odd(i)])

    def z_copy(i):
        return pltpu.make_async_copy(zst.at[odd(i)], z_ref.at[tok(i // nn), col(i)], z_sem.at[odd(i)])

    def hop_copy(p):
        return remote(sbuf.at[p], rbuf.at[p], s_sem.at[p], r_sem.at[p], 'sp', sp_next)

    for g in PAIR:
        x_copy(g).start()
    w_copy(0).start()
    ready()

    def body(i, carry):
        p = i - hop * blk_id

        @pl.when((p >= 0) & (p < pieces))
        def _():
            cols = rows_at(p * pw, pw)

            @pl.when(blk_id == 0)
            def _():
                sbuf[p] = send_ref[:, cols]
                sin_ref[:, cols] = jnp.zeros((n_state, pw), F32)

            @pl.when(blk_id > 0)
            def _():
                hop_copy(p).wait_recv()
                prev = rbuf[p]
                sin_ref[:, cols] = prev
                sbuf[p] = dec_ref[:, cols] * prev + send_ref[:, cols]

            @pl.when(blk_id < blocks - 1)
            def _():
                hop_copy(p).start()

        @pl.when(i < tiles)
        def _():
            g = i // nn

            @pl.when(lax.rem(i, nn) == 0)
            def _():
                x_copy(g).wait()
            w_copy(i).wait()

            @pl.when(i + 1 < tiles)
            def _():
                w_copy(i + 1).start()

            @pl.when(i >= 2)
            def _():
                z_copy(i - 2).wait()
            zst[odd(i)] = dot32(xg[g], wzb[odd(i)]).astype(BF16)
            z_copy(i).start()
        return carry

    lax.fori_loop(0, max(tiles, hop * (blocks - 1) + pieces), body, 0)
    for i in PAIR:
        z_copy(tiles - 1 - i).wait()

    @pl.when(blk_id < blocks - 1)
    def _():
        for p in range(pieces):
            hop_copy(p).wait_send()


def z_chain(x_full, w_z, s_end, dec, chips, blocks, pieces=4, hop=2, nt=512):
    t, d_model = x_full.shape
    n_state, inner = s_end.shape
    tm = t // chips
    piece = scratch(F32, pieces, n_state, inner // pieces)
    two = sems(2)
    return pl.pallas_call(
        functools.partial(chain_kernel, chips, blocks, pieces, hop, nt),
        in_specs=[ANY, ANY, VMEM, VMEM],
        out_specs=[ANY, VMEM],
        out_shape=[out_of(BF16, t, inner), out_of(F32, n_state, inner)],
        scratch_shapes=[scratch(BF16, 2, tm, d_model), scratch(BF16, 2, d_model, nt), scratch(BF16, 2, tm, nt), piece, piece,
                        two, two, two, sems(pieces), sems(pieces)],
        compiler_params=params(60, 2),
        cost_estimate=pl.CostEstimate(flops=t * inner * d_model, bytes_accessed=t * inner, transcendentals=0),
        name='z_chain',
    )(x_full, w_z, s_end, dec)


def out_kernel(chips, nb, wc, slots, zt, xact_ref, bc_ref, cum_ref, cl_ref, seg_ref, segp_ref, sloc_ref, pd_ref, sin_ref, z_ref, xf_ref, wz_ref,
               dskip_ref, nw_ref, wo_ref, wp_ref, x_ref, o_ref, recv_ref,
               va_own, va_par, wbuf, send, rbuf, xo, xg, wzb, zb, xa, bca, sl, sbf, yoff, gated, dlane,
               vs_sem, vr_sem, w_sem, s_sem, r_sem, l_sem, x_sem, o_sem, c_sem, z_sem):
    me = lax.axis_index('tp')
    chip, core = me // CORES, odd(me)
    partner = CORES * chip + flip(core)
    chip_at = lambda d: lax.rem(chip + d, chips)
    ring = [CORES * chip_at(chips - 1) + core, CORES * chip_at(1) + core]
    q = va_own.shape[1]
    inner = xa.shape[1]
    heads = cum_ref.shape[0]
    head_dim = inner // heads
    per = LANES // head_dim
    n_state = sl.shape[0]
    half_cols = nb * wc
    steps = chips * nb * 2
    hq = q // 2
    ready = greet([('tp', partner)] + [('tp', r) for r in ring])

    def cols_of(u):
        return rows_at(odd(u) * half_cols + lax.rem(u // 2, nb) * wc, wc)

    def w_copies(u):
        slot = odd(u)
        return [pltpu.make_async_copy(ref.at[:, cols_of(u)], wbuf.at[slot, i], w_sem.at[slot, i]) for i, ref in enumerate((wo_ref, wp_ref))]

    for cp in w_copies(0):
        cp.start()
    x_copy = pltpu.make_async_copy(x_ref, xo, x_sem)
    x_copy.start()
    dlane[...] = expand_heads(dskip_ref[...], head_dim)
    ready()

    def swap(n, j):
        return remote(va_own.at[chips + odd(n)], va_par.at[j], vs_sem.at[n], vr_sem.at[n], 'tp', partner)

    def mix(c, zrow, tgt):
        at = rows_at(c * q, q)
        copies = [pltpu.make_async_copy(xact_ref.at[at, :], xa, c_sem.at[0]), pltpu.make_async_copy(bc_ref.at[at, :], bca, c_sem.at[1]),
                  pltpu.make_async_copy(sloc_ref.at[c], sl, c_sem.at[2])]
        for cp in copies:
            cp.start()
        seg_row = seg_ref[:, at]
        seg_prev = segp_ref[c][:, LANES - 1:]
        seg_rows = jnp.broadcast_to(seg_row, (q, q))
        causal = lax.broadcasted_iota(jnp.int32, (q, q), 0) >= lax.broadcasted_iota(jnp.int32, (q, q), 1)
        bias = jnp.where(causal & (seg_rows == seg_rows.T), 0.0, NEG)
        cum = cum_ref[:, at]
        cl = cl_ref[:, at]
        cum_cols = cum.T
        in_cols = jnp.where(seg_row == seg_prev, jnp.exp2(cum), 0.0).T
        for cp in copies:
            cp.wait()
        sbf[...] = (sl[...] + pd_ref[c] * sin_ref[...]).astype(BF16)
        c_act = bca[:, n_state:]
        scores = lax.dot_general(c_act, bca[:, 0:n_state], (((1,), (1,)), ((), ())), preferred_element_type=F32)
        yoff[...] = dot32(c_act, sbf[...])
        lane = lax.broadcasted_iota(jnp.int32, (q, LANES), 1) // head_dim
        sq = jnp.zeros((q, LANES), F32)
        for i in range(inner // LANES):
            cols = slice(i * LANES, (i + 1) * LANES)
            x_f = xa[:, cols].astype(F32)
            tops, bots = [], []
            for j in range(per):
                h = i * per + j
                x_h = jnp.where(lane == j, x_f, 0.0).astype(BF16)
                ccol, crow = cum_cols[:, h:h + 1], cl[h:h + 1, :]
                m_top = jnp.exp2(ccol[0:hq] + bias[0:hq, 0:hq] - crow[:, 0:hq]) * scores[0:hq, 0:hq]
                m_bot = jnp.exp2(ccol[hq:] + bias[hq:] - crow) * scores[hq:]
                tops.append(dot32(m_top.astype(BF16), x_h[0:hq]))
                bots.append(dot32(m_bot.astype(BF16), x_h))
            y = jnp.concatenate([sum(tops), sum(bots)], axis=0)
            y = y + yoff[:, cols] * head_lanes(in_cols, i, head_dim) + dlane[:, cols] * x_f
            v = y * silu(zb[zrow, :, cols].astype(F32))
            gated[:, cols] = v
            sq = sq + v * v
        inv = lax.rsqrt(jnp.sum(sq, axis=1, keepdims=True) * (1.0 / inner) + NORM_EPS)
        inv = jnp.broadcast_to(inv, (q, LANES))
        for i in range(inner // LANES):
            cols = slice(i * LANES, (i + 1) * LANES)
            va_own[tgt, :, cols] = (gated[:, cols] * inv * nw_ref[:, cols].astype(F32)).astype(BF16)

    def prep(n):
        j = chip_at(jnp.where(n == 0, chips - 1, jnp.where(n == 3, 0, n)))
        tok = rows_at(j * (CORES * q), CORES * q)

        @pl.when(n < 2)
        def _():
            for p in PAIR:
                pltpu.make_async_copy(z_ref.at[rows_at((CORES * j + p) * q, q), :], zb.at[p], c_sem.at[p]).start()
            for p in PAIR:
                pltpu.make_async_copy(z_ref.at[rows_at((CORES * j + p) * q, q), :], zb.at[p], c_sem.at[p]).wait()

        @pl.when(n >= 2)
        def _():
            def wz_copy(m):
                return pltpu.make_async_copy(wz_ref.at[:, rows_at(m * zt, zt)], wzb.at[odd(m)], z_sem.at[odd(m)])
            rows_copy = pltpu.make_async_copy(xf_ref.at[tok, :], xg, c_sem.at[0])
            rows_copy.start()
            wz_copy(0).start()
            rows_copy.wait()

            def z_body(m, carry):
                wz_copy(m).wait()

                @pl.when(m + 1 < inner // zt)
                def _():
                    wz_copy(m + 1).start()
                res = dot32(xg[...], wzb[odd(m)]).astype(BF16)
                for p in PAIR:
                    zb[p, :, rows_at(m * zt, zt)] = res[p * q:(p + 1) * q]
                return carry
            lax.fori_loop(0, inner // zt, z_body, 0)

            swap(n - 2, j).wait_send()

        def chunk(i, carry):
            par = jnp.where(i == 0, flip(core), core)
            mix(CORES * j + par, par, jnp.where(i == 0, chips + odd(n), j))

            @pl.when(i == 0)
            def _():
                swap(n, j).start()
            return carry
        lax.fori_loop(0, CORES, chunk, 0)
        swap(n, j).wait_recv()

    def ring_copy(d, unit):
        slot = lax.rem(unit, slots)
        return remote(send.at[d, slot], recv_ref.at[d, unit], s_sem.at[d, slot], r_sem.at[d, unit], 'tp', jnp.where(d == 0, ring[1], ring[0]))

    def fetch(d, unit):
        ring_copy(d, unit).wait_recv()
        cp = pltpu.make_async_copy(recv_ref.at[d, unit], rbuf, l_sem)
        cp.start()
        cp.wait()

    def o_copy(d, b):
        cols = rows_at(d * half_cols + b * wc, wc)
        return pltpu.make_async_copy(xo.at[:, cols], o_ref.at[:, cols], o_sem.at[d, b])

    def body(u, carry):
        d = odd(u)
        k = u // (2 * nb)
        b = lax.rem(u // 2, nb)
        unit = k * nb + b

        @pl.when((u < 2) | ((b == 0) & (d == 0) & (k < chips - 1)))
        def _():
            prep(jnp.where(u < 2, u, k + 1))
        dest = chip_at(jnp.where(d == 0, 2 * chips - 1 - k, 1 + k))
        for cp in w_copies(u):
            cp.wait()

        @pl.when(u + 1 < steps)
        def _():
            for cp in w_copies(u + 1):
                cp.start()
        part = dot32(va_own[dest], wbuf[odd(u), 0]) + dot32(va_par[dest], wbuf[odd(u), 1])

        @pl.when(k < chips - 1)
        def _():
            slot = lax.rem(unit, slots)

            @pl.when(unit >= slots)
            def _():
                ring_copy(d, unit - slots).wait_send()

            @pl.when(k == 0)
            def _():
                send[d, slot] = part

            @pl.when(k > 0)
            def _():
                fetch(d, unit - nb)
                send[d, slot] = part + rbuf[...]
            ring_copy(d, unit).start()

        @pl.when(k == chips - 1)
        def _():
            @pl.when((b == 0) & (d == 0))
            def _():
                x_copy.wait()
            fetch(d, unit - nb)
            cols = cols_of(u)
            xo[:, cols] = (xo[:, cols].astype(F32) + (part + rbuf[...])).astype(BF16)
            o_copy(d, b).start()
        return carry

    lax.fori_loop(0, steps, body, 0)

    def drain(i, carry):
        o_copy(odd(i), i // 2).wait()
        return carry

    def drain_send(i, carry):
        ring_copy(odd(i), (chips - 1) * nb - slots + i // 2).wait_send()
        return carry
    lax.fori_loop(0, 2 * slots, drain_send, 0)
    for n in PAIR:
        swap(2 + n, chip).wait_send()
    lax.fori_loop(0, 2 * nb, drain, 0)


def out_proj_scatter(x_act, bc_act, cum, cl, seg_row, seg_prev, sloc, pd, s_in, z_arr, x_full, w_z, d_skip, norm_w, w_own, w_par, x_loc, chips, wc=512, slots=4, zt=256):
    t, inner = x_act.shape
    rows, d_model = x_loc.shape
    gw = bc_act.shape[1]
    n_state = s_in.shape[0]
    nb = d_model // 2 // wc
    units = (chips - 1) * nb
    return pl.pallas_call(
        functools.partial(out_kernel, chips, nb, wc, slots, zt),
        in_specs=[ANY, ANY, VMEM, VMEM, VMEM, VMEM, ANY, VMEM, VMEM, ANY, ANY, ANY, VMEM, VMEM, ANY, ANY, ANY],
        out_specs=[ANY, ANY],
        out_shape=[out_of(BF16, rows, d_model), out_of(F32, 2, units, rows, wc)],
        scratch_shapes=[scratch(BF16, chips + 2, rows, inner), scratch(BF16, chips, rows, inner), scratch(BF16, 2, 2, inner, wc), scratch(F32, 2, slots, rows, wc),
                        scratch(F32, rows, wc), scratch(BF16, rows, d_model), scratch(BF16, CORES * rows, d_model), scratch(BF16, 2, d_model, zt),
                        scratch(BF16, CORES, rows, inner), scratch(BF16, rows, inner), scratch(BF16, rows, gw), scratch(F32, n_state, inner),
                        scratch(BF16, n_state, inner), scratch(F32, rows, inner), scratch(F32, rows, inner), scratch(F32, 1, inner),
                        sems(chips), sems(chips), sems(2, 2), sems(2, slots), sems(2, units), DMA, DMA, sems(2, nb), sems(3), sems(2)],
        compiler_params=params(63, 1),
        cost_estimate=pl.CostEstimate(flops=2 * t * inner * d_model, bytes_accessed=t * d_model, transcendentals=0),
        name='out_proj_scatter',
    )(x_act, bc_act, cum, cl, seg_row, seg_prev, sloc, pd, s_in, z_arr, x_full, w_z, d_skip, norm_w, w_own, w_par, x_loc)[0]


def layer(x_loc, seg_loc, w_zx, w_bc, w_dt, conv_x, conv_bc, bias_x, bias_bc, a_log, dt_bias, d_skip, norm_w, w_out, chips, blocks):
    rows = x_loc.shape[0]
    x_full, x_pre, small, w_z, w_par, seg, seg_tail, tail_x, tail_b = gather_proj(x_loc, w_zx, w_bc, w_dt.T, w_out, seg_loc[None], chips, blocks)
    x_act, bc_act, cum, cl, seg_row, seg_prev, sloc, pd, s_end, dec = phase_a(
        x_pre, small, seg, seg_tail, tail_x, tail_b, conv_x, conv_bc, bias_x[None], bias_bc, a_log[None], dt_bias[None], rows)
    z_arr, s_in = z_chain(x_full, w_z, s_end, dec, chips, blocks)
    return out_proj_scatter(x_act, bc_act, cum, cl, seg_row, seg_prev, sloc, pd, s_in, z_arr, x_full, w_z, d_skip[None], norm_w[None], w_out, w_par, x_loc, chips)


def solution(mesh):
    tokens = ('dp', 'sp', 'tp')
    heads = P('tp')
    cols = P(None, 'tp')
    deep = P(None, None, 'tp')
    specs = (P(tokens, None), P(tokens), deep, deep, cols, cols, deep, heads, cols, heads, heads, heads, heads, P('tp', None))
    body = functools.partial(layer, chips=mesh.shape['tp'] // CORES, blocks=mesh.shape['sp'])
    return jax.shard_map(body, mesh=mesh, in_specs=specs, out_specs=specs[0], check_vma=False)
```

```python
import functools
import jax
import jax.numpy as jnp
from jax import lax
from jax.experimental import pallas as pl
from jax.experimental.pallas import tpu as pltpu
from jax.sharding import PartitionSpec as P

MESH = pl.DeviceIdType.MESH
NORM_EPS = 1e-5
LOG2E = 1.4426950408889634
FAR = -1e6
NEG = -1e30
F32 = jnp.float32
BF16 = jnp.bfloat16
HI = lax.Precision.HIGHEST
MIB = 2 ** 20
LANES = 128
ROW8 = 8
CORES = 2
PAIR = range(2)
ANY = pl.BlockSpec(memory_space=pl.ANY)
VMEM = pl.BlockSpec(memory_space=pltpu.VMEM)
DMA = pltpu.SemaphoreType.DMA


def scratch(dtype, *shape):
    return pltpu.VMEM(shape, dtype)


def out_of(dtype, *shape):
    return jax.ShapeDtypeStruct(shape, dtype)


def sems(*shape):
    return DMA(shape)


def rows_at(start, size):
    return pl.ds(pl.multiple_of(start, size), size)


def odd(i):
    return lax.rem(i, 2)


def flip(i):
    return 1 - i


def dot32(a, b):
    return jnp.dot(a, b, preferred_element_type=F32)


def params(limit, name_id=None):
    if name_id is None:
        return pltpu.CompilerParams(dimension_semantics=('arbitrary',), vmem_limit_bytes=limit * MIB)
    return pltpu.CompilerParams(collective_id=name_id, has_side_effects=True, vmem_limit_bytes=limit * MIB)


def greet(peers):
    barrier = pltpu.get_barrier_semaphore()
    for axis, index in peers:
        pl.semaphore_signal(barrier, inc=1, device_id={axis: index}, device_id_type=MESH)
    return lambda: pl.semaphore_wait(barrier, len(peers))


def remote(src, dst, send, recv, axis, index):
    return pltpu.make_async_remote_copy(src_ref=src, dst_ref=dst, send_sem=send, recv_sem=recv, device_id={axis: index}, device_id_type=MESH)


def silu(v):
    h = v * 0.5
    return h + h * jnp.tanh(h)


def head_lanes(cols, tile_idx, head_dim):
    rows = cols.shape[0]
    per = LANES // head_dim
    lane = lax.broadcasted_iota(jnp.int32, (rows, LANES), 1)
    out = None
    for j in range(per):
        h = tile_idx * per + j
        nxt = jnp.broadcast_to(cols[:, h:h + 1], (rows, LANES))
        out = nxt if out is None else jnp.where(lane >= j * head_dim, nxt, out)
    return out


def expand_heads(row, head_dim):
    heads = row.shape[1]
    shape = (heads, heads * head_dim)
    eye = (lax.broadcasted_iota(jnp.int32, shape, 1) // head_dim == lax.broadcasted_iota(jnp.int32, shape, 0)).astype(F32)
    return jnp.dot(jnp.broadcast_to(row, (ROW8, heads)), eye, precision=HI, preferred_element_type=F32)[0:1]


def column(row):
    return jnp.broadcast_to(row, (LANES, row.shape[1])).T[:, 0:1]


def gather_kernel(chips, blocks, kb, nb, sub, nt, pace, x_ref, wzx_ref, wbc_ref, wdt_ref, wo_ref, seg_ref,
                  xf_ref, xp_ref, bp_ref, wz_ref, wp_ref, segf_ref, segt_ref, tx_ref, tb_ref,
                  wx, wsm, xg, ost, bst, blk, bblk, zst, wdt,
                  ra_sem, rd_sem, so_sem, sf_sem, sd_sem, xl_sem, xs_sem, in_sem, zo_sem, bb_sem, dt_sem, oo_sem, bo_sem,
                  wp_sem, sg_sem, sr_sem, st_sem, hx_sem, hb_sem):
    me = lax.axis_index('tp')
    blk_id = lax.axis_index('sp')
    chip, core = me // CORES, odd(me)
    partner = CORES * chip + flip(core)
    near = [lax.rem(chip + chips - 1, chips), lax.rem(chip + 1, chips)]
    far = lax.rem(chip + chips // 2, chips)
    ring = [CORES * c + core for c in near]
    sp_next = lax.rem(blk_id + 1, blocks)
    n_tp = CORES * chips
    rows = x_ref.shape[0]
    quarters = xl_sem.shape[1]
    qr = rows // quarters
    d_model, inner = wx.shape
    heads = wdt.shape[0]
    n_state = bblk.shape[3]
    nk = d_model // kb
    nblk = nk * (inner // nb)
    opp = 2 + quarters
    last = opp + quarters // 2 - 1
    ready = greet([('tp', lax.rem(me + d, n_tp)) for d in range(1, n_tp)] + [('sp', sp_next), ('sp', lax.rem(blk_id + blocks - 1, blocks))])

    def row_of(lv, b):
        side = odd(b)
        other = jnp.where(lv < 2, lv, b // 2)
        cc = jnp.where(other == 1, flip(core), core)
        ch = jnp.where(lv < 2, chip, jnp.where(lv >= opp, far, jnp.where(side == 0, near[0], near[1])))
        q = jnp.where(lv < 2, b, jnp.where(lv >= opp, side * (quarters // 2) + lv - opp, lv - 2))
        return (CORES * ch + cc) * rows + q * qr

    def full_rows(lv, b, size=qr):
        return xf_ref.at[rows_at(row_of(lv, b), size), :]

    def w_tile(i):
        return rows_at(lax.rem(i, nk) * kb, kb), rows_at((i // nk) * nb, nb)

    def blk_copy(i):
        kk, nn = w_tile(i)
        slot = lax.rem(i, blk.shape[0])
        return pltpu.make_async_copy(wzx_ref.at[kk, :, nn], blk.at[slot], in_sem.at[slot])

    def z_copy(i):
        kk, nn = w_tile(i)
        return pltpu.make_async_copy(zst.at[odd(i)], wz_ref.at[kk, nn], zo_sem.at[odd(i)])

    def bc_copy(i):
        return pltpu.make_async_copy(wbc_ref.at[rows_at(i * kb, kb)], bblk.at[odd(i)], bb_sem.at[odd(i)])

    own_load = pltpu.make_async_copy(x_ref, xg.at[0], xs_sem.at[0])
    dt_load = pltpu.make_async_copy(wdt_ref, wdt, dt_sem)
    own_load.start()
    dt_load.start()
    bc_copy(0).start()
    for i in range(blk.shape[0]):
        blk_copy(i).start()
    ready()

    def own_send(q, to):
        return remote(x_ref.at[rows_at(q * qr, qr), :], full_rows(0, q), so_sem.at[to, q], ra_sem.at[2 + q, flip(to)], 'tp', ring[to])

    own_pair = remote(x_ref, full_rows(0, 0, rows), sd_sem.at[1, 0], rd_sem.at[1, 0], 'tp', partner)

    def pair_send(lv, side):
        return remote(full_rows(lv, side), full_rows(lv, side), sd_sem.at[lv, side], rd_sem.at[lv, side], 'tp', partner)

    def forward(lv, to):
        side = flip(to)
        h = lax.rem(lv - 2, quarters // 2)
        dst_sem = ra_sem.at[opp + h, side]
        return remote(full_rows(lv, side), full_rows(lv, side), sf_sem.at[to, h], dst_sem, 'tp', ring[to])

    def arrival(lv, side):
        return remote(full_rows(lv, side), full_rows(lv, side), so_sem.at[0, 0], ra_sem.at[lv, side], 'tp', ring[0])

    def pair_arrival(lv, side):
        ref = full_rows(lv, 2 + side)
        return remote(ref, ref, sd_sem.at[1, 0], rd_sem.at[lv, side], 'tp', partner)

    pair_own_arrival = remote(full_rows(1, 0, rows), full_rows(1, 0, rows), sd_sem.at[1, 0], rd_sem.at[1, 0], 'tp', partner)

    def send_quarter(q):
        for to in PAIR:
            own_send(q, flip(to)).start()
    send_quarter(0)
    own_pair.start()

    def seg_cols(index):
        return segf_ref.at[:, rows_at(index * rows, rows)]

    def seg_send(d):
        return remote(seg_ref, seg_cols(me), sg_sem.at[d], sr_sem.at[d], 'tp', lax.rem(me + d, n_tp))

    def seg_arrival(d):
        return remote(seg_ref, seg_cols(lax.rem(me + n_tp - d, n_tp)), sg_sem.at[d], sr_sem.at[d], 'tp', lax.rem(me + d, n_tp))

    seg_own = pltpu.make_async_copy(seg_ref, seg_cols(me), sg_sem.at[0])
    seg_own.start()
    for d in range(1, n_tp):
        seg_send(d).start()
    w_swap = remote(wo_ref, wp_ref, wp_sem.at[0], wp_sem.at[1], 'tp', partner)
    w_swap.start()
    seg_halo = remote(segf_ref.at[:, pl.ds(n_tp * rows - LANES, LANES)], segt_ref, st_sem.at[0], st_sem.at[1], 'sp', sp_next)

    end_chip = chips - 1
    hrows = tx_ref.shape[0]
    halo_lv = jnp.where(chip == end_chip, flip(core), jnp.where(far == end_chip, last, opp - 1))
    halo_b = jnp.where(chip == end_chip, quarters - 1, jnp.where((far != end_chip) & (near[0] == end_chip), 0, 1) + CORES * flip(core))

    def halo_copies(slot):
        src = rows_at(halo_b * qr + qr - hrows, hrows)
        return [remote(ost.at[slot, src, :], tx_ref, hx_sem.at[0], hx_sem.at[1], 'sp', sp_next),
                remote(bst.at[slot, src, :], tb_ref, hb_sem.at[0], hb_sem.at[1], 'sp', sp_next)]

    dt_load.wait()

    def small_body(i, carry):
        bc_copy(i).wait()

        @pl.when(i + 1 < nk)
        def _():
            bc_copy(i + 1).start()

        def inner_body(s, carry2):
            part = jnp.swapaxes(bblk[odd(i), rows_at(s * sub, sub)], 0, 1)
            at = rows_at(i * kb + s * sub, sub)
            for g in PAIR:
                wsm[at, g * n_state:(g + 1) * n_state] = part[g]
            wd = jnp.concatenate([wdt[:, at].astype(F32), jnp.zeros((LANES - heads, sub), F32)], axis=0)
            wsm[at, 2 * n_state:] = wd.T.astype(BF16)
            return carry2
        return lax.fori_loop(0, kb // sub, inner_body, carry)
    lax.fori_loop(0, nk, small_body, 0)

    def relay(i, carry):
        slot = lax.rem(i, blk.shape[0])
        blk_copy(i).wait()

        @pl.when(i >= 2)
        def _():
            z_copy(i - 2).wait()
        kk = lax.rem(i, nk) * kb

        def inner_body(s, carry2):
            at = rows_at(s * sub, sub)
            part = jnp.swapaxes(blk[slot, at].astype(F32), 0, 1)
            zst[odd(i), at, :] = part[0].astype(BF16)
            wx[rows_at(kk + s * sub, sub), w_tile(i)[1]] = part[1].astype(BF16)
            return carry2
        lax.fori_loop(0, kb // sub, inner_body, 0)
        z_copy(i).start()
        for q in range(1, quarters - 1):
            pl.when(i == q * pace - 1)(functools.partial(send_quarter, q))

        @pl.when(i + blk.shape[0] < nblk)
        def _():
            blk_copy(i + blk.shape[0]).start()
        return carry
    lax.fori_loop(0, nblk, relay, 0)

    seg_own.wait()
    for d in range(1, n_tp):
        seg_arrival(d).wait_recv()
    seg_halo.start()
    own_load.wait()
    own_store = pltpu.make_async_copy(xg.at[0], full_rows(0, 0, rows), xs_sem.at[1])
    own_store.start()

    def load(lv, b):
        return pltpu.make_async_copy(full_rows(lv, b), xg.at[odd(lv), rows_at(b * qr, qr), :], xl_sem.at[odd(lv), b])

    def take(lv):
        @pl.when(lv >= 2)
        def _():
            for side in PAIR:
                arrival(lv, side).wait_recv()
                pair_send(lv, side).start()

    def fetch(lv):
        @pl.when(lv == 1)
        def _():
            pair_own_arrival.wait_recv()

        @pl.when(lv >= 2)
        def _():
            for side in PAIR:
                pair_arrival(lv, side).wait_recv()
        for b in range(quarters):
            load(lv, b).start()

    def out_copies(lv):
        slot = odd(lv)
        res = []
        for b in range(quarters):
            src, dst = rows_at(b * qr, qr), rows_at(row_of(lv, b), qr)
            res.append(pltpu.make_async_copy(ost.at[slot, src, :], xp_ref.at[dst, :], oo_sem.at[slot, b]))
            res.append(pltpu.make_async_copy(bst.at[slot, src, :], bp_ref.at[dst, :], bo_sem.at[slot, b]))
        return res

    early = opp - 1
    cut = 2 + quarters // 2

    def feed(lv):
        @pl.when(lv == 1)
        def _():
            send_quarter(quarters - 1)
        for h in range(quarters // 2):
            @pl.when(lv == 3 + 2 * h)
            def _(h=h):
                forward(2 + h, 1).start()
                forward(cut + h, 0).start()

    def round_body(lv, carry):
        slot = odd(lv)

        @pl.when(lv > 0)
        def _():
            for b in range(quarters):
                load(lv, b).wait()

        @pl.when(lv == 1)
        def _():
            own_store.wait()

        @pl.when(lv < early)
        def _():
            take(lv + 1)

        @pl.when(lv >= 2)
        def _():
            for cp in out_copies(lv - 2):
                cp.wait()

        def dots(n, carry2):
            @pl.when(n == inner // nt // 2)
            def _():
                feed(lv)

                @pl.when(lv < early)
                def _():
                    fetch(lv + 1)
            cols = rows_at(n * nt, nt)
            ost[slot, :, cols] = dot32(xg[slot], wx[:, cols]).astype(BF16)
            return carry2
        lax.fori_loop(0, inner // nt, dots, 0)
        bst[slot] = dot32(xg[slot], wsm[...]).astype(BF16)
        for cp in out_copies(lv):
            cp.start()

        @pl.when(lv == halo_lv + 1)
        def _():
            for cp in halo_copies(flip(slot)):
                cp.wait_send()

        @pl.when(lv == halo_lv)
        def _():
            for cp in halo_copies(slot):
                cp.start()

        @pl.when((lv >= early) & (lv < last))
        def _():
            take(lv + 1)
            fetch(lv + 1)
        return carry
    lax.fori_loop(0, last + 1, round_body, 0)

    @pl.when(halo_lv == last)
    def _():
        for cp in halo_copies(last % 2):
            cp.wait_send()
    for cp in halo_copies(0):
        cp.wait_recv()
    seg_halo.wait()
    for d in range(1, n_tp):
        seg_send(d).wait_send()
    w_swap.wait()
    for i in PAIR:
        for cp in out_copies(last - i):
            cp.wait()
        z_copy(nblk - 1 - i).wait()
    own_pair.wait_send()
    for to in PAIR:
        for q in range(quarters):
            own_send(q, to).wait_send()
        for h in range(quarters // 2):
            forward(2 + h, to).wait_send()
    for lv in range(2, last + 1):
        for side in PAIR:
            pair_send(lv, side).wait_send()


def gather_proj(x_loc, w_zx, w_bc, w_dt_t, w_out, seg, chips, blocks, kb=2048, nb=256, sub=256, nt=512, quarters=4, pace=12):
    rows, d_model = x_loc.shape
    inner, n_state, heads = w_zx.shape[2], w_bc.shape[2], w_dt_t.shape[0]
    n_tp = CORES * chips
    t = rows * n_tp
    small = CORES * n_state + LANES
    lv = CORES + quarters + quarters // 2
    halo = 16
    two = sems(2)
    return pl.pallas_call(
        functools.partial(gather_kernel, chips, blocks, kb, nb, sub, nt, pace),
        in_specs=[ANY] * 6,
        out_specs=[ANY] * 9,
        out_shape=[out_of(BF16, t, d_model), out_of(BF16, t, inner), out_of(BF16, t, small), out_of(BF16, d_model, inner), out_of(BF16, *w_out.shape),
                   out_of(jnp.int32, 1, t), out_of(jnp.int32, 1, LANES), out_of(BF16, halo, inner), out_of(BF16, halo, small)],
        scratch_shapes=[scratch(BF16, d_model, inner), scratch(BF16, d_model, small), scratch(BF16, 2, rows, d_model),
                        scratch(BF16, 2, rows, inner), scratch(BF16, 2, rows, small), scratch(BF16, 3, kb, CORES, nb),
                        scratch(BF16, 2, kb, CORES, n_state), scratch(BF16, 2, kb, nb), scratch(BF16, heads, d_model),
                        sems(lv, 2), sems(lv, 2), sems(2, quarters), sems(2, quarters), sems(lv, 2), sems(2, quarters), two, sems(3), two, two, DMA,
                        sems(2, quarters), sems(2, quarters), two, sems(n_tp), sems(n_tp), two, two, two],
        compiler_params=params(63, 0),
        cost_estimate=pl.CostEstimate(flops=t * inner * d_model, bytes_accessed=t * inner, transcendentals=0),
        name='gather_proj',
    )(x_loc, w_zx, w_bc, w_dt_t, w_out, seg)


def phase_a_kernel(q, x_ref, small_ref, seg_ref, segt_ref, tailx_ref, tailb_ref, cx_ref, cbc_ref, bx_ref, bbc_ref, alog_ref, dtb_ref,
                   xact_ref, bcact_ref, cum_ref, cl_ref, segf_ref, segp_ref, sloc_ref, pd_ref, send_ref, dec_ref,
                   pad, xw, segtail, base, cw):
    inner = x_ref.shape[1]
    gw = bcact_ref.shape[1]
    n_state = gw // 2
    heads = alog_ref.shape[1]
    head_dim = inner // heads
    taps = cx_ref.shape[0]

    @pl.when(pl.program_id(0) == 0)
    def _():
        first = lax.axis_index('sp') == 0
        base[...] = jnp.broadcast_to(jnp.where(first, seg_ref[:, 0:1], segt_ref[:, LANES - 1:]), base.shape)
        segtail[...] = jnp.where(first, FAR, (segt_ref[...] - base[...]).astype(F32))
        pad[0:ROW8, 0:inner] = tailx_ref[...].astype(F32)[ROW8:]
        pad[0:ROW8, inner:] = tailb_ref[:, 0:gw].astype(F32)[ROW8:]
        cw[0:taps, 0:inner] = cx_ref[...].astype(F32)
        for i in range(inner // LANES):
            cw[taps:taps + 1, i * LANES:(i + 1) * LANES] = bx_ref[i:i + 1, :].astype(F32)
        for g in PAIR:
            cols = slice(inner + g * n_state, inner + (g + 1) * n_state)
            cw[0:taps, cols] = cbc_ref[:, g, :].astype(F32)
            cw[taps:taps + 1, cols] = bbc_ref[g:g + 1, :].astype(F32)
        send_ref[...] = jnp.zeros_like(send_ref)
        dec_ref[...] = jnp.ones_like(dec_ref)

    @pl.when(pl.program_id(0) > 0)
    def _():
        pad[0:ROW8, :] = pad[q:q + ROW8, :]

    pad[ROW8:, 0:inner] = x_ref[...].astype(F32)
    pad[ROW8:, inner:] = small_ref[:, 0:gw].astype(F32)
    seg_row = (seg_ref[...] - base[:, 0:1]).astype(F32)
    prev_row = segtail[...]
    segf_ref[...] = seg_row
    segp_ref[0] = prev_row
    segtail[...] = seg_row[:, q - LANES:]
    ext = jnp.concatenate([prev_row, seg_row], axis=1)
    seg_last, seg_prev = seg_row[:, q - 1:], prev_row[:, LANES - 1:]
    keeps = []
    for j in range(1, taps):
        keep_row = jnp.where(ext[:, LANES - j:LANES - j + q] == seg_row, 1.0, 0.0)
        keeps.append(jnp.broadcast_to(keep_row, (LANES, q)).T)
    raw = small_ref[:, gw:].astype(F32).T[0:heads] + column(dtb_ref[...])
    dt = jnp.maximum(raw, 0.0) + jnp.log1p(jnp.exp(-jnp.abs(raw)))
    log_a = dt * column(jnp.exp(alog_ref[...]) * -LOG2E)
    tri = (lax.broadcasted_iota(jnp.int32, (q, q), 0) <= lax.broadcasted_iota(jnp.int32, (q, q), 1)).astype(F32)
    cum = jnp.dot(log_a, tri, precision=HI, preferred_element_type=F32)
    cum_ref[...] = cum
    cl_ref[...] = cum - jnp.log(dt) * LOG2E
    cum_last = cum[:, q - 1:]
    end_cols = (jnp.where(seg_row == seg_last, jnp.exp2(cum_last - cum), 0.0) * dt).T
    carry = jnp.where(seg_last == seg_prev, jnp.exp2(cum_last), 0.0)
    carry_lane = expand_heads(jnp.broadcast_to(carry, (heads, LANES)).T[0:1], head_dim)
    for i in range((inner + gw) // LANES):
        cols = slice(i * LANES, (i + 1) * LANES)
        src = pad[:, cols]
        acc = cw[taps:taps + 1, cols] + src[ROW8:] * cw[taps - 1:taps, cols]
        for j in range(1, taps):
            at = taps - 1 - j
            acc = acc + pltpu.roll(src, j, axis=0)[ROW8:] * cw[at:at + 1, cols] * keeps[j - 1]
        act = silu(acc).astype(BF16)
        if i * LANES < inner:
            xact_ref[:, cols] = act
            xw[:, cols] = (act.astype(F32) * head_lanes(end_cols, i, head_dim)).astype(BF16)
        else:
            bcact_ref[:, i * LANES - inner:(i + 1) * LANES - inner] = act
    sloc_ref[0] = send_ref[...]
    pd_ref[0] = dec_ref[...]
    send_ref[...] = carry_lane * send_ref[...] + dot32(bcact_ref[:, 0:n_state].T, xw[...])
    dec_ref[...] = dec_ref[...] * carry_lane


def phase_a(x_pre, small, seg, seg_tail, tail_x, tail_b, conv_x, conv_bc, bias_x, bias_bc, a_log, dt_bias, q):
    t, inner = x_pre.shape
    n_state = conv_bc.shape[2]
    gw = CORES * n_state
    heads = a_log.shape[1]
    nt = t // q

    def full(shape):
        return pl.BlockSpec(shape, lambda c: (0,) * len(shape))

    def by_row(width):
        return pl.BlockSpec((q, width), lambda c: (c, 0))

    def by_col(height):
        return pl.BlockSpec((height, q), lambda c: (0, c))

    def by_chunk(a, b):
        return pl.BlockSpec((1, a, b), lambda c: (c, 0, 0))

    rest = (seg_tail, tail_x, tail_b, conv_x, conv_bc, bias_x, bias_bc, a_log, dt_bias)
    return pl.pallas_call(
        functools.partial(phase_a_kernel, q),
        grid=(nt,),
        in_specs=[by_row(inner), by_row(small.shape[1]), by_col(1)] + [full(v.shape) for v in rest],
        out_specs=[by_row(inner), by_row(gw), by_col(heads), by_col(heads), by_col(1), by_chunk(1, LANES), by_chunk(n_state, inner), by_chunk(1, inner),
                   full((n_state, inner)), full((1, inner))],
        out_shape=[out_of(BF16, t, inner), out_of(BF16, t, gw), out_of(F32, heads, t), out_of(F32, heads, t), out_of(F32, 1, t), out_of(F32, nt, 1, LANES),
                   out_of(F32, nt, n_state, inner), out_of(F32, nt, 1, inner), out_of(F32, n_state, inner), out_of(F32, 1, inner)],
        scratch_shapes=[scratch(F32, q + ROW8, inner + gw), scratch(BF16, q, inner), scratch(F32, 1, LANES),
                        scratch(jnp.int32, 1, LANES), scratch(F32, ROW8, inner + gw)],
        compiler_params=params(56),
        cost_estimate=pl.CostEstimate(flops=t * inner * gw, bytes_accessed=t * inner, transcendentals=0),
        name='phase_a',
    )(x_pre, small, seg, *rest)


def chain_kernel(chips, blocks, pieces, hop, nt, xf_ref, wz_ref, send_ref, dec_ref, z_ref, sin_ref,
                 xg, wzb, zst, sbuf, rbuf, x_sem, w_sem, z_sem, s_sem, r_sem):
    chip = lax.axis_index('tp') // CORES
    blk_id = lax.axis_index('sp')
    sp_next = lax.rem(blk_id + 1, blocks)
    ready = greet([('sp', sp_next), ('sp', lax.rem(blk_id + blocks - 1, blocks))])
    n_state, inner = send_ref.shape
    tm = xg.shape[1]
    nn = inner // nt
    tiles = CORES * nn
    pw = inner // pieces
    parts = range(x_sem.shape[1])
    kw = xg.shape[2] // len(parts)

    def tok(g):
        return rows_at(lax.rem(chip + jnp.where(g == 0, chips - 1, 1), chips) * tm, tm)

    def col(i):
        return rows_at(lax.rem(i, nn) * nt, nt)

    def depth(s):
        return pl.ds(s * kw, kw)

    def x_copy(g, s):
        return pltpu.make_async_copy(xf_ref.at[tok(g), depth(s)], xg.at[g, :, depth(s)], x_sem.at[g, s])

    def w_copy(i, s):
        return pltpu.make_async_copy(wz_ref.at[depth(s), col(i)], wzb.at[odd(i), depth(s), :], w_sem.at[odd(i), s])

    def z_copy(i):
        return pltpu.make_async_copy(zst.at[odd(i)], z_ref.at[tok(i // nn), col(i)], z_sem.at[odd(i)])

    def hop_copy(p):
        return remote(sbuf.at[p], rbuf.at[p], s_sem.at[p], r_sem.at[p], 'sp', sp_next)

    for s in parts:
        x_copy(0, s).start()
        w_copy(0, s).start()
    ready()

    def body(i, carry):
        p = i - hop * blk_id

        @pl.when((p >= 0) & (p < pieces))
        def _():
            cols = rows_at(p * pw, pw)

            @pl.when(blk_id == 0)
            def _():
                sbuf[p] = send_ref[:, cols]
                sin_ref[:, cols] = jnp.zeros((n_state, pw), F32)

            @pl.when(blk_id > 0)
            def _():
                hop_copy(p).wait_recv()
                prev = rbuf[p]
                sin_ref[:, cols] = prev
                sbuf[p] = dec_ref[:, cols] * prev + send_ref[:, cols]

            @pl.when(blk_id < blocks - 1)
            def _():
                hop_copy(p).start()

        @pl.when(i < tiles)
        def _():
            g = i // nn

            @pl.when(i >= 2)
            def _():
                z_copy(i - 2).wait()
            res = 0.0
            for s in parts:
                @pl.when(lax.rem(i, nn) == 0)
                def _(s=s):
                    x_copy(g, s).wait()
                w_copy(i, s).wait()

                @pl.when(i + 1 < tiles)
                def _(s=s):
                    w_copy(i + 1, s).start()
                pl.when(i == 1)(x_copy(1, s).start)
                res = res + dot32(xg[g, :, depth(s)], wzb[odd(i), depth(s), :])
            zst[odd(i)] = res.astype(BF16)
            z_copy(i).start()
        return carry

    lax.fori_loop(0, max(tiles, hop * (blocks - 1) + pieces), body, 0)
    for i in PAIR:
        z_copy(tiles - 1 - i).wait()

    @pl.when(blk_id < blocks - 1)
    def _():
        for p in range(pieces):
            hop_copy(p).wait_send()


def z_chain(x_full, w_z, s_end, dec, chips, blocks, pieces=4, hop=2, nt=512, parts=4):
    t, d_model = x_full.shape
    n_state, inner = s_end.shape
    tm = t // chips
    piece = scratch(F32, pieces, n_state, inner // pieces)
    two = sems(2)
    return pl.pallas_call(
        functools.partial(chain_kernel, chips, blocks, pieces, hop, nt),
        in_specs=[ANY, ANY, VMEM, VMEM],
        out_specs=[ANY, VMEM],
        out_shape=[out_of(BF16, t, inner), out_of(F32, n_state, inner)],
        scratch_shapes=[scratch(BF16, 2, tm, d_model), scratch(BF16, 2, d_model, nt), scratch(BF16, 2, tm, nt), piece, piece,
                        sems(2, parts), sems(2, parts), two, sems(pieces), sems(pieces)],
        compiler_params=params(60, 2),
        cost_estimate=pl.CostEstimate(flops=t * inner * d_model, bytes_accessed=t * inner, transcendentals=0),
        name='z_chain',
    )(x_full, w_z, s_end, dec)


def out_kernel(chips, nb, wc, slots, zt, xact_ref, bc_ref, cum_ref, cl_ref, seg_ref, segp_ref, sloc_ref, pd_ref, sin_ref, z_ref, xf_ref, wz_ref,
               dskip_ref, nw_ref, wo_ref, wp_ref, x_ref, o_ref, recv_ref,
               va_own, va_par, wbuf, send, acc, rbuf, xo, xg, wzb, zb, xa, bca, sl, sbf, yoff, gated, dlane,
               vs_sem, vr_sem, w_sem, s_sem, r_sem, l_sem, x_sem, o_sem, c_sem, z_sem, v_sem):
    me = lax.axis_index('tp')
    chip, core = me // CORES, odd(me)
    partner = CORES * chip + flip(core)
    chip_at = lambda d: lax.rem(chip + d, chips)
    ring = [CORES * chip_at(chips - 1) + core, CORES * chip_at(1) + core]
    q = va_own.shape[1]
    inner = xa.shape[2]
    heads = cum_ref.shape[0]
    head_dim = inner // heads
    per = LANES // head_dim
    n_state = sl.shape[1]
    half_cols = nb * wc
    hops = chips - 1
    steps = hops * nb * 2
    lag = acc.shape[1] - 1
    depth = slots // 2
    hq = q // 2
    ready = greet([('tp', partner)] + [('tp', r) for r in ring])

    def cols_of(u):
        return rows_at(odd(u) * half_cols + lax.rem(u // 2, nb) * wc, wc)

    def w_copies(u):
        slot = odd(u)
        return [pltpu.make_async_copy(ref.at[:, cols_of(u)], wbuf.at[slot, i], w_sem.at[slot, i]) for i, ref in enumerate((wo_ref, wp_ref))]

    def place(n):
        return chip_at(jnp.where(n == 0, chips - 1, jnp.where(n == hops, 0, n)))

    def parity(i):
        return jnp.where(i == 0, flip(core), core)

    def load(n, i):
        c = CORES * place(n) + parity(i)
        at = rows_at(c * q, q)
        return [pltpu.make_async_copy(xact_ref.at[at, :], xa.at[i], c_sem.at[i, 0]), pltpu.make_async_copy(bc_ref.at[at, :], bca.at[i], c_sem.at[i, 1]),
                pltpu.make_async_copy(sloc_ref.at[c], sl.at[i], c_sem.at[i, 2]), pltpu.make_async_copy(z_ref.at[at, :], zb.at[parity(i)], c_sem.at[i, 3])]

    for i in PAIR:
        for cp in load(0, i):
            cp.start()
    for cp in w_copies(0):
        cp.start()
    x_copy = pltpu.make_async_copy(x_ref, xo, x_sem)
    dlane[...] = expand_heads(dskip_ref[...], head_dim)
    ready()

    def swap(n, j):
        return remote(va_own.at[chips + odd(n)], va_par.at[j], vs_sem.at[n], vr_sem.at[n], 'tp', partner)

    def mix(c, i, tgt):
        at = rows_at(c * q, q)
        seg_row = seg_ref[:, at]
        seg_prev = segp_ref[c][:, LANES - 1:]
        seg_rows = jnp.broadcast_to(seg_row, (q, q))
        causal = lax.broadcasted_iota(jnp.int32, (q, q), 0) >= lax.broadcasted_iota(jnp.int32, (q, q), 1)
        bias = jnp.where(causal & (seg_rows == seg_rows.T), 0.0, NEG)
        cum = cum_ref[:, at]
        cl = cl_ref[:, at]
        cum_cols = cum.T
        in_cols = jnp.where(seg_row == seg_prev, jnp.exp2(cum), 0.0).T
        sbf[...] = (sl[i] + pd_ref[c] * sin_ref[...]).astype(BF16)
        c_act = bca[i, :, n_state:]
        scores = lax.dot_general(c_act, bca[i, :, 0:n_state], (((1,), (1,)), ((), ())), preferred_element_type=F32)
        yoff[...] = dot32(c_act, sbf[...])
        lane = lax.broadcasted_iota(jnp.int32, (q, LANES), 1) // head_dim
        sq = jnp.zeros((q, LANES), F32)
        for m in range(inner // LANES):
            cols = slice(m * LANES, (m + 1) * LANES)
            x_f = xa[i, :, cols].astype(F32)
            tops, bots = [], []
            for j in range(per):
                h = m * per + j
                x_h = jnp.where(lane == j, x_f, 0.0).astype(BF16)
                ccol, crow = cum_cols[:, h:h + 1], cl[h:h + 1, :]
                m_top = jnp.exp2(ccol[0:hq] + bias[0:hq, 0:hq] - crow[:, 0:hq]) * scores[0:hq, 0:hq]
                m_bot = jnp.exp2(ccol[hq:] + bias[hq:] - crow) * scores[hq:]
                tops.append(dot32(m_top.astype(BF16), x_h[0:hq]))
                bots.append(dot32(m_bot.astype(BF16), x_h))
            y = jnp.concatenate([sum(tops), sum(bots)], axis=0)
            y = y + yoff[:, cols] * head_lanes(in_cols, m, head_dim) + dlane[:, cols] * x_f
            v = y * silu(zb[parity(i), :, cols].astype(F32))
            gated[:, cols] = v
            sq = sq + v * v
        inv = lax.rsqrt(jnp.sum(sq, axis=1, keepdims=True) * (1.0 / inner) + NORM_EPS)
        inv = jnp.broadcast_to(inv, (q, LANES))
        for m in range(inner // LANES):
            cols = slice(m * LANES, (m + 1) * LANES)
            va_own[tgt, :, cols] = (gated[:, cols] * inv * nw_ref[m:m + 1, :].astype(F32)).astype(BF16)

    def prep(n):
        j = place(n)
        tok = rows_at(j * (CORES * q), CORES * q)

        @pl.when(n >= 2)
        def _():
            for i in PAIR:
                for cp in load(n, i)[:3]:
                    cp.start()

            def wz_copy(m):
                return pltpu.make_async_copy(wz_ref.at[:, rows_at(m * zt, zt)], wzb.at[odd(m)], z_sem.at[odd(m)])
            rows_copy = pltpu.make_async_copy(xf_ref.at[tok, :], xg, v_sem)
            rows_copy.start()
            wz_copy(0).start()
            rows_copy.wait()

            def z_body(m, carry):
                wz_copy(m).wait()

                @pl.when(m + 1 < inner // zt)
                def _():
                    wz_copy(m + 1).start()
                res = dot32(xg[...], wzb[odd(m)]).astype(BF16)
                for p in PAIR:
                    zb[p, :, rows_at(m * zt, zt)] = res[p * q:(p + 1) * q]
                return carry
            lax.fori_loop(0, inner // zt, z_body, 0)

            swap(n - 2, j).wait_send()

        def chunk(i, carry):
            for cp in load(n, i)[:3]:
                cp.wait()

            @pl.when(n < 2)
            def _():
                load(n, i)[3].wait()
            mix(CORES * j + parity(i), i, jnp.where(i == 0, chips + odd(n), j))

            @pl.when(n == 0)
            def _():
                for cp in load(1, i):
                    cp.start()

            @pl.when(i == 0)
            def _():
                swap(n, j).start()
            return carry
        lax.fori_loop(0, CORES, chunk, 0)
        swap(n, j).wait_recv()

    def ring_copy(d, unit):
        slot = lax.rem(unit, slots)
        return remote(send.at[d, slot], recv_ref.at[d, unit], s_sem.at[d, slot], r_sem.at[d, unit], 'tp', jnp.where(d == 0, ring[1], ring[0]))

    def fetch(d, unit):
        ring_copy(d, unit).wait_recv()
        cp = pltpu.make_async_copy(recv_ref.at[d, unit], rbuf, l_sem)
        cp.start()
        cp.wait()

    def o_copy(d, b):
        cols = rows_at(d * half_cols + b * wc, wc)
        return pltpu.make_async_copy(xo.at[:, cols], o_ref.at[:, cols], o_sem.at[d, b])

    def product(dest, slot):
        return dot32(va_own[dest], wbuf[slot, 0]) + dot32(va_par[dest], wbuf[slot, 1])

    def finish(d, b):
        fetch(d, (hops - 1) * nb + b)
        cols = rows_at(d * half_cols + b * wc, wc)
        xo[:, cols] = (xo[:, cols].astype(F32) + (acc[d, lax.rem(b, lag + 1)] + rbuf[...])).astype(BF16)
        o_copy(d, b).start()

    def body(u, carry):
        d = odd(u)
        k = u // (2 * nb)
        b = lax.rem(u // 2, nb)
        unit = k * nb + b
        ending = k == hops - 1

        @pl.when((u < 2) | ((b == 0) & (d == 0)))
        def _():
            prep(jnp.where(u < 2, u, k + 1))
        dest = chip_at(jnp.where(d == 0, 2 * chips - 1 - k, 1 + k))
        for cp in w_copies(u):
            cp.wait()

        @pl.when(u + 1 < steps)
        def _():
            for cp in w_copies(u + 1):
                cp.start()

        @pl.when(u == 2)
        def _():
            x_copy.start()
        part = product(dest, d)
        slot = lax.rem(unit, slots)

        @pl.when((unit >= slots) & (flip(ending) | (b < slots - depth)))
        def _():
            ring_copy(d, unit - slots).wait_send()

        @pl.when(ending)
        def _():
            ring_copy(d, unit - depth).wait_send()

        @pl.when(k == 0)
        def _():
            send[d, slot] = part

        @pl.when(k > 0)
        def _():
            fetch(d, unit - nb)
            send[d, slot] = part + rbuf[...]
        ring_copy(d, unit).start()

        @pl.when(ending)
        def _():
            acc[d, lax.rem(b, lag + 1)] = product(chip, d)

            @pl.when(b == 0)
            def _():
                pl.when(d == 0)(x_copy.wait)

            @pl.when(b >= lag)
            def _():
                finish(d, b - lag)
        return carry

    lax.fori_loop(0, steps, body, 0)

    def tail(i, carry):
        finish(odd(i), nb - lag + i // 2)
        return carry

    def drain(i, carry):
        o_copy(odd(i), i // 2).wait()
        return carry

    def drain_send(i, carry):
        ring_copy(odd(i), hops * nb - depth + i // 2).wait_send()
        return carry
    lax.fori_loop(0, 2 * lag, tail, 0)
    lax.fori_loop(0, 2 * depth, drain_send, 0)
    for n in PAIR:
        swap(2 + n, chip).wait_send()
    lax.fori_loop(0, 2 * nb, drain, 0)


def out_proj_scatter(x_act, bc_act, cum, cl, seg_row, seg_prev, sloc, pd, s_in, z_arr, x_full, w_z, d_skip, norm_w, w_own, w_par, x_loc, chips, wc=512, slots=4, zt=256):
    t, inner = x_act.shape
    rows, d_model = x_loc.shape
    gw = bc_act.shape[1]
    n_state = s_in.shape[0]
    nb = d_model // 2 // wc
    units = (chips - 1) * nb
    return pl.pallas_call(
        functools.partial(out_kernel, chips, nb, wc, slots, zt),
        in_specs=[ANY, ANY, VMEM, VMEM, VMEM, VMEM, ANY, VMEM, VMEM, ANY, ANY, ANY, VMEM, VMEM, ANY, ANY, ANY],
        out_specs=[ANY, ANY],
        out_shape=[out_of(BF16, rows, d_model), out_of(F32, 2, units, rows, wc)],
        scratch_shapes=[scratch(BF16, chips + 2, rows, inner), scratch(BF16, chips, rows, inner), scratch(BF16, 2, 2, inner, wc), scratch(F32, 2, slots, rows, wc), scratch(F32, 2, slots, rows, wc),
                        scratch(F32, rows, wc), scratch(BF16, rows, d_model), scratch(BF16, CORES * rows, d_model), scratch(BF16, 2, d_model, zt),
                        scratch(BF16, CORES, rows, inner), scratch(BF16, 2, rows, inner), scratch(BF16, 2, rows, gw), scratch(F32, 2, n_state, inner),
                        scratch(BF16, n_state, inner), scratch(F32, rows, inner), scratch(F32, rows, inner), scratch(F32, 1, inner),
                        sems(chips), sems(chips), sems(2, 2), sems(2, slots), sems(2, units), DMA, DMA, sems(2, nb), sems(2, 4), sems(2), DMA],
        compiler_params=params(63, 1),
        cost_estimate=pl.CostEstimate(flops=2 * t * inner * d_model, bytes_accessed=t * d_model, transcendentals=0),
        name='out_proj_scatter',
    )(x_act, bc_act, cum, cl, seg_row, seg_prev, sloc, pd, s_in, z_arr, x_full, w_z, d_skip, norm_w, w_own, w_par, x_loc)[0]


def layer(x_loc, seg_loc, w_zx, w_bc, w_dt, conv_x, conv_bc, bias_x, bias_bc, a_log, dt_bias, d_skip, norm_w, w_out, chips, blocks):
    rows = x_loc.shape[0]
    tiled = lambda v: v.reshape(v.shape[0] // LANES, LANES)
    x_full, x_pre, small, w_z, w_par, seg, seg_tail, tail_x, tail_b = gather_proj(x_loc, w_zx, w_bc, w_dt.T, w_out, seg_loc[None], chips, blocks)
    x_act, bc_act, cum, cl, seg_row, seg_prev, sloc, pd, s_end, dec = phase_a(
        x_pre, small, seg, seg_tail, tail_x, tail_b, conv_x, conv_bc, tiled(bias_x), bias_bc, a_log[None], dt_bias[None], rows)
    z_arr, s_in = z_chain(x_full, w_z, s_end, dec, chips, blocks)
    return out_proj_scatter(x_act, bc_act, cum, cl, seg_row, seg_prev, sloc, pd, s_in, z_arr, x_full, w_z, d_skip[None], tiled(norm_w), w_out, w_par, x_loc, chips)


def solution(mesh):
    tokens = ('dp', 'sp', 'tp')
    heads = P('tp')
    cols = P(None, 'tp')
    deep = P(None, None, 'tp')
    specs = (P(tokens, None), P(tokens), deep, deep, cols, cols, deep, heads, cols, heads, heads, heads, heads, P('tp', None))
    body = functools.partial(layer, chips=mesh.shape['tp'] // CORES, blocks=mesh.shape['sp'])
    return jax.shard_map(body, mesh=mesh, in_specs=specs, out_specs=specs[0], check_vma=False)
```

```python
import functools
import jax
import jax.numpy as jnp
from jax import lax
from jax.experimental import pallas as pl
from jax.experimental.pallas import tpu as pltpu
from jax.sharding import PartitionSpec as P

MESH = pl.DeviceIdType.MESH
NORM_EPS = 1e-5
LOG2E = 1.4426950408889634
FAR = -1e6
NEG = -1e30
F32 = jnp.float32
BF16 = jnp.bfloat16
HI = lax.Precision.HIGHEST
MIB = 2 ** 20
LANES = 128
ROW8 = 8
CORES = 2
DIRS = 2
PAIR = range(2)
ANY = pl.BlockSpec(memory_space=pl.ANY)
VMEM = pl.BlockSpec(memory_space=pltpu.VMEM)
DMA = pltpu.SemaphoreType.DMA


def scratch(dtype, *shape):
    return pltpu.VMEM(shape, dtype)


def out_of(dtype, *shape):
    return jax.ShapeDtypeStruct(shape, dtype)


def sems(*shape):
    return DMA(shape)


def rows_at(start, size):
    return pl.ds(pl.multiple_of(start, size), size)


def odd(i):
    return lax.rem(i, 2)


def flip(i):
    return 1 - i


def dot32(a, b):
    return jnp.dot(a, b, preferred_element_type=F32)


def params(limit, name_id=None):
    if name_id is None:
        return pltpu.CompilerParams(dimension_semantics=('arbitrary',), vmem_limit_bytes=limit * MIB)
    return pltpu.CompilerParams(collective_id=name_id, has_side_effects=True, vmem_limit_bytes=limit * MIB)


def greet(peers):
    barrier = pltpu.get_barrier_semaphore()
    for axis, index in peers:
        pl.semaphore_signal(barrier, inc=1, device_id={axis: index}, device_id_type=MESH)
    return lambda: pl.semaphore_wait(barrier, len(peers))


def remote(src, dst, send, recv, axis, index):
    return pltpu.make_async_remote_copy(src_ref=src, dst_ref=dst, send_sem=send, recv_sem=recv, device_id={axis: index}, device_id_type=MESH)


def silu(v):
    h = v * 0.5
    return h + h * jnp.tanh(h)


def head_lanes(cols, tile_idx, head_dim):
    rows = cols.shape[0]
    per = LANES // head_dim
    lane = lax.broadcasted_iota(jnp.int32, (rows, LANES), 1)
    out = None
    for j in range(per):
        h = tile_idx * per + j
        nxt = jnp.broadcast_to(cols[:, h:h + 1], (rows, LANES))
        out = nxt if out is None else jnp.where(lane >= j * head_dim, nxt, out)
    return out


def expand_heads(row, head_dim):
    heads = row.shape[1]
    shape = (heads, heads * head_dim)
    eye = (lax.broadcasted_iota(jnp.int32, shape, 1) // head_dim == lax.broadcasted_iota(jnp.int32, shape, 0)).astype(F32)
    return jnp.dot(jnp.broadcast_to(row, (ROW8, heads)), eye, precision=HI, preferred_element_type=F32)[0:1]


def column(row):
    return jnp.broadcast_to(row, (LANES, row.shape[1])).T[:, 0:1]


def gather_kernel(chips, blocks, kb, nb, sub, nt, pace, x_ref, wzx_ref, wbc_ref, wdt_ref, wo_ref, seg_ref,
                  xf_ref, xp_ref, bp_ref, wz_ref, wp_ref, segf_ref, segt_ref, tx_ref, tb_ref,
                  wx, wsm, xg, ost, bst, blk, bblk, zst, wdt,
                  ra_sem, rd_sem, so_sem, sf_sem, sd_sem, xl_sem, xs_sem, in_sem, zo_sem, bb_sem, dt_sem, oo_sem, bo_sem,
                  wp_sem, sg_sem, sr_sem, st_sem, hx_sem, hb_sem):
    me = lax.axis_index('tp')
    blk_id = lax.axis_index('sp')
    chip, core = me // CORES, odd(me)
    partner = CORES * chip + flip(core)
    near = [lax.rem(chip + chips - 1, chips), lax.rem(chip + 1, chips)]
    far = lax.rem(chip + chips // CORES, chips)
    ring = [CORES * c + core for c in near]
    sp_next = lax.rem(blk_id + 1, blocks)
    n_tp = CORES * chips
    rows = x_ref.shape[0]
    quarters = xl_sem.shape[1]
    qr = rows // quarters
    d_model, inner = wx.shape
    heads = wdt.shape[0]
    n_state = bblk.shape[3]
    nk = d_model // kb
    nblk = nk * (inner // nb)
    opp = CORES + quarters
    last = opp + quarters // CORES - 1
    ready = greet([('tp', lax.rem(me + d, n_tp)) for d in range(1, n_tp)] + [('sp', sp_next), ('sp', lax.rem(blk_id + blocks - 1, blocks))])

    def row_of(lv, b):
        side = odd(b)
        other = jnp.where(lv < CORES, lv, b // CORES)
        cc = jnp.where(other == 1, flip(core), core)
        ch = jnp.where(lv < CORES, chip, jnp.where(lv >= opp, far, jnp.where(side == 0, near[0], near[1])))
        q = jnp.where(lv < CORES, b, jnp.where(lv >= opp, side * (quarters // CORES) + lv - opp, lv - CORES))
        return (CORES * ch + cc) * rows + q * qr

    def full_rows(lv, b, size=qr):
        return xf_ref.at[rows_at(row_of(lv, b), size), :]

    def w_tile(i):
        return rows_at(lax.rem(i, nk) * kb, kb), rows_at((i // nk) * nb, nb)

    def blk_copy(i):
        kk, nn = w_tile(i)
        slot = lax.rem(i, blk.shape[0])
        return pltpu.make_async_copy(wzx_ref.at[kk, :, nn], blk.at[slot], in_sem.at[slot])

    def z_copy(i):
        kk, nn = w_tile(i)
        return pltpu.make_async_copy(zst.at[odd(i)], wz_ref.at[kk, nn], zo_sem.at[odd(i)])

    def bc_copy(i):
        return pltpu.make_async_copy(wbc_ref.at[rows_at(i * kb, kb)], bblk.at[odd(i)], bb_sem.at[odd(i)])

    own_load = pltpu.make_async_copy(x_ref, xg.at[0], xs_sem.at[0])
    dt_load = pltpu.make_async_copy(wdt_ref, wdt, dt_sem)
    own_load.start()
    dt_load.start()
    bc_copy(0).start()
    for i in range(blk.shape[0]):
        blk_copy(i).start()
    ready()

    def own_send(q, to):
        return remote(x_ref.at[rows_at(q * qr, qr), :], full_rows(0, q), so_sem.at[to, q], ra_sem.at[CORES + q, flip(to)], 'tp', ring[to])

    own_pair = remote(x_ref, full_rows(0, 0, rows), sd_sem.at[1, 0], rd_sem.at[1, 0], 'tp', partner)

    def pair_send(lv, side):
        return remote(full_rows(lv, side), full_rows(lv, side), sd_sem.at[lv, side], rd_sem.at[lv, side], 'tp', partner)

    def forward(lv, to):
        side = flip(to)
        h = lax.rem(lv - CORES, quarters // CORES)
        dst_sem = ra_sem.at[opp + h, side]
        return remote(full_rows(lv, side), full_rows(lv, side), sf_sem.at[to, h], dst_sem, 'tp', ring[to])

    def arrival(lv, side):
        return remote(full_rows(lv, side), full_rows(lv, side), so_sem.at[0, 0], ra_sem.at[lv, side], 'tp', ring[0])

    def pair_arrival(lv, side):
        ref = full_rows(lv, CORES + side)
        return remote(ref, ref, sd_sem.at[1, 0], rd_sem.at[lv, side], 'tp', partner)

    pair_own_arrival = remote(full_rows(1, 0, rows), full_rows(1, 0, rows), sd_sem.at[1, 0], rd_sem.at[1, 0], 'tp', partner)

    def send_quarter(q):
        for to in PAIR:
            own_send(q, flip(to)).start()
    send_quarter(0)
    own_pair.start()

    def seg_cols(index):
        return segf_ref.at[:, rows_at(index * rows, rows)]

    def seg_send(d):
        return remote(seg_ref, seg_cols(me), sg_sem.at[d], sr_sem.at[d], 'tp', lax.rem(me + d, n_tp))

    def seg_arrival(d):
        return remote(seg_ref, seg_cols(lax.rem(me + n_tp - d, n_tp)), sg_sem.at[d], sr_sem.at[d], 'tp', lax.rem(me + d, n_tp))

    seg_own = pltpu.make_async_copy(seg_ref, seg_cols(me), sg_sem.at[0])
    seg_own.start()
    for d in range(1, n_tp):
        seg_send(d).start()
    w_swap = remote(wo_ref, wp_ref, wp_sem.at[0], wp_sem.at[1], 'tp', partner)
    w_swap.start()
    seg_halo = remote(segf_ref.at[:, pl.ds(n_tp * rows - LANES, LANES)], segt_ref, st_sem.at[0], st_sem.at[1], 'sp', sp_next)

    end_chip = chips - 1
    hrows = tx_ref.shape[0]
    halo_lv = jnp.where(chip == end_chip, flip(core), jnp.where(far == end_chip, last, opp - 1))
    halo_b = jnp.where(chip == end_chip, quarters - 1, jnp.where((far != end_chip) & (near[0] == end_chip), 0, 1) + CORES * flip(core))

    def halo_copies(slot):
        src = rows_at(halo_b * qr + qr - hrows, hrows)
        return [remote(ost.at[slot, src, :], tx_ref, hx_sem.at[0], hx_sem.at[1], 'sp', sp_next),
                remote(bst.at[slot, src, :], tb_ref, hb_sem.at[0], hb_sem.at[1], 'sp', sp_next)]

    dt_load.wait()

    def small_body(i, carry):
        bc_copy(i).wait()

        @pl.when(i + 1 < nk)
        def _():
            bc_copy(i + 1).start()

        def inner_body(s, carry2):
            part = jnp.swapaxes(bblk[odd(i), rows_at(s * sub, sub)], 0, 1)
            at = rows_at(i * kb + s * sub, sub)
            for g in PAIR:
                wsm[at, g * n_state:(g + 1) * n_state] = part[g]
            wd = jnp.concatenate([wdt[:, at].astype(F32), jnp.zeros((LANES - heads, sub), F32)], axis=0)
            wsm[at, CORES * n_state:] = wd.T.astype(BF16)
            return carry2
        return lax.fori_loop(0, kb // sub, inner_body, carry)
    lax.fori_loop(0, nk, small_body, 0)

    def relay(i, carry):
        slot = lax.rem(i, blk.shape[0])
        blk_copy(i).wait()

        @pl.when(i >= CORES)
        def _():
            z_copy(i - CORES).wait()
        kk = lax.rem(i, nk) * kb

        def inner_body(s, carry2):
            at = rows_at(s * sub, sub)
            part = jnp.swapaxes(blk[slot, at].astype(F32), 0, 1)
            zst[odd(i), at, :] = part[0].astype(BF16)
            wx[rows_at(kk + s * sub, sub), w_tile(i)[1]] = part[1].astype(BF16)
            return carry2
        lax.fori_loop(0, kb // sub, inner_body, 0)
        z_copy(i).start()
        for q in range(1, quarters - 1):
            pl.when(i == q * pace - 1)(functools.partial(send_quarter, q))

        @pl.when(i + blk.shape[0] < nblk)
        def _():
            blk_copy(i + blk.shape[0]).start()
        return carry
    lax.fori_loop(0, nblk, relay, 0)

    seg_own.wait()
    for d in range(1, n_tp):
        seg_arrival(d).wait_recv()
    seg_halo.start()
    own_load.wait()
    own_store = pltpu.make_async_copy(xg.at[0], full_rows(0, 0, rows), xs_sem.at[1])
    own_store.start()

    def load(lv, b):
        return pltpu.make_async_copy(full_rows(lv, b), xg.at[odd(lv), rows_at(b * qr, qr), :], xl_sem.at[odd(lv), b])

    def take(lv):
        @pl.when(lv >= CORES)
        def _():
            for side in PAIR:
                arrival(lv, side).wait_recv()
                pair_send(lv, side).start()

    def fetch(lv):
        @pl.when(lv == 1)
        def _():
            pair_own_arrival.wait_recv()

        @pl.when(lv >= CORES)
        def _():
            for side in PAIR:
                pair_arrival(lv, side).wait_recv()
        for b in range(quarters):
            load(lv, b).start()

    def out_copies(lv):
        slot = odd(lv)
        res = []
        for b in range(quarters):
            src, dst = rows_at(b * qr, qr), rows_at(row_of(lv, b), qr)
            res.append(pltpu.make_async_copy(ost.at[slot, src, :], xp_ref.at[dst, :], oo_sem.at[slot, b]))
            res.append(pltpu.make_async_copy(bst.at[slot, src, :], bp_ref.at[dst, :], bo_sem.at[slot, b]))
        return res

    early = opp - 1
    cut = CORES + quarters // CORES

    def feed(lv):
        @pl.when(lv == 1)
        def _():
            send_quarter(quarters - 1)
        for h in range(quarters // CORES):
            @pl.when(lv == 3 + CORES * h)
            def _(h=h):
                forward(CORES + h, 1).start()
                forward(cut + h, 0).start()

    def round_body(lv, carry):
        slot = odd(lv)

        @pl.when(lv > 0)
        def _():
            for b in range(quarters):
                load(lv, b).wait()

        @pl.when(lv == 1)
        def _():
            own_store.wait()

        @pl.when(lv < early)
        def _():
            take(lv + 1)

        @pl.when(lv >= CORES)
        def _():
            for cp in out_copies(lv - CORES):
                cp.wait()

        def dots(n, carry2):
            @pl.when(n == inner // nt // CORES)
            def _():
                feed(lv)

                @pl.when(lv < early)
                def _():
                    fetch(lv + 1)
            cols = rows_at(n * nt, nt)
            ost[slot, :, cols] = dot32(xg[slot], wx[:, cols]).astype(BF16)
            return carry2
        lax.fori_loop(0, inner // nt, dots, 0)
        bst[slot] = dot32(xg[slot], wsm[...]).astype(BF16)
        for cp in out_copies(lv):
            cp.start()

        @pl.when(lv == halo_lv + 1)
        def _():
            for cp in halo_copies(flip(slot)):
                cp.wait_send()

        @pl.when(lv == halo_lv)
        def _():
            for cp in halo_copies(slot):
                cp.start()

        @pl.when((lv >= early) & (lv < last))
        def _():
            take(lv + 1)
            fetch(lv + 1)
        return carry
    lax.fori_loop(0, last + 1, round_body, 0)

    @pl.when(halo_lv == last)
    def _():
        for cp in halo_copies(last % CORES):
            cp.wait_send()
    for cp in halo_copies(0):
        cp.wait_recv()
    seg_halo.wait()
    for d in range(1, n_tp):
        seg_send(d).wait_send()
    w_swap.wait()
    for i in PAIR:
        for cp in out_copies(last - i):
            cp.wait()
        z_copy(nblk - 1 - i).wait()
    own_pair.wait_send()
    for to in PAIR:
        for q in range(quarters):
            own_send(q, to).wait_send()
        for h in range(quarters // CORES):
            forward(CORES + h, to).wait_send()
    for lv in range(CORES, last + 1):
        for side in PAIR:
            pair_send(lv, side).wait_send()


def gather_proj(x_loc, w_zx, w_bc, w_dt_t, w_out, seg, chips, blocks, kb=2048, nb=256, sub=256, nt=512, quarters=4, pace=12):
    rows, d_model = x_loc.shape
    inner, n_state, heads = w_zx.shape[CORES], w_bc.shape[CORES], w_dt_t.shape[0]
    n_tp = CORES * chips
    t = rows * n_tp
    small = CORES * n_state + LANES
    lv = CORES + quarters + quarters // CORES
    halo = 16
    two = sems(CORES)
    return pl.pallas_call(
        functools.partial(gather_kernel, chips, blocks, kb, nb, sub, nt, pace),
        in_specs=[ANY] * 6,
        out_specs=[ANY] * 9,
        out_shape=[out_of(BF16, t, d_model), out_of(BF16, t, inner), out_of(BF16, t, small), out_of(BF16, d_model, inner), out_of(BF16, *w_out.shape),
                   out_of(jnp.int32, 1, t), out_of(jnp.int32, 1, LANES), out_of(BF16, halo, inner), out_of(BF16, halo, small)],
        scratch_shapes=[scratch(BF16, d_model, inner), scratch(BF16, d_model, small), scratch(BF16, CORES, rows, d_model),
                        scratch(BF16, CORES, rows, inner), scratch(BF16, CORES, rows, small), scratch(BF16, 3, kb, CORES, nb),
                        scratch(BF16, CORES, kb, CORES, n_state), scratch(BF16, CORES, kb, nb), scratch(BF16, heads, d_model),
                        sems(lv, CORES), sems(lv, CORES), sems(CORES, quarters), sems(CORES, quarters), sems(lv, CORES), sems(CORES, quarters), two, sems(3), two, two, DMA,
                        sems(CORES, quarters), sems(CORES, quarters), two, sems(n_tp), sems(n_tp), two, two, two],
        compiler_params=params(63, 0),
        cost_estimate=pl.CostEstimate(flops=t * inner * d_model, bytes_accessed=t * inner, transcendentals=0),
        name='gather_proj',
    )(x_loc, w_zx, w_bc, w_dt_t, w_out, seg)


def phase_a_kernel(q, x_ref, small_ref, seg_ref, segt_ref, tailx_ref, tailb_ref, cx_ref, cbc_ref, bx_ref, bbc_ref, alog_ref, dtb_ref,
                   xact_ref, bcact_ref, cum_ref, cl_ref, segf_ref, segp_ref, sloc_ref, pd_ref, send_ref, dec_ref,
                   pad, xw, segtail, base, cw):
    inner = x_ref.shape[1]
    gw = bcact_ref.shape[1]
    n_state = gw // 2
    heads = alog_ref.shape[1]
    head_dim = inner // heads
    taps = cx_ref.shape[0]

    @pl.when(pl.program_id(0) == 0)
    def _():
        first = lax.axis_index('sp') == 0
        base[...] = jnp.broadcast_to(jnp.where(first, seg_ref[:, 0:1], segt_ref[:, LANES - 1:]), base.shape)
        segtail[...] = jnp.where(first, FAR, (segt_ref[...] - base[...]).astype(F32))
        pad[0:ROW8, 0:inner] = tailx_ref[...].astype(F32)[ROW8:]
        pad[0:ROW8, inner:] = tailb_ref[:, 0:gw].astype(F32)[ROW8:]
        cw[0:taps, 0:inner] = cx_ref[...].astype(F32)
        for i in range(inner // LANES):
            cw[taps:taps + 1, i * LANES:(i + 1) * LANES] = bx_ref[i:i + 1, :].astype(F32)
        for g in PAIR:
            cols = slice(inner + g * n_state, inner + (g + 1) * n_state)
            cw[0:taps, cols] = cbc_ref[:, g, :].astype(F32)
            cw[taps:taps + 1, cols] = bbc_ref[g:g + 1, :].astype(F32)
        send_ref[...] = jnp.zeros_like(send_ref)
        dec_ref[...] = jnp.ones_like(dec_ref)

    @pl.when(pl.program_id(0) > 0)
    def _():
        pad[0:ROW8, :] = pad[q:q + ROW8, :]

    pad[ROW8:, 0:inner] = x_ref[...].astype(F32)
    pad[ROW8:, inner:] = small_ref[:, 0:gw].astype(F32)
    seg_row = (seg_ref[...] - base[:, 0:1]).astype(F32)
    prev_row = segtail[...]
    segf_ref[...] = seg_row
    segp_ref[0] = prev_row
    segtail[...] = seg_row[:, q - LANES:]
    ext = jnp.concatenate([prev_row, seg_row], axis=1)
    seg_last, seg_prev = seg_row[:, q - 1:], prev_row[:, LANES - 1:]
    keeps = []
    for j in range(1, taps):
        keep_row = jnp.where(ext[:, LANES - j:LANES - j + q] == seg_row, 1.0, 0.0)
        keeps.append(jnp.broadcast_to(keep_row, (LANES, q)).T)
    raw = small_ref[:, gw:].astype(F32).T[0:heads] + column(dtb_ref[...])
    dt = jnp.maximum(raw, 0.0) + jnp.log1p(jnp.exp(-jnp.abs(raw)))
    log_a = dt * column(jnp.exp(alog_ref[...]) * -LOG2E)
    tri = (lax.broadcasted_iota(jnp.int32, (q, q), 0) <= lax.broadcasted_iota(jnp.int32, (q, q), 1)).astype(F32)
    cum = jnp.dot(log_a, tri, precision=HI, preferred_element_type=F32)
    cum_ref[...] = cum
    cl_ref[...] = cum - jnp.log(dt) * LOG2E
    cum_last = cum[:, q - 1:]
    end_cols = (jnp.where(seg_row == seg_last, jnp.exp2(cum_last - cum), 0.0) * dt).T
    carry = jnp.where(seg_last == seg_prev, jnp.exp2(cum_last), 0.0)
    carry_lane = expand_heads(jnp.broadcast_to(carry, (heads, LANES)).T[0:1], head_dim)
    for i in range((inner + gw) // LANES):
        cols = slice(i * LANES, (i + 1) * LANES)
        src = pad[:, cols]
        acc = cw[taps:taps + 1, cols] + src[ROW8:] * cw[taps - 1:taps, cols]
        for j in range(1, taps):
            at = taps - 1 - j
            acc = acc + pltpu.roll(src, j, axis=0)[ROW8:] * cw[at:at + 1, cols] * keeps[j - 1]
        act = silu(acc).astype(BF16)
        if i * LANES < inner:
            xact_ref[:, cols] = act
            xw[:, cols] = (act.astype(F32) * head_lanes(end_cols, i, head_dim)).astype(BF16)
        else:
            bcact_ref[:, i * LANES - inner:(i + 1) * LANES - inner] = act
    sloc_ref[0] = send_ref[...]
    pd_ref[0] = dec_ref[...]
    send_ref[...] = carry_lane * send_ref[...] + dot32(bcact_ref[:, 0:n_state].T, xw[...])
    dec_ref[...] = dec_ref[...] * carry_lane


def phase_a(x_pre, small, seg, seg_tail, tail_x, tail_b, conv_x, conv_bc, bias_x, bias_bc, a_log, dt_bias, q):
    t, inner = x_pre.shape
    n_state = conv_bc.shape[2]
    gw = CORES * n_state
    heads = a_log.shape[1]
    nt = t // q

    def full(shape):
        return pl.BlockSpec(shape, lambda c: (0,) * len(shape))

    def by_row(width):
        return pl.BlockSpec((q, width), lambda c: (c, 0))

    def by_col(height):
        return pl.BlockSpec((height, q), lambda c: (0, c))

    def by_chunk(a, b):
        return pl.BlockSpec((1, a, b), lambda c: (c, 0, 0))

    rest = (seg_tail, tail_x, tail_b, conv_x, conv_bc, bias_x, bias_bc, a_log, dt_bias)
    return pl.pallas_call(
        functools.partial(phase_a_kernel, q),
        grid=(nt,),
        in_specs=[by_row(inner), by_row(small.shape[1]), by_col(1)] + [full(v.shape) for v in rest],
        out_specs=[by_row(inner), by_row(gw), by_col(heads), by_col(heads), by_col(1), by_chunk(1, LANES), by_chunk(n_state, inner), by_chunk(1, inner),
                   full((n_state, inner)), full((1, inner))],
        out_shape=[out_of(BF16, t, inner), out_of(BF16, t, gw), out_of(F32, heads, t), out_of(F32, heads, t), out_of(F32, 1, t), out_of(F32, nt, 1, LANES),
                   out_of(F32, nt, n_state, inner), out_of(F32, nt, 1, inner), out_of(F32, n_state, inner), out_of(F32, 1, inner)],
        scratch_shapes=[scratch(F32, q + ROW8, inner + gw), scratch(BF16, q, inner), scratch(F32, 1, LANES),
                        scratch(jnp.int32, 1, LANES), scratch(F32, ROW8, inner + gw)],
        compiler_params=params(56),
        cost_estimate=pl.CostEstimate(flops=t * inner * gw, bytes_accessed=t * inner, transcendentals=0),
        name='phase_a',
    )(x_pre, small, seg, *rest)


def chain_kernel(chips, blocks, pieces, hop, gap, nt, xf_ref, wz_ref, send_ref, dec_ref, z_ref, sin_ref,
                 xg, wzb, zst, sbuf, rbuf, x_sem, w_sem, z_sem, s_sem, r_sem):
    chip = lax.axis_index('tp') // CORES
    blk_id = lax.axis_index('sp')
    sp_next = lax.rem(blk_id + 1, blocks)
    ready = greet([('sp', sp_next), ('sp', lax.rem(blk_id + blocks - 1, blocks))])
    n_state, inner = send_ref.shape
    tm = xg.shape[1]
    nn = inner // nt
    tiles = nn + nn // CORES
    pw = inner // pieces
    parts = range(x_sem.shape[1])
    kw = xg.shape[2] // len(parts)

    def tok(g):
        return rows_at(lax.rem(chip + jnp.where(g == 0, chips // 2, 1), chips) * tm, tm)

    def col(i):
        return rows_at(lax.rem(i, nn) * nt, nt)

    def depth(s):
        return pl.ds(s * kw, kw)

    def x_copy(g, s):
        return pltpu.make_async_copy(xf_ref.at[tok(g), depth(s)], xg.at[g, :, depth(s)], x_sem.at[g, s])

    def w_copy(i, s):
        return pltpu.make_async_copy(wz_ref.at[depth(s), col(i)], wzb.at[odd(i), depth(s), :], w_sem.at[odd(i), s])

    def z_copy(i):
        return pltpu.make_async_copy(zst.at[odd(i)], z_ref.at[tok(i // nn), col(i)], z_sem.at[odd(i)])

    def hop_copy(p):
        return remote(sbuf.at[p], rbuf.at[p], s_sem.at[p], r_sem.at[p], 'sp', sp_next)

    for s in parts:
        x_copy(0, s).start()
        w_copy(0, s).start()
    ready()

    def pass_on(j):
        lead = j - hop * blk_id
        p = lead // gap

        @pl.when((lead >= 0) & (lax.rem(lead, gap) == 0) & (p < pieces))
        def _():
            cols = rows_at(p * pw, pw)

            @pl.when(blk_id == 0)
            def _():
                sbuf[p] = send_ref[:, cols]
                sin_ref[:, cols] = jnp.zeros((n_state, pw), F32)

            @pl.when(blk_id > 0)
            def _():
                hop_copy(p).wait_recv()
                prev = rbuf[p]
                sin_ref[:, cols] = prev
                sbuf[p] = dec_ref[:, cols] * prev + send_ref[:, cols]

            @pl.when(blk_id < blocks - 1)
            def _():
                hop_copy(p).start()

    def tile(i):
        g = i // nn

        @pl.when(i >= 2)
        def _():
            z_copy(i - 2).wait()
        res = 0.0
        for s in parts:
            @pl.when(lax.rem(i, nn) == 0)
            def _(s=s):
                x_copy(g, s).wait()
            w_copy(i, s).wait()

            @pl.when(i + 1 < tiles)
            def _(s=s):
                w_copy(i + 1, s).start()
            pl.when(i == 1)(x_copy(1, s).start)
            pass_on(i * len(parts) + s)
            res = res + dot32(xg[g, :, depth(s)], wzb[odd(i), depth(s), :])
        zst[odd(i)] = res.astype(BF16)
        z_copy(i).start()

    steps = hop * (blocks - 1) + gap * (pieces - 1) + 1
    lax.fori_loop(0, tiles, lambda i, carry: (tile(i), carry)[1], 0)
    lax.fori_loop(tiles * len(parts), steps, lambda j, carry: (pass_on(j), carry)[1], 0)

    for i in PAIR:
        z_copy(tiles - 1 - i).wait()

    @pl.when(blk_id < blocks - 1)
    def _():
        for p in range(pieces):
            hop_copy(p).wait_send()


def z_chain(x_full, w_z, s_end, dec, chips, blocks, pieces=8, hop=5, gap=2, nt=512, parts=4):
    t, d_model = x_full.shape
    n_state, inner = s_end.shape
    tm = t // chips
    piece = scratch(F32, pieces, n_state, inner // pieces)
    two = sems(2)
    return pl.pallas_call(
        functools.partial(chain_kernel, chips, blocks, pieces, hop, gap, nt),
        in_specs=[ANY, ANY, VMEM, VMEM],
        out_specs=[ANY, VMEM],
        out_shape=[out_of(BF16, t, inner), out_of(F32, n_state, inner)],
        scratch_shapes=[scratch(BF16, 2, tm, d_model), scratch(BF16, 2, d_model, nt), scratch(BF16, 2, tm, nt), piece, piece,
                        sems(2, parts), sems(2, parts), two, sems(pieces), sems(pieces)],
        compiler_params=params(60, 2),
        cost_estimate=pl.CostEstimate(flops=t * inner * d_model, bytes_accessed=t * inner, transcendentals=0),
        name='z_chain',
    )(x_full, w_z, s_end, dec)


def out_kernel(chips, nb, wc, slots, zt, zlast, xact_ref, bc_ref, cum_ref, cl_ref, seg_ref, segp_ref, sloc_ref, pd_ref, sin_ref, z_ref, xf_ref, wz_ref,
               dskip_ref, nw_ref, wo_ref, wp_ref, x_ref, o_ref, recv_ref,
               va_own, va_par, wbuf, send, acc, rbuf, xo, xg, wzb, zb, xa, bca, sl, sbf, yoff, gated, dlane,
               vs_sem, vr_sem, w_sem, s_sem, r_sem, l_sem, x_sem, o_sem, c_sem, z_sem, v_sem):
    me = lax.axis_index('tp')
    chip, core = me // CORES, odd(me)
    partner = CORES * chip + flip(core)
    chip_at = lambda d: lax.rem(chip + d, chips)
    ring = [CORES * chip_at(chips - 1) + core, CORES * chip_at(1) + core]
    q = va_own.shape[1]
    inner = xa.shape[DIRS]
    heads = cum_ref.shape[0]
    head_dim = inner // heads
    per = LANES // head_dim
    n_state = sl.shape[1]
    half_cols = nb * wc
    hops = chips - 1
    steps = hops * nb * DIRS
    lag = acc.shape[1] - 1
    depth = slots // DIRS
    hq = q // DIRS
    ready = greet([('tp', partner)] + [('tp', r) for r in ring])

    def cols_of(u):
        d = odd(u)
        side = jnp.where(u < DIRS * nb * (hops - 1), d, flip(d))
        return rows_at(side * half_cols + lax.rem(u // DIRS, nb) * wc, wc)

    def w_copies(u):
        slot = odd(u)
        return [pltpu.make_async_copy(ref.at[:, cols_of(u)], wbuf.at[slot, i], w_sem.at[slot, i]) for i, ref in enumerate((wo_ref, wp_ref))]

    def place(n):
        return chip_at(jnp.where(n == 0, chips // DIRS, jnp.where(n == 1, 1, jnp.where(n == DIRS, chips - 1, 0))))

    def parity(i):
        return jnp.where(i == 0, flip(core), core)

    def load(n, i):
        c = CORES * place(n) + parity(i)
        at = rows_at(c * q, q)
        return [pltpu.make_async_copy(xact_ref.at[at, :], xa.at[i], c_sem.at[i, 0]), pltpu.make_async_copy(bc_ref.at[at, :], bca.at[i], c_sem.at[i, 1]),
                pltpu.make_async_copy(sloc_ref.at[c], sl.at[i], c_sem.at[i, DIRS]), pltpu.make_async_copy(z_ref.at[at, :], zb.at[parity(i)], c_sem.at[i, 3])]

    for i in PAIR:
        for cp in load(0, i):
            cp.start()
    for cp in w_copies(0):
        cp.start()
    x_copy = pltpu.make_async_copy(x_ref, xo, x_sem)
    dlane[...] = expand_heads(dskip_ref[...], head_dim)
    ready()

    def swap(n, j):
        return remote(va_own.at[chips + odd(n)], va_par.at[j], vs_sem.at[n], vr_sem.at[n], 'tp', partner)

    def mix(c, i, tgt):
        at = rows_at(c * q, q)
        seg_row = seg_ref[:, at]
        seg_prev = segp_ref[c][:, LANES - 1:]
        seg_rows = jnp.broadcast_to(seg_row, (q, q))
        causal = lax.broadcasted_iota(jnp.int32, (q, q), 0) >= lax.broadcasted_iota(jnp.int32, (q, q), 1)
        bias = jnp.where(causal & (seg_rows == seg_rows.T), 0.0, NEG)
        cum = cum_ref[:, at]
        cl = cl_ref[:, at]
        cum_cols = cum.T
        in_cols = jnp.where(seg_row == seg_prev, jnp.exp2(cum), 0.0).T
        sbf[...] = (sl[i] + pd_ref[c] * sin_ref[...]).astype(BF16)
        c_act = bca[i, :, n_state:]
        scores = lax.dot_general(c_act, bca[i, :, 0:n_state], (((1,), (1,)), ((), ())), preferred_element_type=F32)
        yoff[...] = dot32(c_act, sbf[...])
        lane = lax.broadcasted_iota(jnp.int32, (q, LANES), 1) // head_dim
        sq = jnp.zeros((q, LANES), F32)
        for m in range(inner // LANES):
            cols = slice(m * LANES, (m + 1) * LANES)
            x_f = xa[i, :, cols].astype(F32)
            tops, bots = [], []
            for j in range(per):
                h = m * per + j
                x_h = jnp.where(lane == j, x_f, 0.0).astype(BF16)
                ccol, crow = cum_cols[:, h:h + 1], cl[h:h + 1, :]
                m_top = jnp.exp2(ccol[0:hq] + bias[0:hq, 0:hq] - crow[:, 0:hq]) * scores[0:hq, 0:hq]
                m_bot = jnp.exp2(ccol[hq:] + bias[hq:] - crow) * scores[hq:]
                tops.append(dot32(m_top.astype(BF16), x_h[0:hq]))
                bots.append(dot32(m_bot.astype(BF16), x_h))
            y = jnp.concatenate([sum(tops), sum(bots)], axis=0)
            y = y + yoff[:, cols] * head_lanes(in_cols, m, head_dim) + dlane[:, cols] * x_f
            v = y * silu(zb[parity(i), :, cols].astype(F32))
            gated[:, cols] = v
            sq = sq + v * v
        inv = lax.rsqrt(jnp.sum(sq, axis=1, keepdims=True) * (1.0 / inner) + NORM_EPS)
        inv = jnp.broadcast_to(inv, (q, LANES))
        for m in range(inner // LANES):
            cols = slice(m * LANES, (m + 1) * LANES)
            va_own[tgt, :, cols] = (gated[:, cols] * inv * nw_ref[m:m + 1, :].astype(F32)).astype(BF16)

    def prep(n):
        j = place(n)
        tok = rows_at(j * (CORES * q), CORES * q)

        @pl.when(n >= DIRS)
        def _():
            for i in PAIR:
                for cp in load(n, i)[:3]:
                    cp.start()

        @pl.when(n < DIRS)
        def _():
            for i in PAIR:
                load(n, i)[3].wait()

        @pl.when(n >= 1)
        def _():
            first = jnp.where(n == 1, (inner - zlast) // zt, 0)

            def wz_copy(m):
                return pltpu.make_async_copy(wz_ref.at[:, rows_at(m * zt, zt)], wzb.at[odd(m)], z_sem.at[odd(m)])
            rows_copy = pltpu.make_async_copy(xf_ref.at[tok, :], xg, v_sem)
            rows_copy.start()
            wz_copy(first).start()
            rows_copy.wait()

            def z_body(m, carry):
                wz_copy(m).wait()

                @pl.when(m + 1 < inner // zt)
                def _():
                    wz_copy(m + 1).start()
                res = dot32(xg[...], wzb[odd(m)]).astype(BF16)
                for p in PAIR:
                    zb[p, :, rows_at(m * zt, zt)] = res[p * q:(p + 1) * q]
                return carry
            lax.fori_loop(first, inner // zt, z_body, 0)

        @pl.when(n >= DIRS)
        def _():
            swap(n - DIRS, j).wait_send()

        def chunk(i, carry):
            for cp in load(n, i)[:3]:
                cp.wait()
            mix(CORES * j + parity(i), i, jnp.where(i == 0, chips + odd(n), j))

            @pl.when(n == 0)
            def _():
                for cp in load(1, i):
                    cp.start()

            @pl.when(i == 0)
            def _():
                swap(n, j).start()
            return carry
        lax.fori_loop(0, CORES, chunk, 0)
        swap(n, j).wait_recv()

    def ring_copy(d, unit):
        slot = lax.rem(unit, slots)
        return remote(send.at[d, slot], recv_ref.at[d, unit], s_sem.at[d, slot], r_sem.at[d, unit], 'tp', jnp.where(d == 0, ring[1], ring[0]))

    def fetch(d, unit, at):
        ring_copy(d, unit).wait_recv()
        cp = pltpu.make_async_copy(recv_ref.at[d, unit], rbuf.at[at], l_sem.at[at])
        cp.start()
        return cp

    def o_copy(d, b):
        cols = rows_at(d * half_cols + b * wc, wc)
        return pltpu.make_async_copy(xo.at[:, cols], o_ref.at[:, cols], o_sem.at[d, b])

    def product(dest, slot):
        return dot32(va_own[dest], wbuf[slot, 0]) + dot32(va_par[dest], wbuf[slot, 1])

    def finish(d, b):
        last = (hops - 1) * nb + b
        copies = [fetch(d, last, 0), fetch(flip(d), last - nb, 1)]
        for cp in copies:
            cp.wait()
        cols = rows_at(flip(d) * half_cols + b * wc, wc)
        xo[:, cols] = (xo[:, cols].astype(F32) + (acc[d, lax.rem(b, lag + 1)] + (rbuf[0] + rbuf[1]))).astype(BF16)
        o_copy(flip(d), b).start()

    def body(u, carry):
        d = odd(u)
        k = u // (DIRS * nb)
        b = lax.rem(u // DIRS, nb)
        unit = k * nb + b
        ending = k == hops - 1

        @pl.when((d == 0) & ((b == 0) | ((k == 0) & (b == slots + 1))))
        def _():
            prep(jnp.where(u == 0, 0, k + 1))
        dest = chip_at(jnp.where(k == 0, chips // DIRS, jnp.where(d == 0, 1, chips - 1)))
        for cp in w_copies(u):
            cp.wait()

        @pl.when(u + 1 < steps)
        def _():
            for cp in w_copies(u + 1):
                cp.start()

        @pl.when(u == DIRS)
        def _():
            x_copy.start()
        part = product(dest, d)
        slot = lax.rem(unit, slots)

        @pl.when((unit >= slots) & (flip(ending) | (b < slots - depth)))
        def _():
            ring_copy(d, unit - slots).wait_send()

        @pl.when(ending)
        def _():
            ring_copy(d, unit - depth).wait_send()

        @pl.when(k != 1)
        def _():
            send[d, slot] = part

        @pl.when(k == 1)
        def _():
            fetch(d, unit - nb, 0).wait()
            send[d, slot] = part + rbuf[0]
        ring_copy(d, unit).start()

        @pl.when(ending)
        def _():
            acc[d, lax.rem(b, lag + 1)] = product(chip, d)

            @pl.when(b == 0)
            def _():
                pl.when(d == 0)(x_copy.wait)

            @pl.when(b >= lag)
            def _():
                finish(d, b - lag)
        return carry

    lax.fori_loop(0, steps, body, 0)

    def tail(i, carry):
        finish(odd(i), nb - lag + i // DIRS)
        return carry

    def drain(i, carry):
        o_copy(odd(i), i // DIRS).wait()
        return carry

    def drain_send(i, carry):
        ring_copy(odd(i), hops * nb - depth + i // DIRS).wait_send()
        return carry
    lax.fori_loop(0, DIRS * lag, tail, 0)
    lax.fori_loop(0, DIRS * depth, drain_send, 0)
    for n in PAIR:
        swap(DIRS + n, chip).wait_send()
    lax.fori_loop(0, DIRS * nb, drain, 0)


def out_proj_scatter(x_act, bc_act, cum, cl, seg_row, seg_prev, sloc, pd, s_in, z_arr, x_full, w_z, d_skip, norm_w, w_own, w_par, x_loc, chips, wc=512, slots=4, zt=256, zlast=1024):
    t, inner = x_act.shape
    rows, d_model = x_loc.shape
    gw = bc_act.shape[1]
    n_state = s_in.shape[0]
    nb = d_model // DIRS // wc
    units = (chips - 1) * nb
    return pl.pallas_call(
        functools.partial(out_kernel, chips, nb, wc, slots, zt, zlast),
        in_specs=[ANY, ANY, VMEM, VMEM, VMEM, VMEM, ANY, VMEM, VMEM, ANY, ANY, ANY, VMEM, VMEM, ANY, ANY, ANY],
        out_specs=[ANY, ANY],
        out_shape=[out_of(BF16, rows, d_model), out_of(F32, DIRS, units, rows, wc)],
        scratch_shapes=[scratch(BF16, chips + DIRS, rows, inner), scratch(BF16, chips, rows, inner), scratch(BF16, DIRS, DIRS, inner, wc), scratch(F32, DIRS, slots, rows, wc), scratch(F32, DIRS, slots, rows, wc),
                        scratch(F32, DIRS, rows, wc), scratch(BF16, rows, d_model), scratch(BF16, CORES * rows, d_model), scratch(BF16, DIRS, d_model, zt),
                        scratch(BF16, CORES, rows, inner), scratch(BF16, DIRS, rows, inner), scratch(BF16, DIRS, rows, gw), scratch(F32, DIRS, n_state, inner),
                        scratch(BF16, n_state, inner), scratch(F32, rows, inner), scratch(F32, rows, inner), scratch(F32, 1, inner),
                        sems(chips), sems(chips), sems(DIRS, DIRS), sems(DIRS, slots), sems(DIRS, units), sems(DIRS), DMA, sems(DIRS, nb), sems(DIRS, 4), sems(DIRS), DMA],
        compiler_params=params(63, 1),
        cost_estimate=pl.CostEstimate(flops=DIRS * t * inner * d_model, bytes_accessed=t * d_model, transcendentals=0),
        name='out_proj_scatter',
    )(x_act, bc_act, cum, cl, seg_row, seg_prev, sloc, pd, s_in, z_arr, x_full, w_z, d_skip, norm_w, w_own, w_par, x_loc)[0]


def layer(x_loc, seg_loc, w_zx, w_bc, w_dt, conv_x, conv_bc, bias_x, bias_bc, a_log, dt_bias, d_skip, norm_w, w_out, chips, blocks):
    rows = x_loc.shape[0]
    tiled = lambda v: v.reshape(v.shape[0] // LANES, LANES)
    x_full, x_pre, small, w_z, w_par, seg, seg_tail, tail_x, tail_b = gather_proj(x_loc, w_zx, w_bc, w_dt.T, w_out, seg_loc[None], chips, blocks)
    x_act, bc_act, cum, cl, seg_row, seg_prev, sloc, pd, s_end, dec = phase_a(
        x_pre, small, seg, seg_tail, tail_x, tail_b, conv_x, conv_bc, tiled(bias_x), bias_bc, a_log[None], dt_bias[None], rows)
    z_arr, s_in = z_chain(x_full, w_z, s_end, dec, chips, blocks)
    return out_proj_scatter(x_act, bc_act, cum, cl, seg_row, seg_prev, sloc, pd, s_in, z_arr, x_full, w_z, d_skip[None], tiled(norm_w), w_out, w_par, x_loc, chips)


def solution(mesh):
    tokens = ('dp', 'sp', 'tp')
    heads = P('tp')
    cols = P(None, 'tp')
    deep = P(None, None, 'tp')
    specs = (P(tokens, None), P(tokens), deep, deep, cols, cols, deep, heads, cols, heads, heads, heads, heads, P('tp', None))
    body = functools.partial(layer, chips=mesh.shape['tp'] // CORES, blocks=mesh.shape['sp'])
    return jax.shard_map(body, mesh=mesh, in_specs=specs, out_specs=specs[0], check_vma=False)
```

```python
import functools
import jax
import jax.numpy as jnp
from jax import lax
from jax.experimental import pallas as pl
from jax.experimental.pallas import tpu as pltpu
from jax.sharding import PartitionSpec as P

MESH = pl.DeviceIdType.MESH
NORM_EPS = 1e-5
LOG2E = 1.4426950408889634
FAR = -1e6
NEG = -1e30
F32 = jnp.float32
BF16 = jnp.bfloat16
HI = lax.Precision.HIGHEST
MIB = 2 ** 20
LANES = 128
ROW8 = 8
CORES = 2
DIRS = 2
PAIR = range(2)
ANY = pl.BlockSpec(memory_space=pl.ANY)
VMEM = pl.BlockSpec(memory_space=pltpu.VMEM)
DMA = pltpu.SemaphoreType.DMA


def scratch(dtype, *shape):
    return pltpu.VMEM(shape, dtype)


def out_of(dtype, *shape):
    return jax.ShapeDtypeStruct(shape, dtype)


def sems(*shape):
    return DMA(shape)


def rows_at(start, size):
    return pl.ds(pl.multiple_of(start, size), size)


def odd(i):
    return lax.rem(i, 2)


def flip(i):
    return 1 - i


def dot32(a, b):
    return jnp.dot(a, b, preferred_element_type=F32)


def params(limit, name_id=None):
    if name_id is None:
        return pltpu.CompilerParams(dimension_semantics=('arbitrary',), vmem_limit_bytes=limit * MIB)
    return pltpu.CompilerParams(collective_id=name_id, has_side_effects=True, vmem_limit_bytes=limit * MIB)


def greet(peers):
    barrier = pltpu.get_barrier_semaphore()
    for axis, index in peers:
        pl.semaphore_signal(barrier, inc=1, device_id={axis: index}, device_id_type=MESH)
    return lambda: pl.semaphore_wait(barrier, len(peers))


def remote(src, dst, send, recv, axis, index):
    return pltpu.make_async_remote_copy(src_ref=src, dst_ref=dst, send_sem=send, recv_sem=recv, device_id={axis: index}, device_id_type=MESH)


def silu(v):
    h = v * 0.5
    return h + h * jnp.tanh(h)


def head_lanes(cols, tile_idx, head_dim):
    rows = cols.shape[0]
    per = LANES // head_dim
    lane = lax.broadcasted_iota(jnp.int32, (rows, LANES), 1)
    out = None
    for j in range(per):
        h = tile_idx * per + j
        nxt = jnp.broadcast_to(cols[:, h:h + 1], (rows, LANES))
        out = nxt if out is None else jnp.where(lane >= j * head_dim, nxt, out)
    return out


def expand_heads(row, head_dim):
    heads = row.shape[1]
    shape = (heads, heads * head_dim)
    eye = (lax.broadcasted_iota(jnp.int32, shape, 1) // head_dim == lax.broadcasted_iota(jnp.int32, shape, 0)).astype(F32)
    return jnp.dot(jnp.broadcast_to(row, (ROW8, heads)), eye, precision=HI, preferred_element_type=F32)[0:1]


def column(row):
    return jnp.broadcast_to(row, (LANES, row.shape[1])).T[:, 0:1]


def gather_kernel(chips, blocks, kb, nb, sub, nt, pace, x_ref, wzx_ref, wbc_ref, wdt_ref, wo_ref, seg_ref,
                  xf_ref, xp_ref, bp_ref, wz_ref, wp_ref, segf_ref, segt_ref, tx_ref, tb_ref,
                  wx, wsm, xg, ost, bst, blk, bblk, zst, wdt,
                  ra_sem, rd_sem, so_sem, sf_sem, sd_sem, xl_sem, xs_sem, in_sem, zo_sem, bb_sem, dt_sem, oo_sem, bo_sem,
                  wp_sem, sg_sem, sr_sem, st_sem, hx_sem, hb_sem):
    me = lax.axis_index('tp')
    blk_id = lax.axis_index('sp')
    chip, core = me // CORES, odd(me)
    partner = CORES * chip + flip(core)
    near = [lax.rem(chip + chips - 1, chips), lax.rem(chip + 1, chips)]
    far = lax.rem(chip + chips // CORES, chips)
    ring = [CORES * c + core for c in near]
    sp_next = lax.rem(blk_id + 1, blocks)
    n_tp = CORES * chips
    rows = x_ref.shape[0]
    quarters = xl_sem.shape[1]
    qr = rows // quarters
    d_model, inner = wx.shape
    heads = wdt.shape[0]
    n_state = bblk.shape[3]
    nk = d_model // kb
    nblk = nk * (inner // nb)
    opp = CORES + quarters
    last = opp + quarters // CORES - 1
    ready = greet([('tp', lax.rem(me + d, n_tp)) for d in range(1, n_tp)] + [('sp', sp_next), ('sp', lax.rem(blk_id + blocks - 1, blocks))])

    def row_of(lv, b):
        side = odd(b)
        other = jnp.where(lv < CORES, lv, b // CORES)
        cc = jnp.where(other == 1, flip(core), core)
        ch = jnp.where(lv < CORES, chip, jnp.where(lv >= opp, far, jnp.where(side == 0, near[0], near[1])))
        q = jnp.where(lv < CORES, b, jnp.where(lv >= opp, side * (quarters // CORES) + lv - opp, lv - CORES))
        return (CORES * ch + cc) * rows + q * qr

    def full_rows(lv, b, size=qr):
        return xf_ref.at[rows_at(row_of(lv, b), size), :]

    def w_tile(i):
        return rows_at(lax.rem(i, nk) * kb, kb), rows_at((i // nk) * nb, nb)

    def blk_copy(i):
        kk, nn = w_tile(i)
        slot = lax.rem(i, blk.shape[0])
        return pltpu.make_async_copy(wzx_ref.at[kk, :, nn], blk.at[slot], in_sem.at[slot])

    def z_copy(i):
        kk, nn = w_tile(i)
        return pltpu.make_async_copy(zst.at[odd(i)], wz_ref.at[kk, nn], zo_sem.at[odd(i)])

    def bc_copy(i):
        return pltpu.make_async_copy(wbc_ref.at[rows_at(i * kb, kb)], bblk.at[odd(i)], bb_sem.at[odd(i)])

    own_load = pltpu.make_async_copy(x_ref, xg.at[0], xs_sem.at[0])
    dt_load = pltpu.make_async_copy(wdt_ref, wdt, dt_sem)
    own_load.start()
    dt_load.start()
    bc_copy(0).start()
    for i in range(blk.shape[0]):
        blk_copy(i).start()
    ready()

    def own_send(q, to):
        return remote(x_ref.at[rows_at(q * qr, qr), :], full_rows(0, q), so_sem.at[to, q], ra_sem.at[CORES + q, flip(to)], 'tp', ring[to])

    own_pair = remote(x_ref, full_rows(0, 0, rows), sd_sem.at[1, 0], rd_sem.at[1, 0], 'tp', partner)

    def pair_send(lv, side):
        return remote(full_rows(lv, side), full_rows(lv, side), sd_sem.at[lv, side], rd_sem.at[lv, side], 'tp', partner)

    def forward(lv, to):
        side = flip(to)
        h = lax.rem(lv - CORES, quarters // CORES)
        dst_sem = ra_sem.at[opp + h, side]
        return remote(full_rows(lv, side), full_rows(lv, side), sf_sem.at[to, h], dst_sem, 'tp', ring[to])

    def arrival(lv, side):
        return remote(full_rows(lv, side), full_rows(lv, side), so_sem.at[0, 0], ra_sem.at[lv, side], 'tp', ring[0])

    def pair_arrival(lv, side):
        ref = full_rows(lv, CORES + side)
        return remote(ref, ref, sd_sem.at[1, 0], rd_sem.at[lv, side], 'tp', partner)

    pair_own_arrival = remote(full_rows(1, 0, rows), full_rows(1, 0, rows), sd_sem.at[1, 0], rd_sem.at[1, 0], 'tp', partner)

    def send_quarter(q):
        for to in PAIR:
            own_send(q, flip(to)).start()
    send_quarter(0)
    own_pair.start()

    def seg_cols(index):
        return segf_ref.at[:, rows_at(index * rows, rows)]

    def seg_send(d):
        return remote(seg_ref, seg_cols(me), sg_sem.at[d], sr_sem.at[d], 'tp', lax.rem(me + d, n_tp))

    def seg_arrival(d):
        return remote(seg_ref, seg_cols(lax.rem(me + n_tp - d, n_tp)), sg_sem.at[d], sr_sem.at[d], 'tp', lax.rem(me + d, n_tp))

    seg_own = pltpu.make_async_copy(seg_ref, seg_cols(me), sg_sem.at[0])
    seg_own.start()
    for d in range(1, n_tp):
        seg_send(d).start()
    w_swap = remote(wo_ref, wp_ref, wp_sem.at[0], wp_sem.at[1], 'tp', partner)
    w_swap.start()
    seg_halo = remote(segf_ref.at[:, pl.ds(n_tp * rows - LANES, LANES)], segt_ref, st_sem.at[0], st_sem.at[1], 'sp', sp_next)

    end_chip = chips - 1
    hrows = tx_ref.shape[0]
    halo_lv = jnp.where(chip == end_chip, flip(core), jnp.where(far == end_chip, last, opp - 1))
    halo_b = jnp.where(chip == end_chip, quarters - 1, jnp.where((far != end_chip) & (near[0] == end_chip), 0, 1) + CORES * flip(core))

    def halo_copies(slot):
        src = rows_at(halo_b * qr + qr - hrows, hrows)
        return [remote(ost.at[slot, src, :], tx_ref, hx_sem.at[0], hx_sem.at[1], 'sp', sp_next),
                remote(bst.at[slot, src, :], tb_ref, hb_sem.at[0], hb_sem.at[1], 'sp', sp_next)]

    dt_load.wait()

    def small_body(i, carry):
        bc_copy(i).wait()

        @pl.when(i + 1 < nk)
        def _():
            bc_copy(i + 1).start()

        def inner_body(s, carry2):
            part = jnp.swapaxes(bblk[odd(i), rows_at(s * sub, sub)], 0, 1)
            at = rows_at(i * kb + s * sub, sub)
            for g in PAIR:
                wsm[at, g * n_state:(g + 1) * n_state] = part[g]
            wd = jnp.concatenate([wdt[:, at].astype(F32), jnp.zeros((LANES - heads, sub), F32)], axis=0)
            wsm[at, CORES * n_state:] = wd.T.astype(BF16)
            return carry2
        return lax.fori_loop(0, kb // sub, inner_body, carry)
    lax.fori_loop(0, nk, small_body, 0)

    def relay(i, carry):
        slot = lax.rem(i, blk.shape[0])
        blk_copy(i).wait()

        @pl.when(i >= CORES)
        def _():
            z_copy(i - CORES).wait()
        kk = lax.rem(i, nk) * kb

        def inner_body(s, carry2):
            at = rows_at(s * sub, sub)
            part = jnp.swapaxes(blk[slot, at].astype(F32), 0, 1)
            zst[odd(i), at, :] = part[0].astype(BF16)
            wx[rows_at(kk + s * sub, sub), w_tile(i)[1]] = part[1].astype(BF16)
            return carry2
        lax.fori_loop(0, kb // sub, inner_body, 0)
        z_copy(i).start()
        for q in range(1, quarters - 1):
            pl.when(i == q * pace - 1)(functools.partial(send_quarter, q))

        @pl.when(i + blk.shape[0] < nblk)
        def _():
            blk_copy(i + blk.shape[0]).start()
        return carry
    lax.fori_loop(0, nblk, relay, 0)

    seg_own.wait()
    for d in range(1, n_tp):
        seg_arrival(d).wait_recv()
    seg_halo.start()
    own_load.wait()
    own_store = pltpu.make_async_copy(xg.at[0], full_rows(0, 0, rows), xs_sem.at[1])
    own_store.start()

    def load(lv, b):
        return pltpu.make_async_copy(full_rows(lv, b), xg.at[odd(lv), rows_at(b * qr, qr), :], xl_sem.at[odd(lv), b])

    def take(lv):
        @pl.when(lv >= CORES)
        def _():
            for side in PAIR:
                arrival(lv, side).wait_recv()
                pair_send(lv, side).start()

    def fetch(lv):
        @pl.when(lv == 1)
        def _():
            pair_own_arrival.wait_recv()

        @pl.when(lv >= CORES)
        def _():
            for side in PAIR:
                pair_arrival(lv, side).wait_recv()
        for b in range(quarters):
            load(lv, b).start()

    def out_copies(lv):
        slot = odd(lv)
        res = []
        for b in range(quarters):
            src, dst = rows_at(b * qr, qr), rows_at(row_of(lv, b), qr)
            res.append(pltpu.make_async_copy(ost.at[slot, src, :], xp_ref.at[dst, :], oo_sem.at[slot, b]))
            res.append(pltpu.make_async_copy(bst.at[slot, src, :], bp_ref.at[dst, :], bo_sem.at[slot, b]))
        return res

    early = opp - 1
    cut = CORES + quarters // CORES

    def feed(lv):
        @pl.when(lv == 1)
        def _():
            send_quarter(quarters - 1)
        for h in range(quarters // CORES):
            @pl.when(lv == 3 + CORES * h)
            def _(h=h):
                forward(CORES + h, 1).start()
                forward(cut + h, 0).start()

    def round_body(lv, carry):
        slot = odd(lv)

        @pl.when(lv > 0)
        def _():
            for b in range(quarters):
                load(lv, b).wait()

        @pl.when(lv == 1)
        def _():
            own_store.wait()

        @pl.when(lv < early)
        def _():
            take(lv + 1)

        @pl.when(lv >= CORES)
        def _():
            for cp in out_copies(lv - CORES):
                cp.wait()

        def dots(n, carry2):
            @pl.when(n == inner // nt // CORES)
            def _():
                feed(lv)

                @pl.when(lv < early)
                def _():
                    fetch(lv + 1)
            cols = rows_at(n * nt, nt)
            ost[slot, :, cols] = dot32(xg[slot], wx[:, cols]).astype(BF16)
            return carry2
        lax.fori_loop(0, inner // nt, dots, 0)
        bst[slot] = dot32(xg[slot], wsm[...]).astype(BF16)
        for cp in out_copies(lv):
            cp.start()

        @pl.when(lv == halo_lv + 1)
        def _():
            for cp in halo_copies(flip(slot)):
                cp.wait_send()

        @pl.when(lv == halo_lv)
        def _():
            for cp in halo_copies(slot):
                cp.start()

        @pl.when(lv >= early)
        def _():
            take(lv + 1)

        @pl.when((lv >= early) & (lv < last - 1))
        def _():
            fetch(lv + 1)

        @pl.when(lv == last - 1)
        def _():
            for b in PAIR:
                load(last, b).start()
        return carry
    lax.fori_loop(0, last, round_body, 0)

    slot = last % CORES
    for cp in out_copies(last - CORES):
        cp.wait()
    copies = out_copies(last)
    for part in PAIR:
        for b in PAIR:
            load(last, CORES * part + b).wait()
        some = pl.ds(part * CORES * qr, CORES * qr)

        def half_dots(n, carry, part=part, some=some):
            if part == 0:
                @pl.when(n == 1)
                def _():
                    for side in PAIR:
                        pair_arrival(last, side).wait_recv()
                        load(last, CORES + side).start()
            cols = rows_at(n * nt, nt)
            ost[slot, some, cols] = dot32(xg[slot, some, :], wx[:, cols]).astype(BF16)
            return carry
        lax.fori_loop(0, inner // nt, half_dots, 0)
        bst[slot, some, :] = dot32(xg[slot, some, :], wsm[...]).astype(BF16)
        for cp in copies[part * quarters:(part + 1) * quarters]:
            cp.start()

    @pl.when(halo_lv == last)
    def _():
        for cp in halo_copies(slot):
            cp.start()
        for cp in halo_copies(slot):
            cp.wait_send()
    for cp in halo_copies(0):
        cp.wait_recv()
    seg_halo.wait()
    for d in range(1, n_tp):
        seg_send(d).wait_send()
    w_swap.wait()
    for i in PAIR:
        for cp in out_copies(last - i):
            cp.wait()
        z_copy(nblk - 1 - i).wait()
    own_pair.wait_send()
    for to in PAIR:
        for q in range(quarters):
            own_send(q, to).wait_send()
        for h in range(quarters // CORES):
            forward(CORES + h, to).wait_send()
    for lv in range(CORES, last + 1):
        for side in PAIR:
            pair_send(lv, side).wait_send()


def gather_proj(x_loc, w_zx, w_bc, w_dt_t, w_out, seg, chips, blocks, kb=2048, nb=256, sub=256, nt=512, quarters=4, pace=12):
    rows, d_model = x_loc.shape
    inner, n_state, heads = w_zx.shape[CORES], w_bc.shape[CORES], w_dt_t.shape[0]
    n_tp = CORES * chips
    t = rows * n_tp
    small = CORES * n_state + LANES
    lv = CORES + quarters + quarters // CORES
    halo = 16
    two = sems(CORES)
    return pl.pallas_call(
        functools.partial(gather_kernel, chips, blocks, kb, nb, sub, nt, pace),
        in_specs=[ANY] * 6,
        out_specs=[ANY] * 9,
        out_shape=[out_of(BF16, t, d_model), out_of(BF16, t, inner), out_of(BF16, t, small), out_of(BF16, d_model, inner), out_of(BF16, *w_out.shape),
                   out_of(jnp.int32, 1, t), out_of(jnp.int32, 1, LANES), out_of(BF16, halo, inner), out_of(BF16, halo, small)],
        scratch_shapes=[scratch(BF16, d_model, inner), scratch(BF16, d_model, small), scratch(BF16, CORES, rows, d_model),
                        scratch(BF16, CORES, rows, inner), scratch(BF16, CORES, rows, small), scratch(BF16, 3, kb, CORES, nb),
                        scratch(BF16, CORES, kb, CORES, n_state), scratch(BF16, CORES, kb, nb), scratch(BF16, heads, d_model),
                        sems(lv, CORES), sems(lv, CORES), sems(CORES, quarters), sems(CORES, quarters), sems(lv, CORES), sems(CORES, quarters), two, sems(3), two, two, DMA,
                        sems(CORES, quarters), sems(CORES, quarters), two, sems(n_tp), sems(n_tp), two, two, two],
        compiler_params=params(63, 0),
        cost_estimate=pl.CostEstimate(flops=t * inner * d_model, bytes_accessed=t * inner, transcendentals=0),
        name='gather_proj',
    )(x_loc, w_zx, w_bc, w_dt_t, w_out, seg)


def phase_a_kernel(q, x_ref, small_ref, seg_ref, segt_ref, tailx_ref, tailb_ref, cx_ref, cbc_ref, bx_ref, bbc_ref, alog_ref, dtb_ref,
                   xact_ref, bcact_ref, cum_ref, cl_ref, segf_ref, segp_ref, sloc_ref, pd_ref, send_ref, dec_ref,
                   pad, xw, segtail, base, cw):
    inner = x_ref.shape[1]
    gw = bcact_ref.shape[1]
    n_state = gw // 2
    heads = alog_ref.shape[1]
    head_dim = inner // heads
    taps = cx_ref.shape[0]

    @pl.when(pl.program_id(0) == 0)
    def _():
        first = lax.axis_index('sp') == 0
        base[...] = jnp.broadcast_to(jnp.where(first, seg_ref[:, 0:1], segt_ref[:, LANES - 1:]), base.shape)
        segtail[...] = jnp.where(first, FAR, (segt_ref[...] - base[...]).astype(F32))
        pad[0:ROW8, 0:inner] = tailx_ref[...].astype(F32)[ROW8:]
        pad[0:ROW8, inner:] = tailb_ref[:, 0:gw].astype(F32)[ROW8:]
        cw[0:taps, 0:inner] = cx_ref[...].astype(F32)
        for i in range(inner // LANES):
            cw[taps:taps + 1, i * LANES:(i + 1) * LANES] = bx_ref[i:i + 1, :].astype(F32)
        for g in PAIR:
            cols = slice(inner + g * n_state, inner + (g + 1) * n_state)
            cw[0:taps, cols] = cbc_ref[:, g, :].astype(F32)
            cw[taps:taps + 1, cols] = bbc_ref[g:g + 1, :].astype(F32)
        send_ref[...] = jnp.zeros_like(send_ref)
        dec_ref[...] = jnp.ones_like(dec_ref)

    @pl.when(pl.program_id(0) > 0)
    def _():
        pad[0:ROW8, :] = pad[q:q + ROW8, :]

    pad[ROW8:, 0:inner] = x_ref[...].astype(F32)
    pad[ROW8:, inner:] = small_ref[:, 0:gw].astype(F32)
    seg_row = (seg_ref[...] - base[:, 0:1]).astype(F32)
    prev_row = segtail[...]
    segf_ref[...] = seg_row
    segp_ref[0] = prev_row
    segtail[...] = seg_row[:, q - LANES:]
    ext = jnp.concatenate([prev_row, seg_row], axis=1)
    seg_last, seg_prev = seg_row[:, q - 1:], prev_row[:, LANES - 1:]
    keeps = []
    for j in range(1, taps):
        keep_row = jnp.where(ext[:, LANES - j:LANES - j + q] == seg_row, 1.0, 0.0)
        keeps.append(jnp.broadcast_to(keep_row, (LANES, q)).T)
    raw = small_ref[:, gw:].astype(F32).T[0:heads] + column(dtb_ref[...])
    dt = jnp.maximum(raw, 0.0) + jnp.log1p(jnp.exp(-jnp.abs(raw)))
    log_a = dt * column(jnp.exp(alog_ref[...]) * -LOG2E)
    tri = (lax.broadcasted_iota(jnp.int32, (q, q), 0) <= lax.broadcasted_iota(jnp.int32, (q, q), 1)).astype(F32)
    cum = jnp.dot(log_a, tri, precision=HI, preferred_element_type=F32)
    cum_ref[...] = cum
    cl_ref[...] = cum - jnp.log(dt) * LOG2E
    cum_last = cum[:, q - 1:]
    end_cols = (jnp.where(seg_row == seg_last, jnp.exp2(cum_last - cum), 0.0) * dt).T
    carry = jnp.where(seg_last == seg_prev, jnp.exp2(cum_last), 0.0)
    carry_lane = expand_heads(jnp.broadcast_to(carry, (heads, LANES)).T[0:1], head_dim)
    for i in range((inner + gw) // LANES):
        cols = slice(i * LANES, (i + 1) * LANES)
        src = pad[:, cols]
        acc = cw[taps:taps + 1, cols] + src[ROW8:] * cw[taps - 1:taps, cols]
        for j in range(1, taps):
            at = taps - 1 - j
            acc = acc + pltpu.roll(src, j, axis=0)[ROW8:] * cw[at:at + 1, cols] * keeps[j - 1]
        act = silu(acc).astype(BF16)
        if i * LANES < inner:
            xact_ref[:, cols] = act
            xw[:, cols] = (act.astype(F32) * head_lanes(end_cols, i, head_dim)).astype(BF16)
        else:
            bcact_ref[:, i * LANES - inner:(i + 1) * LANES - inner] = act
    sloc_ref[0] = send_ref[...]
    pd_ref[0] = dec_ref[...]
    send_ref[...] = carry_lane * send_ref[...] + dot32(bcact_ref[:, 0:n_state].T, xw[...])
    dec_ref[...] = dec_ref[...] * carry_lane


def phase_a(x_pre, small, seg, seg_tail, tail_x, tail_b, conv_x, conv_bc, bias_x, bias_bc, a_log, dt_bias, q):
    t, inner = x_pre.shape
    n_state = conv_bc.shape[2]
    gw = CORES * n_state
    heads = a_log.shape[1]
    nt = t // q

    def full(shape):
        return pl.BlockSpec(shape, lambda c: (0,) * len(shape))

    def by_row(width):
        return pl.BlockSpec((q, width), lambda c: (c, 0))

    def by_col(height):
        return pl.BlockSpec((height, q), lambda c: (0, c))

    def by_chunk(a, b):
        return pl.BlockSpec((1, a, b), lambda c: (c, 0, 0))

    rest = (seg_tail, tail_x, tail_b, conv_x, conv_bc, bias_x, bias_bc, a_log, dt_bias)
    return pl.pallas_call(
        functools.partial(phase_a_kernel, q),
        grid=(nt,),
        in_specs=[by_row(inner), by_row(small.shape[1]), by_col(1)] + [full(v.shape) for v in rest],
        out_specs=[by_row(inner), by_row(gw), by_col(heads), by_col(heads), by_col(1), by_chunk(1, LANES), by_chunk(n_state, inner), by_chunk(1, inner),
                   full((n_state, inner)), full((1, inner))],
        out_shape=[out_of(BF16, t, inner), out_of(BF16, t, gw), out_of(F32, heads, t), out_of(F32, heads, t), out_of(F32, 1, t), out_of(F32, nt, 1, LANES),
                   out_of(F32, nt, n_state, inner), out_of(F32, nt, 1, inner), out_of(F32, n_state, inner), out_of(F32, 1, inner)],
        scratch_shapes=[scratch(F32, q + ROW8, inner + gw), scratch(BF16, q, inner), scratch(F32, 1, LANES),
                        scratch(jnp.int32, 1, LANES), scratch(F32, ROW8, inner + gw)],
        compiler_params=params(56),
        cost_estimate=pl.CostEstimate(flops=t * inner * gw, bytes_accessed=t * inner, transcendentals=0),
        name='phase_a',
    )(x_pre, small, seg, *rest)


def chain_kernel(chips, blocks, pieces, hop, gap, nt, xf_ref, wz_ref, send_ref, dec_ref, z_ref, sin_ref,
                 xg, wzb, zst, sbuf, rbuf, x_sem, w_sem, z_sem, s_sem, r_sem):
    chip = lax.axis_index('tp') // CORES
    blk_id = lax.axis_index('sp')
    sp_next = lax.rem(blk_id + 1, blocks)
    ready = greet([('sp', sp_next), ('sp', lax.rem(blk_id + blocks - 1, blocks))])
    n_state, inner = send_ref.shape
    tm = xg.shape[1]
    nn = inner // nt
    tiles = nn + nn // CORES
    pw = inner // pieces
    parts = range(x_sem.shape[1])
    kw = xg.shape[2] // len(parts)

    def tok(g):
        return rows_at(lax.rem(chip + jnp.where(g == 0, chips // 2, 1), chips) * tm, tm)

    def col(i):
        return rows_at(lax.rem(i, nn) * nt, nt)

    def depth(s):
        return pl.ds(s * kw, kw)

    def x_copy(g, s):
        return pltpu.make_async_copy(xf_ref.at[tok(g), depth(s)], xg.at[g, :, depth(s)], x_sem.at[g, s])

    def w_copy(i, s):
        return pltpu.make_async_copy(wz_ref.at[depth(s), col(i)], wzb.at[odd(i), depth(s), :], w_sem.at[odd(i), s])

    def z_copy(i):
        return pltpu.make_async_copy(zst.at[odd(i)], z_ref.at[tok(i // nn), col(i)], z_sem.at[odd(i)])

    def hop_copy(p):
        return remote(sbuf.at[p], rbuf.at[p], s_sem.at[p], r_sem.at[p], 'sp', sp_next)

    for s in parts:
        x_copy(0, s).start()
        w_copy(0, s).start()
    ready()

    def pass_on(j):
        lead = j - hop * blk_id
        p = lead // gap

        @pl.when((lead >= 0) & (lax.rem(lead, gap) == 0) & (p < pieces))
        def _():
            cols = rows_at(p * pw, pw)

            @pl.when(blk_id == 0)
            def _():
                sbuf[p] = send_ref[:, cols]
                sin_ref[:, cols] = jnp.zeros((n_state, pw), F32)

            @pl.when(blk_id > 0)
            def _():
                hop_copy(p).wait_recv()
                prev = rbuf[p]
                sin_ref[:, cols] = prev
                sbuf[p] = dec_ref[:, cols] * prev + send_ref[:, cols]

            @pl.when(blk_id < blocks - 1)
            def _():
                hop_copy(p).start()

    def tile(i):
        g = i // nn

        @pl.when(i >= 2)
        def _():
            z_copy(i - 2).wait()
        res = 0.0
        for s in parts:
            @pl.when(lax.rem(i, nn) == 0)
            def _(s=s):
                x_copy(g, s).wait()
            w_copy(i, s).wait()

            @pl.when(i + 1 < tiles)
            def _(s=s):
                w_copy(i + 1, s).start()
            pl.when(i == 1)(x_copy(1, s).start)
            pass_on(i * len(parts) + s)
            res = res + dot32(xg[g, :, depth(s)], wzb[odd(i), depth(s), :])
        zst[odd(i)] = res.astype(BF16)
        z_copy(i).start()

    steps = hop * (blocks - 1) + gap * (pieces - 1) + 1
    lax.fori_loop(0, tiles, lambda i, carry: (tile(i), carry)[1], 0)
    lax.fori_loop(tiles * len(parts), steps, lambda j, carry: (pass_on(j), carry)[1], 0)

    for i in PAIR:
        z_copy(tiles - 1 - i).wait()

    @pl.when(blk_id < blocks - 1)
    def _():
        for p in range(pieces):
            hop_copy(p).wait_send()


def z_chain(x_full, w_z, s_end, dec, chips, blocks, pieces=8, hop=5, gap=2, nt=512, parts=4):
    t, d_model = x_full.shape
    n_state, inner = s_end.shape
    tm = t // chips
    piece = scratch(F32, pieces, n_state, inner // pieces)
    two = sems(2)
    return pl.pallas_call(
        functools.partial(chain_kernel, chips, blocks, pieces, hop, gap, nt),
        in_specs=[ANY, ANY, VMEM, VMEM],
        out_specs=[ANY, VMEM],
        out_shape=[out_of(BF16, t, inner), out_of(F32, n_state, inner)],
        scratch_shapes=[scratch(BF16, 2, tm, d_model), scratch(BF16, 2, d_model, nt), scratch(BF16, 2, tm, nt), piece, piece,
                        sems(2, parts), sems(2, parts), two, sems(pieces), sems(pieces)],
        compiler_params=params(60, 2),
        cost_estimate=pl.CostEstimate(flops=t * inner * d_model, bytes_accessed=t * inner, transcendentals=0),
        name='z_chain',
    )(x_full, w_z, s_end, dec)


def out_kernel(chips, nb, wc, slots, zt, zlast, xact_ref, bc_ref, cum_ref, cl_ref, seg_ref, segp_ref, sloc_ref, pd_ref, sin_ref, z_ref, xf_ref, wz_ref,
               dskip_ref, nw_ref, wo_ref, wp_ref, x_ref, o_ref, recv_ref,
               va_own, va_par, wbuf, send, acc, rbuf, xo, xg, wzb, zb, xa, bca, sl, sbf, yoff, gated, dlane,
               vs_sem, vr_sem, w_sem, s_sem, r_sem, l_sem, x_sem, o_sem, c_sem, z_sem, v_sem):
    me = lax.axis_index('tp')
    chip, core = me // CORES, odd(me)
    partner = CORES * chip + flip(core)
    chip_at = lambda d: lax.rem(chip + d, chips)
    ring = [CORES * chip_at(chips - 1) + core, CORES * chip_at(1) + core]
    q = va_own.shape[1]
    inner = xa.shape[DIRS]
    heads = cum_ref.shape[0]
    head_dim = inner // heads
    per = LANES // head_dim
    n_state = sl.shape[1]
    half_cols = nb * wc
    hops = chips - 1
    steps = hops * nb * DIRS
    lag = acc.shape[1] - 1
    depth = slots // DIRS
    hq = q // DIRS
    ready = greet([('tp', partner)] + [('tp', r) for r in ring])

    def cols_of(u):
        d = odd(u)
        side = jnp.where(u < DIRS * nb * (hops - 1), d, flip(d))
        return rows_at(side * half_cols + lax.rem(u // DIRS, nb) * wc, wc)

    def w_copies(u):
        slot = odd(u)
        return [pltpu.make_async_copy(ref.at[:, cols_of(u)], wbuf.at[slot, i], w_sem.at[slot, i]) for i, ref in enumerate((wo_ref, wp_ref))]

    def place(n):
        return chip_at(jnp.where(n == 0, chips // DIRS, jnp.where(n == 1, 1, jnp.where(n == DIRS, chips - 1, 0))))

    def parity(i):
        return jnp.where(i == 0, flip(core), core)

    def load(n, i):
        c = CORES * place(n) + parity(i)
        at = rows_at(c * q, q)
        return [pltpu.make_async_copy(xact_ref.at[at, :], xa.at[i], c_sem.at[i, 0]), pltpu.make_async_copy(bc_ref.at[at, :], bca.at[i], c_sem.at[i, 1]),
                pltpu.make_async_copy(sloc_ref.at[c], sl.at[i], c_sem.at[i, DIRS]), pltpu.make_async_copy(z_ref.at[at, :], zb.at[parity(i)], c_sem.at[i, 3])]

    for i in PAIR:
        for cp in load(0, i):
            cp.start()
    for cp in w_copies(0):
        cp.start()
    x_copy = pltpu.make_async_copy(x_ref, xo, x_sem)
    dlane[...] = expand_heads(dskip_ref[...], head_dim)
    ready()

    def swap(n, j):
        return remote(va_own.at[chips + odd(n)], va_par.at[j], vs_sem.at[n], vr_sem.at[n], 'tp', partner)

    def mix(c, i, tgt):
        at = rows_at(c * q, q)
        seg_row = seg_ref[:, at]
        seg_prev = segp_ref[c][:, LANES - 1:]
        seg_rows = jnp.broadcast_to(seg_row, (q, q))
        causal = lax.broadcasted_iota(jnp.int32, (q, q), 0) >= lax.broadcasted_iota(jnp.int32, (q, q), 1)
        bias = jnp.where(causal & (seg_rows == seg_rows.T), 0.0, NEG)
        cum = cum_ref[:, at]
        cl = cl_ref[:, at]
        cum_cols = cum.T
        in_cols = jnp.where(seg_row == seg_prev, jnp.exp2(cum), 0.0).T
        sbf[...] = (sl[i] + pd_ref[c] * sin_ref[...]).astype(BF16)
        c_act = bca[i, :, n_state:]
        scores = lax.dot_general(c_act, bca[i, :, 0:n_state], (((1,), (1,)), ((), ())), preferred_element_type=F32)
        yoff[...] = dot32(c_act, sbf[...])
        lane = lax.broadcasted_iota(jnp.int32, (q, LANES), 1) // head_dim
        sq = jnp.zeros((q, LANES), F32)
        for m in range(inner // LANES):
            cols = slice(m * LANES, (m + 1) * LANES)
            x_f = xa[i, :, cols].astype(F32)
            tops, bots = [], []
            for j in range(per):
                h = m * per + j
                x_h = jnp.where(lane == j, x_f, 0.0).astype(BF16)
                ccol, crow = cum_cols[:, h:h + 1], cl[h:h + 1, :]
                m_top = jnp.exp2(ccol[0:hq] + bias[0:hq, 0:hq] - crow[:, 0:hq]) * scores[0:hq, 0:hq]
                m_bot = jnp.exp2(ccol[hq:] + bias[hq:] - crow) * scores[hq:]
                tops.append(dot32(m_top.astype(BF16), x_h[0:hq]))
                bots.append(dot32(m_bot.astype(BF16), x_h))
            y = jnp.concatenate([sum(tops), sum(bots)], axis=0)
            y = y + yoff[:, cols] * head_lanes(in_cols, m, head_dim) + dlane[:, cols] * x_f
            v = y * silu(zb[parity(i), :, cols].astype(F32))
            gated[:, cols] = v
            sq = sq + v * v
        inv = lax.rsqrt(jnp.sum(sq, axis=1, keepdims=True) * (1.0 / inner) + NORM_EPS)
        inv = jnp.broadcast_to(inv, (q, LANES))
        for m in range(inner // LANES):
            cols = slice(m * LANES, (m + 1) * LANES)
            va_own[tgt, :, cols] = (gated[:, cols] * inv * nw_ref[m:m + 1, :].astype(F32)).astype(BF16)

    def prep(n):
        j = place(n)
        tok = rows_at(j * (CORES * q), CORES * q)

        @pl.when(n >= DIRS)
        def _():
            for i in PAIR:
                for cp in load(n, i)[:3]:
                    cp.start()

        @pl.when(n < DIRS)
        def _():
            for i in PAIR:
                load(n, i)[3].wait()

        @pl.when(n >= 1)
        def _():
            first = jnp.where(n == 1, (inner - zlast) // zt, 0)

            def wz_copy(m):
                return pltpu.make_async_copy(wz_ref.at[:, rows_at(m * zt, zt)], wzb.at[odd(m)], z_sem.at[odd(m)])
            rows_copy = pltpu.make_async_copy(xf_ref.at[tok, :], xg, v_sem)
            rows_copy.start()
            wz_copy(first).start()
            rows_copy.wait()

            def z_body(m, carry):
                wz_copy(m).wait()

                @pl.when(m + 1 < inner // zt)
                def _():
                    wz_copy(m + 1).start()
                res = dot32(xg[...], wzb[odd(m)]).astype(BF16)
                for p in PAIR:
                    zb[p, :, rows_at(m * zt, zt)] = res[p * q:(p + 1) * q]
                return carry
            lax.fori_loop(first, inner // zt, z_body, 0)

        @pl.when(n >= DIRS)
        def _():
            swap(n - DIRS, j).wait_send()

        def chunk(i, carry):
            for cp in load(n, i)[:3]:
                cp.wait()
            mix(CORES * j + parity(i), i, jnp.where(i == 0, chips + odd(n), j))

            @pl.when(n == 0)
            def _():
                for cp in load(1, i):
                    cp.start()

            @pl.when(i == 0)
            def _():
                swap(n, j).start()
            return carry
        lax.fori_loop(0, CORES, chunk, 0)
        swap(n, j).wait_recv()

    def ring_copy(d, unit):
        slot = lax.rem(unit, slots)
        return remote(send.at[d, slot], recv_ref.at[d, unit], s_sem.at[d, slot], r_sem.at[d, unit], 'tp', jnp.where(d == 0, ring[1], ring[0]))

    def fetch(d, unit, at):
        ring_copy(d, unit).wait_recv()
        cp = pltpu.make_async_copy(recv_ref.at[d, unit], rbuf.at[at], l_sem.at[at])
        cp.start()
        return cp

    def o_copy(d, b):
        cols = rows_at(d * half_cols + b * wc, wc)
        return pltpu.make_async_copy(xo.at[:, cols], o_ref.at[:, cols], o_sem.at[d, b])

    def product(dest, slot):
        return dot32(va_own[dest], wbuf[slot, 0]) + dot32(va_par[dest], wbuf[slot, 1])

    def finish(d, b):
        last = (hops - 1) * nb + b
        copies = [fetch(d, last, 0), fetch(flip(d), last - nb, 1)]
        for cp in copies:
            cp.wait()
        cols = rows_at(flip(d) * half_cols + b * wc, wc)
        xo[:, cols] = (xo[:, cols].astype(F32) + (acc[d, lax.rem(b, lag + 1)] + (rbuf[0] + rbuf[1]))).astype(BF16)
        o_copy(flip(d), b).start()

    def body(u, carry):
        d = odd(u)
        k = u // (DIRS * nb)
        b = lax.rem(u // DIRS, nb)
        unit = k * nb + b
        ending = k == hops - 1

        @pl.when((d == 0) & ((b == 0) | ((k == 0) & (b == slots + 1))))
        def _():
            prep(jnp.where(u == 0, 0, k + 1))
        dest = chip_at(jnp.where(k == 0, chips // DIRS, jnp.where(d == 0, 1, chips - 1)))
        for cp in w_copies(u):
            cp.wait()

        @pl.when(u + 1 < steps)
        def _():
            for cp in w_copies(u + 1):
                cp.start()

        @pl.when(u == DIRS)
        def _():
            x_copy.start()
        part = product(dest, d)
        slot = lax.rem(unit, slots)

        @pl.when((unit >= slots) & (flip(ending) | (b < slots - depth)))
        def _():
            ring_copy(d, unit - slots).wait_send()

        @pl.when(ending)
        def _():
            ring_copy(d, unit - depth).wait_send()

        @pl.when(k != 1)
        def _():
            send[d, slot] = part

        @pl.when(k == 1)
        def _():
            fetch(d, unit - nb, 0).wait()
            send[d, slot] = part + rbuf[0]
        ring_copy(d, unit).start()

        @pl.when(ending)
        def _():
            acc[d, lax.rem(b, lag + 1)] = product(chip, d)

            @pl.when(b == 0)
            def _():
                pl.when(d == 0)(x_copy.wait)

            @pl.when(b >= lag)
            def _():
                finish(d, b - lag)
        return carry

    lax.fori_loop(0, steps, body, 0)

    def tail(i, carry):
        finish(odd(i), nb - lag + i // DIRS)
        return carry

    def drain(i, carry):
        o_copy(odd(i), i // DIRS).wait()
        return carry

    def drain_send(i, carry):
        ring_copy(odd(i), hops * nb - depth + i // DIRS).wait_send()
        return carry
    lax.fori_loop(0, DIRS * lag, tail, 0)
    lax.fori_loop(0, DIRS * depth, drain_send, 0)
    for n in PAIR:
        swap(DIRS + n, chip).wait_send()
    lax.fori_loop(0, DIRS * nb, drain, 0)


def out_proj_scatter(x_act, bc_act, cum, cl, seg_row, seg_prev, sloc, pd, s_in, z_arr, x_full, w_z, d_skip, norm_w, w_own, w_par, x_loc, chips, wc=512, slots=4, zt=256, zlast=1024):
    t, inner = x_act.shape
    rows, d_model = x_loc.shape
    gw = bc_act.shape[1]
    n_state = s_in.shape[0]
    nb = d_model // DIRS // wc
    units = (chips - 1) * nb
    return pl.pallas_call(
        functools.partial(out_kernel, chips, nb, wc, slots, zt, zlast),
        in_specs=[ANY, ANY, VMEM, VMEM, VMEM, VMEM, ANY, VMEM, VMEM, ANY, ANY, ANY, VMEM, VMEM, ANY, ANY, ANY],
        out_specs=[ANY, ANY],
        out_shape=[out_of(BF16, rows, d_model), out_of(F32, DIRS, units, rows, wc)],
        scratch_shapes=[scratch(BF16, chips + DIRS, rows, inner), scratch(BF16, chips, rows, inner), scratch(BF16, DIRS, DIRS, inner, wc), scratch(F32, DIRS, slots, rows, wc), scratch(F32, DIRS, slots, rows, wc),
                        scratch(F32, DIRS, rows, wc), scratch(BF16, rows, d_model), scratch(BF16, CORES * rows, d_model), scratch(BF16, DIRS, d_model, zt),
                        scratch(BF16, CORES, rows, inner), scratch(BF16, DIRS, rows, inner), scratch(BF16, DIRS, rows, gw), scratch(F32, DIRS, n_state, inner),
                        scratch(BF16, n_state, inner), scratch(F32, rows, inner), scratch(F32, rows, inner), scratch(F32, 1, inner),
                        sems(chips), sems(chips), sems(DIRS, DIRS), sems(DIRS, slots), sems(DIRS, units), sems(DIRS), DMA, sems(DIRS, nb), sems(DIRS, 4), sems(DIRS), DMA],
        compiler_params=params(63, 1),
        cost_estimate=pl.CostEstimate(flops=DIRS * t * inner * d_model, bytes_accessed=t * d_model, transcendentals=0),
        name='out_proj_scatter',
    )(x_act, bc_act, cum, cl, seg_row, seg_prev, sloc, pd, s_in, z_arr, x_full, w_z, d_skip, norm_w, w_own, w_par, x_loc)[0]


def layer(x_loc, seg_loc, w_zx, w_bc, w_dt, conv_x, conv_bc, bias_x, bias_bc, a_log, dt_bias, d_skip, norm_w, w_out, chips, blocks):
    rows = x_loc.shape[0]
    tiled = lambda v: v.reshape(v.shape[0] // LANES, LANES)
    x_full, x_pre, small, w_z, w_par, seg, seg_tail, tail_x, tail_b = gather_proj(x_loc, w_zx, w_bc, w_dt.T, w_out, seg_loc[None], chips, blocks)
    x_act, bc_act, cum, cl, seg_row, seg_prev, sloc, pd, s_end, dec = phase_a(
        x_pre, small, seg, seg_tail, tail_x, tail_b, conv_x, conv_bc, tiled(bias_x), bias_bc, a_log[None], dt_bias[None], rows)
    z_arr, s_in = z_chain(x_full, w_z, s_end, dec, chips, blocks)
    return out_proj_scatter(x_act, bc_act, cum, cl, seg_row, seg_prev, sloc, pd, s_in, z_arr, x_full, w_z, d_skip[None], tiled(norm_w), w_out, w_par, x_loc, chips)


def solution(mesh):
    tokens = ('dp', 'sp', 'tp')
    heads = P('tp')
    cols = P(None, 'tp')
    deep = P(None, None, 'tp')
    specs = (P(tokens, None), P(tokens), deep, deep, cols, cols, deep, heads, cols, heads, heads, heads, heads, P('tp', None))
    body = functools.partial(layer, chips=mesh.shape['tp'] // CORES, blocks=mesh.shape['sp'])
    return jax.shard_map(body, mesh=mesh, in_specs=specs, out_specs=specs[0], check_vma=False)
```
